32 devices in a mesh: dp: 1 (over z), tp: 4 (over y), ep: 8 (over x, core).
Axes of the slice: x: 4, y: 4, z: 1, core: 2. Of those that a mesh axis runs over, the one named last changes fastest.
The devices are a block of a 4x4x8 slice.
Arguments:
- tokens_x: bfloat16 [16384, 2048], P(('dp', 'ep', 'tp'))
- expert_ids: int32 [16384, 6], P(('dp', 'ep', 'tp'))
- route_gate: float32 [16384, 6], P(('dp', 'ep', 'tp'))
- w_gate: bfloat16 [64, 2048, 1408], P('ep', None, 'tp')
- w_up: bfloat16 [64, 2048, 1408], P('ep', None, 'tp')
- w_down: bfloat16 [64, 1408, 2048], P('ep', 'tp')
Outputs:
- output: bfloat16 [16384, 2048], P(('dp', 'ep', 'tp'))
All inputs are finite; a program needn't handle non-finite values.
Results may differ from the reference program's by a relative error of at most 0.00122.
Values are sent between devices in bfloat16 or wider.
A program may use at most 768 MiB of HBM per device.

```python
import jax
import jax.numpy as jnp
from jax import lax

D_MODEL = 2048
FF_DIM = 1408
EXPERTS = 64
TOP_K = 6
EP_GROUP = 8
TOKENS = 16384


def draw_routing(route_key):
    num_blocks = TOKENS // EXPERTS
    per_dev = EXPERTS // EP_GROUP
    key_pos, key_dev, key_loc = jax.random.split(route_key, 3)
    row_pos = jax.vmap(lambda one_key: jax.random.permutation(one_key, EXPERTS))(jax.random.split(key_pos, num_blocks))
    dev_perm = jax.vmap(lambda one_key: jax.random.permutation(one_key, EP_GROUP))(jax.random.split(key_dev, num_blocks))
    loc_perm = jax.vmap(lambda one_key: jax.random.permutation(one_key, per_dev))(jax.random.split(key_loc, num_blocks * EP_GROUP))
    loc_perm = loc_perm.reshape(num_blocks, EP_GROUP, per_dev)
    slot_offset = jnp.arange(TOP_K, dtype=jnp.int32)

    def block_ids(dev_order, loc_order, positions):
        labels = (positions[:, None] + slot_offset[None, :]) % EXPERTS
        dev_slot = labels % EP_GROUP
        return dev_order[dev_slot] * per_dev + loc_order[dev_slot, labels // EP_GROUP]

    all_ids = jax.vmap(block_ids)(dev_perm, loc_perm, row_pos)
    return all_ids.reshape(TOKENS, TOP_K).astype(jnp.int32)


def setup_inputs(seed: int = 0, part: int = 0) -> dict:
    part_key = jax.random.fold_in(jax.random.key(seed), part)
    key_x, key_gate, key_route = jax.random.split(part_key, 3)
    key_wg, key_wu, key_wd = jax.random.split(jax.random.key(seed + 1), 3)
    tokens_x = jax.random.normal(key_x, (TOKENS, D_MODEL), jnp.float32).astype(jnp.bfloat16)
    expert_ids = draw_routing(key_route)
    route_gate = jax.random.uniform(key_gate, (TOKENS, TOP_K), jnp.float32, 0.5, 1.5) * TOP_K ** -0.5
    w_gate = (jax.random.normal(key_wg, (EXPERTS, D_MODEL, FF_DIM), jnp.float32) * D_MODEL ** -0.5).astype(jnp.bfloat16)
    w_up = (jax.random.normal(key_wu, (EXPERTS, D_MODEL, FF_DIM), jnp.float32) * D_MODEL ** -0.5).astype(jnp.bfloat16)
    w_down = (jax.random.normal(key_wd, (EXPERTS, FF_DIM, D_MODEL), jnp.float32) * FF_DIM ** -0.5).astype(jnp.bfloat16)
    return dict(tokens_x=tokens_x, expert_ids=expert_ids, route_gate=route_gate, w_gate=w_gate, w_up=w_up, w_down=w_down)


def reference(tokens_x, expert_ids, route_gate, w_gate, w_up, w_down):
    expert_cap = TOKENS * TOP_K // EXPERTS
    sort_order = jnp.argsort(expert_ids.reshape(-1), stable=True)
    tok_rows = (sort_order // TOP_K).reshape(EXPERTS, expert_cap)
    gate_rows = route_gate.reshape(-1)[sort_order].reshape(EXPERTS, expert_cap)

    def add_expert(acc_sum, per_expert):
        rows_e, gates_e, wg_e, wu_e, wd_e = per_expert
        x_rows = tokens_x[rows_e]
        h_gate = jnp.dot(x_rows, wg_e, preferred_element_type=jnp.float32)
        h_up = jnp.dot(x_rows, wu_e, preferred_element_type=jnp.float32)
        hidden = (jax.nn.silu(h_gate) * h_up).astype(jnp.bfloat16)
        out_rows = jnp.dot(hidden, wd_e, preferred_element_type=jnp.float32) * gates_e[:, None]
        return acc_sum.at[rows_e].add(out_rows), None

    acc_init = jnp.zeros((TOKENS, D_MODEL), jnp.float32)
    y_total, _ = lax.scan(add_expert, acc_init, (tok_rows, gate_rows, w_gate, w_up, w_down))
    return y_total.astype(jnp.bfloat16)
```

```python
import functools

import jax
import jax.numpy as jnp
from jax import lax
from jax.experimental import pallas as pl
from jax.experimental.pallas import tpu as pltpu
from jax.sharding import PartitionSpec as P

MESH = pl.DeviceIdType.MESH
CHUNKS = 4
BF16 = jnp.bfloat16
F32 = jnp.float32

S, A, B, O = 0, 1, 2, 3


def order_of(i):
    t = i + (i + 13) // 16 + 3 * (i // 15)
    p, r = t // 4, t % 4
    return r + r // 2 - 2 * (r // 3), p - r // 3


BATCH = {order_of(i): i for i in range(16)}


def place(y, q):
    high, low = y // 2, y % 2
    return 2 * ((high + q // 2) % 2) + (low + (q + 1) // 2) % 2


def routing_tables(ids, gates, experts, per_expert):
    rows = ids.shape[0]
    chosen = ids[:, :, None] == jnp.arange(experts, dtype=ids.dtype)
    picked = jnp.any(chosen, axis=1)
    weight = jnp.sum(jnp.where(chosen, gates[:, :, None], 0.0), axis=1)
    before = (jnp.arange(rows)[:, None] > jnp.arange(rows)[None, :]).astype(BF16)
    rank = jnp.dot(before, picked.astype(BF16), preferred_element_type=F32)
    rank = jnp.where(picked, rank, -1.0)
    hit = rank[:, :, None] == jnp.arange(per_expert, dtype=F32)
    row = jnp.arange(rows, dtype=F32)[:, None, None]
    position = jnp.sum(jnp.where(hit, row, 0.0), axis=0)
    value = jnp.sum(jnp.where(hit, weight[:, :, None], 0.0), axis=0)
    return position, value


def moe_kernel(nx, ny, x_ref, meta_ref, wg_ref, wu_ref, wd_ref, out_ref, tok_ref, h_ref, w_ref, db_ref,
               metav, rb, ms, mr, ty_s, ty_r, tx_s, tx_r, td_s, td_r, hd_r, hf_s, hf_r, wa_s, wa_r, wb_s, wb_r, wf_s, wf_r,
               rs_r, db_r, of_r):
    rows, width = x_ref.shape
    half = rows // 2
    el, _, ff = wg_ref.shape
    per = h_ref.shape[5]
    pairs = el * per
    kc, cw = w_ref.shape[0], w_ref.shape[4]
    eps = 2 * nx
    y = lax.axis_index('tp')
    ep = lax.axis_index('ep')
    x, c = ep // 2, ep % 2
    ya, yb, yo = place(y, A), place(y, B), place(y, O)
    yq = (y, ya, yb, yo)
    xp, xm = (x + 1) % nx, (x + nx - 1) % nx
    colb = ((y + y // 2) % 2) * (kc * cw)
    cola = ((ya + ya // 2) % 2) * (kc * cw)
    me = y * eps + ep

    dev_a = {'tp': ya, 'ep': ep}
    dev_b = {'tp': yb, 'ep': ep}
    dev_p = {'tp': y, 'ep': 2 * x + 1 - c}
    dev_xp = {'tp': y, 'ep': 2 * xp + c}
    dev_xm = {'tp': y, 'ep': 2 * xm + c}

    def remote(src, dst, send, recv, dev):
        return pltpu.make_async_remote_copy(src_ref=src, dst_ref=dst, send_sem=send, recv_sem=recv, device_id=dev, device_id_type=MESH)

    def lin(xs, ys, cs):
        return ys * eps + 2 * xs + cs

    barrier = pltpu.get_barrier_semaphore()

    def peer_of(d):
        other = (me + d) % (ny * eps)
        return other // eps, other % eps

    def greet(d, carry):
        py, pe = peer_of(d)
        pl.semaphore_signal(barrier, inc=1, device_id={'tp': py, 'ep': pe}, device_id_type=MESH)
        return carry

    lax.fori_loop(1, ny * eps, greet, 0)
    pl.semaphore_wait(barrier, ny * eps - 1)

    def meta_copy(d):
        py, pe = peer_of(d)
        return remote(meta_ref.at[pe], metav.at[me], ms.at[d], mr.at[me], {'tp': py, 'ep': pe})

    def meta_send(d, carry):
        meta_copy(d).start()
        return carry

    lax.fori_loop(1, ny * eps, meta_send, 0)
    metav[me] = meta_ref[ep]

    def own(dxm, q):
        return tok_ref.at[(x + dxm) % nx, yq[q], c]

    def rows_of(ref, part):
        return ref.at[pl.ds(part * half, half)]

    def ty(n):
        if n == 0:
            return remote(x_ref, tok_ref.at[x, y, c], ty_s.at[0], ty_r.at[0], dev_a)
        if n == 1:
            return remote(x_ref, tok_ref.at[x, y, c], ty_s.at[1], ty_r.at[1], dev_b)
        if n == 2:
            return remote(rows_of(own(0, B), 0), rows_of(own(0, B), 0), ty_s.at[2], ty_r.at[2], dev_a)
        return remote(rows_of(own(0, A), 1), rows_of(own(0, A), 1), ty_s.at[3], ty_r.at[3], dev_b)

    def tx(q, n):
        if n < 2:
            src = x_ref if q == S else own(0, q)
            return remote(src, own(0, q), tx_s.at[q, n], tx_r.at[q, n], (dev_xp, dev_xm)[n])
        block = rows_of(own((3, 1)[n - 2], q), n - 2)
        return remote(block, block, tx_s.at[q, n], tx_r.at[q, n], (dev_xp, dev_xm)[n - 2])

    def td(q, dxm):
        src = x_ref if (q == S and dxm == 0) else own(dxm, q)
        return remote(src, own(dxm, q), td_s.at[q, dxm], td_r.at[q, dxm], dev_p)

    def wa(k):
        src = wd_ref.at[:, :, pl.ds(pl.multiple_of(cola + k * cw, cw), cw)]
        return remote(src, w_ref.at[k, y], wa_s.at[k], wa_r.at[k], dev_a)

    def wb(k):
        src = wd_ref.at[:, :, pl.ds(pl.multiple_of(colb + k * cw, cw), cw)]
        return remote(src, w_ref.at[k, y], wb_s.at[k], wb_r.at[k], dev_b)

    def wf(k):
        return remote(w_ref.at[k, ya], w_ref.at[k, ya], wf_s.at[k], wf_r.at[k], dev_b)

    def forward_w(k):
        wa(k).wait_recv()
        wf(k).start()

    def hf(i):
        dxm, q = order_of(i)
        block = h_ref.at[yb, (x + dxm) % nx, place(yb, q)]
        return remote(block, block, hf_s.at[i], hf_r.at[i], dev_a)

    def hd_wait(i):
        block = h_ref.at[0, 0, 0]
        remote(block, block, hf_s.at[i], hd_r.at[i], dev_a).wait_recv()

    def forward_h(i):
        hd_wait(i)
        hf(i).start()

    for n in (0, 1):
        ty(n).start()
        tx(S, n).start()
    td(S, 0).start()
    wa(0).start()
    wb(0).start()

    def comm(step):
        if step == 1:
            ty(0).wait_recv()
            ty(1).wait_recv()
            ty(2).start()
            ty(3).start()
            tx(A, 0).start()
            tx(A, 1).start()
            td(A, 0).start()
            td(B, 0).start()
            for n in (0, 1):
                tx(S, n).wait_recv()
            for n in (2, 3):
                tx(S, n).start()
            td(S, 3).start()
            td(S, 1).start()
            tx(B, 0).start()
            tx(B, 1).start()
        if step == 4:
            for n in (0, 1):
                tx(A, n).wait_recv()
            for n in (2, 3):
                tx(A, n).start()
            td(A, 3).start()
            td(A, 1).start()
            ty(2).wait_recv()
            ty(3).wait_recv()
            td(O, 0).start()
            tx(O, 0).start()
            tx(O, 1).start()
            forward_w(0)
            wb(1).start()
        if step in (6, 10, 14, 15):
            q = {6: S, 10: A, 14: B, 15: O}[step]
            tx(q, 2).wait_recv()
            tx(q, 3).wait_recv()
            td(q, 2).start()
        if step in (8, 12):
            q = {8: B, 12: O}[step]
            for n in (0, 1):
                tx(q, n).wait_recv()
            for n in (2, 3):
                tx(q, n).start()
            td(q, 3).start()
            td(q, 1).start()
        if step == 8:
            wa(1).start()
        for i in {10: (7,), 12: (8, 9), 14: (11,), 15: (12, 13)}.get(step, ()):
            forward_h(i)
        if step == 12:
            forward_w(1)
            wb(2).start()
        if step == 15:
            wa(2).start()

    row_id = lax.broadcasted_iota(jnp.int32, (rows, pairs), 0)

    def one_hot(src):
        pos = metav[src, 0:1, :].astype(jnp.int32)
        return (row_id == pos).astype(F32).astype(BF16)

    def meta_wait(src):
        remote(meta_ref.at[0], metav.at[src], ms.at[0], mr.at[src], dev_p).wait_recv()

    def phase_one(wg, wu, tb, xg, hb, wl, tl, hl, hd_s):
        load_g = pltpu.make_async_copy(wg_ref, wg, wl.at[0])
        load_u = pltpu.make_async_copy(wu_ref, wu, wl.at[1])
        load_g.start()
        load_u.start()

        def hidden_out(i, dxm, q, slot):
            xs, ys = (x + dxm) % nx, place(y, q)
            return (
                pltpu.make_async_copy(hb.at[slot], h_ref.at[y, xs, ys], hl.at[slot]),
                remote(hb.at[slot], h_ref.at[y, xs, ys], hd_s.at[slot], hd_r.at[i], dev_a),
                remote(hb.at[slot], h_ref.at[y, xs, ys], hd_s.at[slot], hd_r.at[i], dev_b),
            )

        def drain(i):
            dxm, q = order_of(i)
            local, _, away = hidden_out(i, dxm, q, i % 2)

            @pl.when(q < 2)
            def _():
                local.wait()

            away.wait_send()

        def batch(i, carry):
            for step in (1, 4, 6, 8, 10, 12, 14, 15):
                pl.when(i == step)(functools.partial(comm, step))
            dxm, q = order_of(i)
            xs, ys = (x + dxm) % nx, place(y, q)
            slot = i % 2
            remote(tok_ref.at[xs, ys, c], tok_ref.at[xs, ys, c], td_s.at[q, dxm], td_r.at[q, dxm], dev_p).wait_recv()
            mine = pltpu.make_async_copy(x_ref, tb.at[0], tl.at[0])
            other = pltpu.make_async_copy(tok_ref.at[xs, ys, c], tb.at[0], tl.at[0])
            theirs = pltpu.make_async_copy(tok_ref.at[xs, ys, 1 - c], tb.at[1], tl.at[1])

            @pl.when(i == 0)
            def _():
                mine.start()

            @pl.when(i > 0)
            def _():
                other.start()

            theirs.start()

            @pl.when(i > 0)
            def _():
                meta_wait(lin(xs, ys, c))

            meta_wait(lin(xs, ys, 1 - c))

            @pl.when(i == 0)
            def _():
                load_g.wait()
                load_u.wait()

            @pl.when(i > 1)
            def _():
                drain(i - 2)

            for s in (0, 1):
                (other, theirs)[s].wait()
                hot = one_hot(lin(xs, ys, c if s == 0 else 1 - c))
                step = min(512, width)
                for lo in range(0, width, step):
                    got = lax.dot_general(hot, tb[s, :, lo:lo + step], (((0,), (0,)), ((), ())), preferred_element_type=F32)
                    xg[:, s, :, lo:lo + step] = got.astype(BF16).reshape(el, per, step)

            def expert(e, carry):
                lhs = xg[e].reshape(2 * per, width)
                a = jnp.dot(lhs, wg[e], preferred_element_type=F32)
                b = jnp.dot(lhs, wu[e], preferred_element_type=F32)
                hid = (a * jax.nn.sigmoid(a) * b).astype(BF16).reshape(2, per, ff)
                for s in (0, 1):
                    hb[slot, jnp.where(c == s, 0, 1), e] = hid[0] if s == 0 else hid[1]
                return carry

            lax.fori_loop(0, el, expert, 0)
            local, to_a, to_b = hidden_out(i, dxm, q, slot)

            @pl.when(q < 2)
            def _():
                local.start()
                to_a.start()

            @pl.when(q >= 2)
            def _():
                to_b.start()

            return carry

        lax.fori_loop(0, 16, batch, 0)
        drain(14)
        drain(15)

    pl.run_scoped(
        phase_one,
        pltpu.VMEM((el, width, ff), BF16),
        pltpu.VMEM((el, width, ff), BF16),
        pltpu.VMEM((2, rows, width), BF16),
        pltpu.VMEM((el, 2, per, width), BF16),
        pltpu.VMEM((2, 2, el, per, ff), BF16),
        pltpu.SemaphoreType.DMA((2,)),
        pltpu.SemaphoreType.DMA((2,)),
        pltpu.SemaphoreType.DMA((2,)),
        pltpu.SemaphoreType.DMA((2,)),
    )
    wa(3).start()
    wb(3).start()
    forward_h(14)
    forward_h(15)

    def unit_of(n):
        return 2 * (n // 8) + n % 2, (n % 8) // 2

    def phase_two(wv, hv, gc, o3, pb, pp, sb, dv, fb, wl, hvl, dl, pp_s, rs_s, of_s, ol):
        def shape_of(n):
            k, j = unit_of(n)
            return k, j, ((x + 2 * nx - 1 - j) % nx, (x + 1 + j) % nx), (y, ya)

        def load_w(k):
            src = wd_ref.at[:, :, pl.ds(pl.multiple_of(colb + k * cw, cw), cw)]
            copies = [pltpu.make_async_copy(src, wv.at[k % 2, S], wl.at[S])]
            for q in (A, B, O):
                copies.append(pltpu.make_async_copy(w_ref.at[k, yq[q]], wv.at[k % 2, q], wl.at[q]))
            return copies

        def partner_copy(n, d):
            k, j, _, _ = shape_of(n)
            return remote(pp.at[n % 2, d], db_ref.at[d, k, j], pp_s.at[n % 2, d], db_r.at[d, k, j], dev_p)

        def ring_copy(n, d, k, j):
            return remote(sb.at[n % 4, d], rb.at[d, k, j], rs_s.at[n % 4, d], rs_r.at[d, k, j], (dev_xp, dev_xm)[d])

        def out_copies(n, k):
            cols = out_ref.at[:, pl.ds(pl.multiple_of(colb + k * cw, cw), cw)]
            return (
                pltpu.make_async_copy(fb.at[n % 2, 0], cols, ol.at[n % 2]),
                remote(fb.at[n % 2, 1], cols, of_s.at[n % 2], of_r.at[k], dev_a),
            )

        def make(n):
            k, j, xs, ys = shape_of(n)
            for step in range(4):
                @pl.when(n == 2 * step)
                def _(step=step):
                    minus, plus = (3 - step) % 4, (1 + step) % 4
                    hd_wait(BATCH[(minus, A)])
                    hd_wait(BATCH[(plus, S)])
                    for i in (BATCH[(minus, O)], BATCH[(plus, B)]):
                        hf(i).wait_recv()

            @pl.when(n == 4)
            def _():
                forward_w(2)

            @pl.when(n == 6)
            def _():
                forward_w(3)

            for kk, at in ((0, 0), (1, 1), (2, 8), (3, 9)):
                @pl.when(n == at)
                def _(kk=kk):
                    wb(kk).wait_recv()
                    wf(kk).wait_recv()
                    copies = load_w(kk)
                    for copy in copies:
                        copy.start()
                    for copy in copies:
                        copy.wait()

            @pl.when(n % 2 == 0)
            def _():
                copies = []
                for d in (0, 1):
                    for rel in (0, 1):
                        cs = c if rel == 0 else 1 - c
                        for q in (S, A, B, O):
                            copies.append(pltpu.make_async_copy(
                                h_ref.at[yq[q], xs[d], ys[d], cs], hv.at[q, :, 2 * d + rel], hvl.at[q, 2 * d + rel]))
                for copy in copies:
                    copy.start()
                for d in (0, 1):
                    for rel in (0, 1):
                        gate = metav[lin(xs[d], ys[d], c if rel == 0 else 1 - c), 1:2, :]
                        gc[:, 2 * d + rel] = jnp.transpose(jnp.broadcast_to(gate, (gc.shape[3], pairs))).reshape(el, per, gc.shape[3])
                for copy in copies:
                    copy.wait()

            def expert(e, carry):
                o = jnp.zeros((4 * per, cw), F32)
                for q in (S, A, B, O):
                    o = o + jnp.dot(hv[q, e].reshape(4 * per, ff), wv[k % 2, q, e], preferred_element_type=F32)
                g = gc[e].reshape(4 * per, gc.shape[3])
                v = o * jnp.concatenate([g] * (cw // gc.shape[3]), axis=1)
                hi = v.astype(BF16)
                rest = v - hi.astype(F32)
                mid = rest.astype(BF16)
                low = (rest - mid.astype(F32)).astype(BF16)
                o3[:, 0, e] = hi.reshape(4, per, cw)
                o3[:, 1, e] = mid.reshape(4, per, cw)
                o3[:, 2, e] = low.reshape(4, per, cw)
                return carry

            lax.fori_loop(0, el, expert, 0)

            @pl.when(n >= 2)
            def _():
                for d in (0, 1):
                    partner_copy(n - 2, d).wait_send()

            for rel in (1, 0):
                for d in (0, 1):
                    hot = one_hot(lin(xs[d], ys[d], c if rel == 0 else 1 - c))
                    total = jnp.dot(hot, o3[2 * d + rel, 0].reshape(pairs, cw), preferred_element_type=F32)
                    total += jnp.dot(hot, o3[2 * d + rel, 1].reshape(pairs, cw), preferred_element_type=F32)
                    total += jnp.dot(hot, o3[2 * d + rel, 2].reshape(pairs, cw), preferred_element_type=F32)
                    if rel == 1:
                        pp[n % 2, d] = total
                        partner_copy(n, d).start()
                    else:
                        pb[n % 2, d] = total

        def join(n):
            k, j, _, _ = shape_of(n)
            loads = [pltpu.make_async_copy(db_ref.at[d, k, j], dv.at[d], dl.at[d]) for d in (0, 1)]
            for d in (0, 1):
                partner_copy(n, d).wait_recv()
                loads[d].start()

            @pl.when((j < 3) & (n >= 4))
            def _():
                for d in (0, 1):
                    ring_copy(n, d, k, j).wait_send()

            @pl.when((j == 3) & (n >= 8))
            def _():
                local, away = out_copies(n, k)
                local.wait()
                away.wait_send()

            for d in (0, 1):
                loads[d].wait()

                @pl.when(j == 0)
                def _():
                    sb[n % 4, d] = pb[n % 2, d] + dv[d]

                @pl.when((j > 0) & (j < 3))
                def _():
                    ring_copy(n, d, k, j - 1).wait_recv()
                    sb[n % 4, d] = pb[n % 2, d] + dv[d] + rb[d, k, j - 1]

                @pl.when(j == 3)
                def _():
                    ring_copy(n, d, k, j - 1).wait_recv()
                    fb[n % 2, d] = (pb[n % 2, d] + dv[d] + rb[d, k, j - 1]).astype(BF16)

                @pl.when(j < 3)
                def _():
                    ring_copy(n, d, k, j).start()

            @pl.when(j == 3)
            def _():
                local, away = out_copies(n, k)
                local.start()
                away.start()

        def unit(n, carry):
            @pl.when(n < 4 * kc)
            def _():
                make(n)

            @pl.when(n > 0)
            def _():
                join(n - 1)

            return carry

        lax.fori_loop(0, 4 * kc + 1, unit, 0)
        for d in (0, 1):
            for n in (14, 15):
                partner_copy(n, d).wait_send()
            for n in (10, 11, 12, 13):
                ring_copy(n, d, 0, 0).wait_send()
        for n in (14, 15):
            local, away = out_copies(n, n - 12)
            local.wait()
            away.wait_send()
        for k in range(kc):
            out_copies(0, k)[1].wait_recv()

    lane = min(128, cw)
    pl.run_scoped(
        phase_two,
        pltpu.VMEM((2, 4, el, ff, cw), BF16),
        pltpu.VMEM((4, el, 4, per, ff), BF16),
        pltpu.VMEM((el, 4, per, lane), F32),
        pltpu.VMEM((4, 3, el, per, cw), BF16),
        pltpu.VMEM((2, 2, rows, cw), F32),
        pltpu.VMEM((2, 2, rows, cw), F32),
        pltpu.VMEM((4, 2, rows, cw), F32),
        pltpu.VMEM((2, rows, cw), F32),
        pltpu.VMEM((2, 2, rows, cw), BF16),
        pltpu.SemaphoreType.DMA((4,)),
        pltpu.SemaphoreType.DMA((4, 4)),
        pltpu.SemaphoreType.DMA((2,)),
        pltpu.SemaphoreType.DMA((2, 2)),
        pltpu.SemaphoreType.DMA((4, 2)),
        pltpu.SemaphoreType.DMA((2,)),
        pltpu.SemaphoreType.DMA((2,)),
    )

    def meta_done(d, carry):
        meta_copy(d).wait_send()
        return carry

    lax.fori_loop(1, ny * eps, meta_done, 0)
    for n in range(4):
        ty(n).wait_send()
    for q in (S, A, B, O):
        for n in range(4):
            tx(q, n).wait_send()
        for dxm in range(4):
            td(q, dxm).wait_send()
    for k in range(kc):
        wa(k).wait_send()
        wb(k).wait_send()
        wf(k).wait_send()
    for i in (7, 8, 9, 11, 12, 13, 14, 15):
        hf(i).wait_send()


def solution(mesh):
    ny, eps = mesh.shape['tp'], mesh.shape['ep']
    nx = eps // 2
    row_spec = P(('dp', 'ep', 'tp'), None)
    w_in_spec = P('ep', None, 'tp')
    w_out_spec = P('ep', 'tp', None)

    def local_moe(x, ids, gates, w_gate, w_up, w_down):
        rows, width = x.shape
        el, _, ff = w_gate.shape
        experts = el * eps
        per = rows * ids.shape[1] // experts
        pairs = el * per
        cw = width // 2 // CHUNKS
        position, value = routing_tables(ids, gates, experts, per)
        meta = jnp.stack([position.reshape(eps, pairs), value.reshape(eps, pairs)], axis=1)
        meta = jnp.pad(meta, ((0, 0), (0, 6), (0, 0)))
        hbm = pl.BlockSpec(memory_space=pl.ANY)
        vmem = pl.BlockSpec(memory_space=pltpu.VMEM)
        dma = pltpu.SemaphoreType.DMA
        outs = pl.pallas_call(
            functools.partial(moe_kernel, nx, ny),
            name='moe_kernel',
            out_shape=[
                jax.ShapeDtypeStruct((rows, width), BF16),
                jax.ShapeDtypeStruct((nx, ny, 2, rows, width), BF16),
                jax.ShapeDtypeStruct((ny, nx, ny, 2, el, per, ff), BF16),
                jax.ShapeDtypeStruct((CHUNKS, ny, el, ff, cw), BF16),
                jax.ShapeDtypeStruct((2, CHUNKS, 4, rows, cw), F32),
            ],
            in_specs=[hbm, vmem, hbm, hbm, hbm],
            out_specs=[hbm] * 5,
            scratch_shapes=[
                pltpu.VMEM((ny * eps, 8, pairs), F32),
                pltpu.VMEM((2, CHUNKS, 3, rows, cw), F32),
                dma((ny * eps,)), dma((ny * eps,)),
                dma((4,)), dma((4,)),
                dma((4, 4)), dma((4, 4)),
                dma((4, 4)), dma((4, 4)),
                dma((16,)), dma((16,)), dma((16,)),
                dma((CHUNKS,)), dma((CHUNKS,)), dma((CHUNKS,)), dma((CHUNKS,)), dma((CHUNKS,)), dma((CHUNKS,)),
                dma((2, CHUNKS, 3)), dma((2, CHUNKS, 4)), dma((CHUNKS,)),
            ],
            compiler_params=pltpu.CompilerParams(collective_id=0, has_side_effects=True, vmem_limit_bytes=66 * 1000 * 1000),
        )(x, meta, w_gate, w_up, w_down)
        return outs[0]

    return jax.shard_map(
        local_moe, mesh=mesh, in_specs=(row_spec, row_spec, row_spec, w_in_spec, w_in_spec, w_out_spec),
        out_specs=row_spec, check_vma=False)
```

```python
import functools

import jax
import jax.numpy as jnp
from jax import lax
from jax.experimental import pallas as pl
from jax.experimental.pallas import tpu as pltpu
from jax.sharding import PartitionSpec as P

MESH = pl.DeviceIdType.MESH
CHUNKS = 4
PIECES = 2
BF16 = jnp.bfloat16
F32 = jnp.float32

S, A, B, O = 0, 1, 2, 3

UNITS = ((3, 0), (2, 0), (2, 1), (3, 1), (0, 0), (2, 2), (0, 1), (1, 0), (0, 2), (1, 1), (3, 2), (0, 3), (1, 2), (3, 3), (2, 3), (1, 3), )
SEND_START = (('wa', 3, 0), ('wa', 3, 1), ('wb', 3, 0), ('wb', 1, 0), )
SEND_BEFORE = (
    (),
    (),
    (('wf', 3, 0), ('wb', 2, 1), ),
    (('hd', 2), ),
    (('hd', 3), ('wa', 2, 1), ('wa', 2, 0), ('wf', 3, 1), ('wb', 0, 1), ),
    (),
    (('hd', 5), ('wa', 0, 1), ('hd', 4), ('wa', 0, 0), ),
    (),
    (('hd', 7), ('wb', 0, 0), ('wf', 2, 1), ('wb', 3, 1), ),
    (('wf', 2, 0), ),
    (),
    (),
    (('hd', 11), ('wb', 2, 0), ('hd', 8), ('hd', 10), ),
    (('hd', 12), ),
    (('hd', 13), ('wa', 1, 0), ),
    (('hd', 14), ),
)
SEND_AFTER = (
    (),
    (),
    (),
    (),
    (),
    (),
    (),
    (),
    (),
    (),
    (('hf', 7), ('hd', 1), ),
    (),
    (),
    (),
    (('hf', 11), ('wa', 1, 1), ),
    (),
)
SEND_END = (('hd', 15), ('wf', 0, 1), ('wf', 0, 0), ('wb', 1, 1), ('wf', 1, 0), ('lw', 2), ('lw', 3), )
SEND_MAKE = (
    (('hf', 14), ('hf', 15), ('hf', 8), ('hd', 0), ('hf', 10), ('wf', 1, 1), ('hd', 6), ('hd', 9), ),
    (),
    (),
    (),
    (('lw', 0), ),
    (),
    (),
    (('lw', 1), ),
    (),
    (('hf', 6), ),
    (),
    (),
    (),
    (),
    (),
    (),
)
SEND_JOIN = (
    (),
    (),
    (),
    (),
    (),
    (),
    (),
    (),
    (),
    (('hf', 9), ),
    (),
    (),
    (),
    (),
    (),
    (),
)
SEND_PRE = (
    (),
    (),
    (),
    (),
    (),
    (),
    (),
    (),
    (),
    (),
    (),
    (),
    (),
    (),
    (),
    (),
)


def order_of(i):
    last, r = i // 12, i % 3
    return (1 - last) * (r + r // 2) + 2 * last, (1 - last) * (i // 3) + last * (i - 12)


BATCH = {order_of(i): i for i in range(16)}
FIRST_STEP = {}
for place_in_order, (chunk_of, step_of) in enumerate(UNITS):
    FIRST_STEP.setdefault(step_of, place_in_order)
SENDS = [n for n, (_, j) in enumerate(UNITS) if j < 3]
FINALS = [n for n, (_, j) in enumerate(UNITS) if j == 3]


def place(y, q):
    high, low = y // 2, y % 2
    return 2 * ((high + q // 2) % 2) + (low + (q + 1) // 2) % 2


def look_up(table, n):
    value = jnp.int32(table[0])
    for at in range(1, len(table)):
        if table[at] != table[0]:
            value = jnp.where(n == at, table[at], value)
    return value


def routing_tables(ids, gates, experts, per_expert):
    rows = ids.shape[0]
    chosen = ids[:, :, None] == jnp.arange(experts, dtype=ids.dtype)
    picked = jnp.any(chosen, axis=1)
    weight = jnp.sum(jnp.where(chosen, gates[:, :, None], 0.0), axis=1)
    before = (jnp.arange(rows)[:, None] > jnp.arange(rows)[None, :]).astype(BF16)
    rank = jnp.dot(before, picked.astype(BF16), preferred_element_type=F32)
    rank = jnp.where(picked, rank, -1.0)
    hit = rank[:, :, None] == jnp.arange(per_expert, dtype=F32)
    row = jnp.arange(rows, dtype=F32)[:, None, None]
    position = jnp.sum(jnp.where(hit, row, 0.0), axis=0)
    value = jnp.sum(jnp.where(hit, weight[:, :, None], 0.0), axis=0)
    return position, value


def moe_kernel(nx, ny, x_ref, meta_ref, wg_ref, wu_ref, wd_ref, out_ref, tok_ref, h_ref, w_ref,
               metav, rb, db, ms, mr, ty_s, ty_r, tx_s, tx_r, td_s, td_r, hd_s, hd_r, hf_s, hf_r,
               wa_s, wa_r, wb_s, wb_r, wf_s, wf_r, rs_r, db_r, of_r, credit):
    rows, width = x_ref.shape
    half = rows // 2
    el, ff, _ = wg_ref.shape
    per = h_ref.shape[5]
    pairs = el * per
    kc, cw = w_ref.shape[0], w_ref.shape[4]
    ep_piece = el // PIECES
    eps = 2 * nx
    y = lax.axis_index('tp')
    ep = lax.axis_index('ep')
    x, c = ep // 2, ep % 2
    ya, yb, yo = place(y, A), place(y, B), place(y, O)
    yq = (y, ya, yb, yo)
    xp, xm = (x + 1) % nx, (x + nx - 1) % nx
    colb = ((y + y // 2) % 2) * (kc * cw)
    cola = ((ya + ya // 2) % 2) * (kc * cw)
    me = y * eps + ep

    dev_a = {'tp': ya, 'ep': ep}
    dev_b = {'tp': yb, 'ep': ep}
    dev_p = {'tp': y, 'ep': 2 * x + 1 - c}
    dev_xp = {'tp': y, 'ep': 2 * xp + c}
    dev_xm = {'tp': y, 'ep': 2 * xm + c}

    def remote(src, dst, send, recv, dev):
        return pltpu.make_async_remote_copy(src_ref=src, dst_ref=dst, send_sem=send, recv_sem=recv, device_id=dev, device_id_type=MESH)

    def lin(xs, ys, cs):
        return ys * eps + 2 * xs + cs

    def either(rel):
        return c if rel == 0 else 1 - c

    barrier = pltpu.get_barrier_semaphore()

    def peer_of(d):
        other = (me + d) % (ny * eps)
        return other // eps, other % eps

    def greet(d, carry):
        py, pe = peer_of(d)
        pl.semaphore_signal(barrier, inc=1, device_id={'tp': py, 'ep': pe}, device_id_type=MESH)
        return carry

    lax.fori_loop(1, ny * eps, greet, 0)
    pl.semaphore_wait(barrier, ny * eps - 1)

    def meta_copy(d):
        py, pe = peer_of(d)
        return remote(meta_ref.at[pe], metav.at[me], ms.at[d], mr.at[me], {'tp': py, 'ep': pe})

    def meta_send(d, carry):
        meta_copy(d).start()
        return carry

    lax.fori_loop(1, ny * eps, meta_send, 0)
    metav[me] = meta_ref[ep]

    def own(dxm, q):
        return tok_ref.at[(x + dxm) % nx, yq[q], c]

    def rows_of(ref, part):
        return ref.at[pl.ds(part * half, half)]

    def ty(n):
        if n < 2:
            return remote(x_ref, tok_ref.at[x, y, c], ty_s.at[n], ty_r.at[n], (dev_a, dev_b)[n])
        block = rows_of(own(0, (B, A)[n - 2]), n - 2)
        return remote(block, block, ty_s.at[n], ty_r.at[n], (dev_a, dev_b)[n - 2])

    def tx(q, n):
        if n < 2:
            return remote(x_ref if q == S else own(0, q), own(0, q), tx_s.at[q, n], tx_r.at[q, n], (dev_xp, dev_xm)[n])
        block = rows_of(own((3, 1)[n - 2], q), n - 2)
        return remote(block, block, tx_s.at[q, n], tx_r.at[q, n], (dev_xp, dev_xm)[n - 2])

    def td(q, dxm):
        return remote(x_ref if (q == S and dxm == 0) else own(dxm, q), own(dxm, q), td_s.at[q, dxm], td_r.at[q, dxm], dev_p)

    def wa(k, g):
        src = wd_ref.at[pl.ds(g * ep_piece, ep_piece), :, pl.ds(pl.multiple_of(cola + k * cw, cw), cw)]
        return remote(src, w_ref.at[k, y, pl.ds(g * ep_piece, ep_piece)], wa_s.at[k, g], wa_r.at[k, g], dev_a)

    def wb(k, g):
        src = wd_ref.at[pl.ds(g * ep_piece, ep_piece), :, pl.ds(pl.multiple_of(colb + k * cw, cw), cw)]
        return remote(src, w_ref.at[k, y, pl.ds(g * ep_piece, ep_piece)], wb_s.at[k, g], wb_r.at[k, g], dev_b)

    def wf(k, g):
        block = w_ref.at[k, ya, pl.ds(g * ep_piece, ep_piece)]
        return remote(block, block, wf_s.at[k, g], wf_r.at[k, g], dev_b)

    def hd(i):
        dxm, q = order_of(i)
        block = h_ref.at[y, (x + dxm) % nx, yq[q]]
        return remote(block, block, hd_s.at[i], hd_r.at[i], dev_a if q < 2 else dev_b)

    def hf(i):
        dxm, q = order_of(i)
        block = h_ref.at[yb, (x + dxm) % nx, place(yb, q)]
        return remote(block, block, hf_s.at[i], hf_r.at[i], dev_a)

    def send(actions, load_w=None):
        for action in actions:
            kind, at = action[0], action[1:]
            if kind == 'wf':
                wa(*at).wait_recv()
            if kind == 'hf':
                hd(*at).wait_recv()
            if kind == 'lw':
                load_w(*at)
            else:
                {'wa': wa, 'wb': wb, 'wf': wf, 'hd': hd, 'hf': hf}[kind](*at).start()

    for n in (0, 1):
        ty(n).start()
        tx(S, n).start()
    td(S, 0).start()
    send(SEND_START)

    def came(q):
        for n in (0, 1):
            tx(q, n).wait_recv()
        td(q, 1).start()
        td(q, 3).start()

    def both(q, first):
        tx(q, first).start()
        tx(q, first + 1).start()

    def comm(step):
        if step == 1:
            ty(0).wait_recv()
            ty(1).wait_recv()
            ty(2).start()
            ty(3).start()
            both(A, 0)
            both(B, 0)
            came(S)
            td(A, 0).start()
            td(B, 0).start()
        if step == 4:
            came(A)
            ty(2).wait_recv()
            ty(3).wait_recv()
            both(O, 0)
            both(S, 2)
            both(A, 2)
            td(O, 0).start()
        if step in (7, 10):
            q = {7: B, 10: O}[step]
            came(q)
            both(q, 2)
        if step >= 12:
            tx(step - 12, 2).wait_recv()
            tx(step - 12, 3).wait_recv()
            td(step - 12, 2).start()

    row_id = lax.broadcasted_iota(jnp.int32, (rows, pairs), 0)

    def one_hot(src):
        pos = metav[src, 0:1, :].astype(jnp.int32)
        return (row_id == pos).astype(F32).astype(BF16)

    def meta_wait(src):
        remote(meta_ref.at[0], metav.at[src], ms.at[0], mr.at[src], dev_p).wait_recv()

    def phase_one(wg, wu, tb, xg, hb, wl, tl, hl):
        load_g = pltpu.make_async_copy(wg_ref, wg, wl.at[0])
        load_u = pltpu.make_async_copy(wu_ref, wu, wl.at[1])
        load_g.start()
        load_u.start()

        def store(i):
            dxm, q = order_of(i)
            return pltpu.make_async_copy(hb, h_ref.at[y, (x + dxm) % nx, place(y, q)], hl.at[0])

        def batch(i, carry):
            @pl.when(i > 0)
            def _():
                store(i - 1).wait()

            for step in range(1, 16):
                if SEND_BEFORE[step] or SEND_AFTER[step] or step in (1, 4, 7, 10) or step >= 12:
                    @pl.when(i == step)
                    def _(step=step):
                        send(SEND_BEFORE[step])
                        comm(step)
                        send(SEND_AFTER[step])

            dxm, q = order_of(i)
            xs, ys = (x + dxm) % nx, place(y, q)
            mine = pltpu.make_async_copy(x_ref, tb.at[0], tl.at[0])
            other = pltpu.make_async_copy(tok_ref.at[xs, ys, c], tb.at[0], tl.at[0])
            theirs = pltpu.make_async_copy(tok_ref.at[xs, ys, 1 - c], tb.at[1], tl.at[1])

            @pl.when(i == 0)
            def _():
                mine.start()

            @pl.when(i > 0)
            def _():
                other.start()
                meta_wait(lin(xs, ys, c))

            remote(tok_ref.at[xs, ys, c], tok_ref.at[xs, ys, c], td_s.at[q, dxm], td_r.at[q, dxm], dev_p).wait_recv()
            theirs.start()
            meta_wait(lin(xs, ys, 1 - c))
            for s in (0, 1):
                (other, theirs)[s].wait()
                hot = one_hot(lin(xs, ys, either(s)))
                step = min(512, width)
                for lo in range(0, width, step):
                    got = lax.dot_general(hot, tb[s, :, lo:lo + step], (((0,), (0,)), ((), ())), preferred_element_type=F32)
                    xg[:, s, :, lo:lo + step] = got.astype(BF16).reshape(el, per, step)

            @pl.when(i == 0)
            def _():
                load_g.wait()
                load_u.wait()

            def expert(e, carry):
                lhs = xg[e].reshape(2 * per, width)
                a = lax.dot_general(lhs, wg[e], (((1,), (1,)), ((), ())), preferred_element_type=F32)
                b = lax.dot_general(lhs, wu[e], (((1,), (1,)), ((), ())), preferred_element_type=F32)
                hid = (a * jax.nn.sigmoid(a) * b).astype(BF16).reshape(2, per, ff)
                for s in (0, 1):
                    hb[either(s), e] = hid[s]
                return carry

            lax.fori_loop(0, el, expert, 0)
            store(i).start()
            return carry

        lax.fori_loop(0, 16, batch, 0)
        store(15).wait()

    pl.run_scoped(
        phase_one,
        pltpu.VMEM((el, ff, width), BF16),
        pltpu.VMEM((el, ff, width), BF16),
        pltpu.VMEM((2, rows, width), BF16),
        pltpu.VMEM((el, 2, per, width), BF16),
        pltpu.VMEM((2, el, per, ff), BF16),
        pltpu.SemaphoreType.DMA((2,)),
        pltpu.SemaphoreType.DMA((2,)),
        pltpu.SemaphoreType.DMA((1,)),
    )

    units = len(UNITS)

    def phase_two(wv, hv, gc, o3, pb, pp, sb, fb, wl, hvl, pp_s, rs_s, of_s, ol):
        lane = gc.shape[4]

        def blocks(j):
            return ((x + 2 * nx - 1 - j) % nx, (x + 1 + j) % nx), (y, ya)

        def w_loads(k):
            src = wd_ref.at[:, :, pl.ds(pl.multiple_of(colb + k * cw, cw), cw)]
            copies = [pltpu.make_async_copy(src, wv.at[k, S], wl.at[k, S])]
            for q in (A, B, O):
                copies.append(pltpu.make_async_copy(w_ref.at[k, yq[q]], wv.at[k, q], wl.at[k, q]))
            return copies

        def load_w(k):
            for g in range(PIECES):
                wb(k, g).wait_recv()
                wf(k, g).wait_recv()
            for copy in w_loads(k):
                copy.start()

        def h_loads(n, j):
            xs, ys = blocks(j)
            copies = []
            for d in (0, 1):
                for rel in (0, 1):
                    for q in (S, A, B, O):
                        copies.append(pltpu.make_async_copy(
                            h_ref.at[yq[q], xs[d], ys[d], either(rel)], hv.at[n % 2, q, :, 2 * d + rel], hvl.at[n % 2, q, 2 * d + rel]))
            return copies

        def first_use(j):
            minus, plus = (3 - j) % 4, (1 + j) % 4
            hd(BATCH[(minus, A)]).wait_recv()
            hd(BATCH[(plus, S)]).wait_recv()
            hf(BATCH[(minus, O)]).wait_recv()
            hf(BATCH[(plus, B)]).wait_recv()
            xs, ys = blocks(j)
            for d in (0, 1):
                for rel in (0, 1):
                    gate = metav[lin(xs[d], ys[d], either(rel)), 1:2, :]
                    gc[j, :, 2 * d + rel] = jnp.transpose(jnp.broadcast_to(gate, (lane, pairs))).reshape(el, per, lane)

        def partner_copy(n, d):
            return remote(pp.at[n % 2, d], db.at[n % 2, d], pp_s.at[n % 2, d], db_r.at[n % 2, d], dev_p)

        def ring_copy(slot, d, k, j):
            return remote(sb.at[slot, d], rb.at[d, k, j], rs_s.at[slot, d], rs_r.at[d, k, j], (dev_xp, dev_xm)[d])

        def out_copies(slot, k):
            cols = out_ref.at[:, pl.ds(pl.multiple_of(colb + k * cw, cw), cw)]
            return (
                pltpu.make_async_copy(fb.at[slot, 0], cols, ol.at[slot]),
                remote(fb.at[slot, 1], cols, of_s.at[slot], of_r.at[k], dev_a),
            )

        def make(n):
            k, j = look_up([u[0] for u in UNITS], n), look_up([u[1] for u in UNITS], n)
            xs, ys = blocks(j)
            for at in range(units):
                new_chunk = UNITS[at][0] not in [u[0] for u in UNITS[:at]]
                if (at and SEND_MAKE[at]) or new_chunk:
                    @pl.when(n == at)
                    def _(at=at, new_chunk=new_chunk):
                        if at:
                            send(SEND_MAKE[at], load_w)
                        if new_chunk:
                            for copy in w_loads(UNITS[at][0]):
                                copy.wait()
            for copy in h_loads(n, j):
                copy.wait()

            def expert(e, carry):
                o = jnp.zeros((4 * per, cw), F32)
                for q in (S, A, B, O):
                    o = o + jnp.dot(hv[n % 2, q, e].reshape(4 * per, ff), wv[k, q, e], preferred_element_type=F32)
                g = gc[j, e].reshape(4 * per, lane)
                v = o * jnp.concatenate([g] * (cw // lane), axis=1)
                hi = v.astype(BF16)
                rest = v - hi.astype(F32)
                mid = rest.astype(BF16)
                low = (rest - mid.astype(F32)).astype(BF16)
                o3[:, 0, e] = hi.reshape(4, per, cw)
                o3[:, 1, e] = mid.reshape(4, per, cw)
                o3[:, 2, e] = low.reshape(4, per, cw)
                return carry

            lax.fori_loop(0, el, expert, 0)

            @pl.when(n >= 2)
            def _():
                for d in (0, 1):
                    partner_copy(n - 2, d).wait_send()
                pl.semaphore_wait(credit, 1)

            for rel in (1, 0):
                for d in (0, 1):
                    hot = one_hot(lin(xs[d], ys[d], either(rel)))
                    total = jnp.dot(hot, o3[2 * d + rel, 0].reshape(pairs, cw), preferred_element_type=F32)
                    total += jnp.dot(hot, o3[2 * d + rel, 1].reshape(pairs, cw), preferred_element_type=F32)
                    total += jnp.dot(hot, o3[2 * d + rel, 2].reshape(pairs, cw), preferred_element_type=F32)
                    if rel == 1:
                        pp[n % 2, d] = total
                        partner_copy(n, d).start()
                    else:
                        pb[n % 2, d] = total

        def join(n):
            k, j = look_up([u[0] for u in UNITS], n), look_up([u[1] for u in UNITS], n)
            count = look_up([sum(1 for m in SENDS if m < at) for at in range(units)], n)
            slot = count % 4
            for at in range(units):
                if SEND_JOIN[at]:
                    @pl.when(n == at)
                    def _(at=at):
                        send(SEND_JOIN[at], load_w)
            for d in (0, 1):
                partner_copy(n, d).wait_recv()

            @pl.when((j < 3) & (count >= 4))
            def _():
                for d in (0, 1):
                    ring_copy(slot, d, k, 0).wait_send()

            for d in (0, 1):
                @pl.when(j == 0)
                def _():
                    sb[slot, d] = pb[n % 2, d] + db[n % 2, d]

                @pl.when((j > 0) & (j < 3))
                def _():
                    ring_copy(slot, d, k, j - 1).wait_recv()
                    sb[slot, d] = pb[n % 2, d] + db[n % 2, d] + rb[d, k, j - 1]

                @pl.when(j < 3)
                def _():
                    ring_copy(slot, d, k, j).start()

            for order, at in enumerate(FINALS):
                @pl.when(n == at)
                def _(order=order, at=at):
                    kk = UNITS[at][0]
                    if order >= 2:
                        local, away = out_copies(order % 2, kk)
                        local.wait()
                        away.wait_send()
                    for d in (0, 1):
                        ring_copy(0, d, kk, 2).wait_recv()
                        fb[order % 2, d] = (pb[at % 2, d] + db[at % 2, d] + rb[d, kk, 2]).astype(BF16)
                    local, away = out_copies(order % 2, kk)
                    local.start()
                    away.start()

            @pl.when(n < units - 2)
            def _():
                pl.semaphore_signal(credit, inc=1, device_id=dev_p, device_id_type=MESH)

        send([action for action in SEND_END if action[0] == 'lw'], load_w)
        send(SEND_MAKE[0], load_w)
        first_use(UNITS[0][1])
        for copy in h_loads(0, UNITS[0][1]):
            copy.start()
        seen = [int(at + 1 < units and FIRST_STEP[UNITS[at + 1][1]] <= at) for at in range(units)]

        def unit(n, carry):
            @pl.when(n < units)
            def _():
                make(n)

                @pl.when(look_up(seen, n) == 1)
                def _():
                    for copy in h_loads(n + 1, look_up([u[1] for u in UNITS[1:]], n)):
                        copy.start()

            @pl.when(n > 0)
            def _():
                join(n - 1)

            for step, at in FIRST_STEP.items():
                if at > 0:
                    @pl.when(n == at - 1)
                    def _(step=step, at=at):
                        send(SEND_PRE[at], load_w)
                        first_use(step)
                        for copy in h_loads(at, step):
                            copy.start()

            return carry

        lax.fori_loop(0, units + 1, unit, 0)
        for d in (0, 1):
            for n in (units - 2, units - 1):
                partner_copy(n, d).wait_send()
            for slot in range(4):
                ring_copy(slot, d, 0, 0).wait_send()
        for slot in (0, 1):
            local, away = out_copies(slot, 0)
            local.wait()
            away.wait_send()
        for k in range(kc):
            out_copies(0, k)[1].wait_recv()

    lane = min(128, cw)
    send([action for action in SEND_END if action[0] != 'lw'])

    pl.run_scoped(
        phase_two,
        pltpu.VMEM((kc, 4, el, ff, cw), BF16),
        pltpu.VMEM((2, 4, el, 4, per, ff), BF16),
        pltpu.VMEM((4, el, 4, per, lane), F32),
        pltpu.VMEM((4, 3, el, per, cw), BF16),
        pltpu.VMEM((2, 2, rows, cw), F32),
        pltpu.VMEM((2, 2, rows, cw), F32),
        pltpu.VMEM((4, 2, rows, cw), F32),
        pltpu.VMEM((2, 2, rows, cw), BF16),
        pltpu.SemaphoreType.DMA((kc, 4)),
        pltpu.SemaphoreType.DMA((2, 4, 4)),
        pltpu.SemaphoreType.DMA((2, 2)),
        pltpu.SemaphoreType.DMA((4, 2)),
        pltpu.SemaphoreType.DMA((2,)),
        pltpu.SemaphoreType.DMA((2,)),
    )

    def meta_done(d, carry):
        meta_copy(d).wait_send()
        return carry

    lax.fori_loop(1, ny * eps, meta_done, 0)
    for n in range(4):
        ty(n).wait_send()
    for q in (S, A, B, O):
        for n in range(4):
            tx(q, n).wait_send()
        for dxm in range(4):
            td(q, dxm).wait_send()
    for k in range(kc):
        for g in range(PIECES):
            wa(k, g).wait_send()
            wb(k, g).wait_send()
            wf(k, g).wait_send()
    for i in range(16):
        hd(i).wait_send()
        if order_of(i)[1] >= 2:
            hf(i).wait_send()


def solution(mesh):
    ny, eps = mesh.shape['tp'], mesh.shape['ep']
    nx = eps // 2
    row_spec = P(('dp', 'ep', 'tp'), None)
    w_in_spec = P('ep', None, 'tp')
    w_out_spec = P('ep', 'tp', None)

    def local_moe(x, ids, gates, w_gate, w_up, w_down):
        rows, width = x.shape
        el, _, ff = w_gate.shape
        experts = el * eps
        per = rows * ids.shape[1] // experts
        pairs = el * per
        cw = width // 2 // CHUNKS
        position, value = routing_tables(ids, gates, experts, per)
        meta = jnp.stack([position.reshape(eps, pairs), value.reshape(eps, pairs)], axis=1)
        meta = jnp.pad(meta, ((0, 0), (0, 6), (0, 0)))
        hbm = pl.BlockSpec(memory_space=pl.ANY)
        vmem = pl.BlockSpec(memory_space=pltpu.VMEM)
        dma = pltpu.SemaphoreType.DMA
        outs = pl.pallas_call(
            functools.partial(moe_kernel, nx, ny),
            name='moe_kernel',
            out_shape=[
                jax.ShapeDtypeStruct((rows, width), BF16),
                jax.ShapeDtypeStruct((nx, ny, 2, rows, width), BF16),
                jax.ShapeDtypeStruct((ny, nx, ny, 2, el, per, ff), BF16),
                jax.ShapeDtypeStruct((CHUNKS, ny, el, ff, cw), BF16),
            ],
            in_specs=[hbm, vmem, hbm, hbm, hbm],
            out_specs=[hbm] * 4,
            scratch_shapes=[
                pltpu.VMEM((ny * eps, 8, pairs), F32),
                pltpu.VMEM((2, CHUNKS, 3, rows, cw), F32),
                pltpu.VMEM((2, 2, rows, cw), F32),
                dma((ny * eps,)), dma((ny * eps,)),
                dma((4,)), dma((4,)),
                dma((4, 4)), dma((4, 4)),
                dma((4, 4)), dma((4, 4)),
                dma((16,)), dma((16,)), dma((16,)), dma((16,)),
            ] + [dma((CHUNKS, PIECES))] * 6 + [
                dma((2, CHUNKS, 3)), dma((2, 2)), dma((CHUNKS,)),
                pltpu.SemaphoreType.REGULAR,
            ],
            compiler_params=pltpu.CompilerParams(collective_id=0, has_side_effects=True, vmem_limit_bytes=67 * 1000 * 1000),
        )(x, meta, jnp.transpose(w_gate, (0, 2, 1)), jnp.transpose(w_up, (0, 2, 1)), w_down)
        return outs[0]

    return jax.shard_map(
        local_moe, mesh=mesh, in_specs=(row_spec, row_spec, row_spec, w_in_spec, w_in_spec, w_out_spec),
        out_specs=row_spec, check_vma=False)
```

```python
import functools

import jax
import jax.numpy as jnp
from jax import lax
from jax.experimental import pallas as pl
from jax.experimental.pallas import tpu as pltpu
from jax.sharding import PartitionSpec as P

MESH = pl.DeviceIdType.MESH
CHUNKS = 4
LANES = 256
PIECES = 2
BF16 = jnp.bfloat16
F32 = jnp.float32

S, A, B, O = 0, 1, 2, 3

UNITS = ((2, 0), (1, 0), (0, 0), (2, 1), (0, 1), (1, 1), (0, 2), (3, 0), (1, 2), (3, 1), (2, 2), (1, 3), (3, 2), (0, 3), (2, 3), (3, 3), )
ORDER = ((0, 0), (0, 1), (1, 0), (0, 2), (1, 1), (1, 2), (0, 3), (0, 4), (1, 3), (1, 4), (0, 5), (0, 6), (1, 5), (1, 6), (0, 7), (0, 8), (1, 7), (0, 9), (1, 8), (0, 10), (1, 9), (1, 10), (0, 11), (0, 12), (1, 11), (0, 13), (1, 12), (0, 14), (1, 13), (0, 15), (1, 14), (1, 15), )
OPPOSITE_VIA_A = 4
OPPOSITE = (2,)
SEND_START = (('wa', 1, 1), ('wb', 3, 1), ('wb', 1, 0), )
SEND_BEFORE = (
    (),
    (),
    (('hd', 1), ('wa', 2, 0), ('wa', 0, 1), ('wa', 2, 1), ('wa', 3, 0), ('wa', 1, 0), ('wa', 0, 0), ('wf', 1, 1), ('wb', 2, 0), ('wb', 0, 0), ('wb', 0, 1), ('wb', 1, 1), ('wb', 2, 1), ),
    (),
    (),
    (),
    (),
    (('wf', 2, 0), ),
    (),
    (('hd', 8), ('hd', 7), ('wf', 0, 1), ),
    (),
    (('hf', 8), ('wa', 3, 1), ('hd', 5), ('wf', 1, 0), ),
    (('hd', 11), ('hd', 10), ('wf', 0, 0), ('wf', 2, 1), ),
    (('hd', 12), ('hf', 7), ),
    (('hf', 11), ('hd', 13), ),
    (('hf', 10), ('hd', 14), ),
)
SEND_AFTER = (
    (),
    (),
    (),
    (),
    (),
    (),
    (),
    (),
    (),
    (),
    (),
    (),
    (),
    (),
    (),
    (),
)
SEND_END = (('hd', 15), ('wf', 3, 1), ('hd', 9), ('wf', 3, 0), ('wb', 3, 0), ('hd', 6), ('lw', 0), ('lw', 1), ('lw', 2), )
SEND_MAKE = (
    (),
    (('hf', 14), ),
    (),
    (),
    (),
    (),
    (),
    (('lw', 3), ),
    (),
    (),
    (),
    (),
    (),
    (),
    (),
    (),
)
SEND_JOIN = (
    (),
    (('hf', 15), ('hd', 2), ('hd', 4), ('hd', 0), ('hd', 3), ),
    (),
    (('hf', 9), ),
    (),
    (),
    (),
    (('hf', 6), ),
    (),
    (),
    (),
    (),
    (),
    (),
    (),
    (),
)


def order_of(i):
    last, r = i // 12, i % 3
    return (1 - last) * (r + r // 2) + 2 * last, (1 - last) * (i // 3) + last * (i - 12)


BATCH = {order_of(i): i for i in range(16)}
FIRST_STEP = {}
for place_in_order, (chunk_of, step_of) in enumerate(UNITS):
    FIRST_STEP.setdefault(step_of, place_in_order)
SENDS = [n for n, (_, j) in enumerate(UNITS) if j < 3]
FINALS = [n for n, (_, j) in enumerate(UNITS) if j == 3]


def place(y, q):
    high, low = y // 2, y % 2
    return 2 * ((high + q // 2) % 2) + (low + (q + 1) // 2) % 2


def look_up(table, n):
    value = jnp.int32(table[0])
    for at in range(1, len(table)):
        if table[at] != table[0]:
            value = jnp.where(n == at, table[at], value)
    return value


def routing_tables(ids, gates, experts, per_expert):
    rows = ids.shape[0]
    chosen = ids[:, :, None] == jnp.arange(experts, dtype=ids.dtype)
    picked = jnp.any(chosen, axis=1)
    weight = jnp.sum(jnp.where(chosen, gates[:, :, None], 0.0), axis=1)
    before = (jnp.arange(rows)[:, None] > jnp.arange(rows)[None, :]).astype(BF16)
    rank = jnp.dot(before, picked.astype(BF16), preferred_element_type=F32)
    rank = jnp.where(picked, rank, -1.0)
    hit = rank[:, :, None] == jnp.arange(per_expert, dtype=F32)
    row = jnp.arange(rows, dtype=F32)[:, None, None]
    position = jnp.sum(jnp.where(hit, row, 0.0), axis=0)
    value = jnp.sum(jnp.where(hit, weight[:, :, None], 0.0), axis=0)
    return position, value


def moe_kernel(nx, ny, x_ref, meta_ref, wg_ref, wu_ref, wd_ref, out_ref, tok_ref, h_ref, w_ref,
               metav, rb, db, ms, mr, ty_s, ty_r, tx_s, tx_r, td_s, td_r, hd_s, hd_r, hf_s, hf_r,
               wa_s, wa_r, wb_s, wb_r, wf_s, wf_r, rs_r, db_r, of_r, credit):
    rows, width = x_ref.shape
    half = rows // 2
    el, ff, _ = wg_ref.shape
    per = h_ref.shape[5]
    rest = ff - LANES * (ff // LANES)
    whole = el * (ff // LANES)
    assert ff // LANES == 1 and (el * rest) % LANES == 0 and rest <= 128
    pairs = el * per
    kc, cw = w_ref.shape[0], w_ref.shape[4]
    ep_piece = el // PIECES
    eps = 2 * nx
    y = lax.axis_index('tp')
    ep = lax.axis_index('ep')
    x, c = ep // 2, ep % 2
    ya, yb, yo = place(y, A), place(y, B), place(y, O)
    yq = (y, ya, yb, yo)
    xp, xm = (x + 1) % nx, (x + nx - 1) % nx
    colb = ((y + y // 2) % 2) * (kc * cw)
    cola = ((ya + ya // 2) % 2) * (kc * cw)
    me = y * eps + ep

    dev_a = {'tp': ya, 'ep': ep}
    dev_b = {'tp': yb, 'ep': ep}
    dev_p = {'tp': y, 'ep': 2 * x + 1 - c}
    dev_xp = {'tp': y, 'ep': 2 * xp + c}
    dev_xm = {'tp': y, 'ep': 2 * xm + c}

    def remote(src, dst, send, recv, dev):
        return pltpu.make_async_remote_copy(src_ref=src, dst_ref=dst, send_sem=send, recv_sem=recv, device_id=dev, device_id_type=MESH)

    def lin(xs, ys, cs):
        return ys * eps + 2 * xs + cs

    def either(rel):
        return c if rel == 0 else 1 - c

    barrier = pltpu.get_barrier_semaphore()

    def peer_of(d):
        other = (me + d) % (ny * eps)
        return other // eps, other % eps

    def greet(d, carry):
        py, pe = peer_of(d)
        pl.semaphore_signal(barrier, inc=1, device_id={'tp': py, 'ep': pe}, device_id_type=MESH)
        return carry

    lax.fori_loop(1, ny * eps, greet, 0)
    pl.semaphore_wait(barrier, ny * eps - 1)

    def meta_copy(d):
        py, pe = peer_of(d)
        return remote(meta_ref.at[pe], metav.at[me], ms.at[d], mr.at[me], {'tp': py, 'ep': pe})

    def meta_send(d, carry):
        meta_copy(d).start()
        return carry

    lax.fori_loop(1, ny * eps, meta_send, 0)
    metav[me] = meta_ref[ep]

    def own(dxm, q):
        return tok_ref.at[(x + dxm) % nx, yq[q], c]

    def rows_of(ref, part, cut=None):
        cut = half if cut is None else cut
        return ref.at[pl.ds(part * cut, (cut, rows - cut)[part])]

    def ty(n):
        if n < 2:
            return remote(x_ref, tok_ref.at[x, y, c], ty_s.at[n], ty_r.at[n], (dev_a, dev_b)[n])
        block = rows_of(own(0, (B, A)[n - 2]), n - 2, rows * OPPOSITE_VIA_A // 4)
        return remote(block, block, ty_s.at[n], ty_r.at[n], (dev_a, dev_b)[n - 2])

    def tx(q, n):
        if n < 2:
            return remote(x_ref if q == S else own(0, q), own(0, q), tx_s.at[q, n], tx_r.at[q, n], (dev_xp, dev_xm)[n])
        block = rows_of(own((3, 1)[n - 2], q), n - 2)
        return remote(block, block, tx_s.at[q, n], tx_r.at[q, n], (dev_xp, dev_xm)[n - 2])

    def td(q, dxm):
        return remote(x_ref if (q == S and dxm == 0) else own(dxm, q), own(dxm, q), td_s.at[q, dxm], td_r.at[q, dxm], dev_p)

    def wa(k, g):
        src = wd_ref.at[pl.ds(g * ep_piece, ep_piece), :, pl.ds(pl.multiple_of(cola + k * cw, cw), cw)]
        return remote(src, w_ref.at[k, y, pl.ds(g * ep_piece, ep_piece)], wa_s.at[k, g], wa_r.at[k, g], dev_a)

    def wb(k, g):
        src = wd_ref.at[pl.ds(g * ep_piece, ep_piece), :, pl.ds(pl.multiple_of(colb + k * cw, cw), cw)]
        return remote(src, w_ref.at[k, y, pl.ds(g * ep_piece, ep_piece)], wb_s.at[k, g], wb_r.at[k, g], dev_b)

    def wf(k, g):
        block = w_ref.at[k, ya, pl.ds(g * ep_piece, ep_piece)]
        return remote(block, block, wf_s.at[k, g], wf_r.at[k, g], dev_b)

    def hd(i):
        dxm, q = order_of(i)
        block = h_ref.at[y, (x + dxm) % nx, yq[q]]
        return remote(block, block, hd_s.at[i], hd_r.at[i], dev_a if q < 2 else dev_b)

    def hf(i):
        dxm, q = order_of(i)
        block = h_ref.at[yb, (x + dxm) % nx, place(yb, q)]
        return remote(block, block, hf_s.at[i], hf_r.at[i], dev_a)

    def send(actions, load_w=None):
        for action in actions:
            kind, at = action[0], action[1:]
            if kind == 'wf':
                wa(*at).wait_recv()
            if kind == 'hf':
                hd(*at).wait_recv()
            if kind == 'lw':
                load_w(*at)
            else:
                {'wa': wa, 'wb': wb, 'wf': wf, 'hd': hd, 'hf': hf}[kind](*at).start()

    for n in (0, 1):
        ty(n).start()
        tx(S, n).start()
    td(S, 0).start()
    send(SEND_START)

    def came(q):
        for n in (0, 1):
            tx(q, n).wait_recv()
        td(q, 1).start()
        td(q, 3).start()

    def both(q, first):
        tx(q, first).start()
        tx(q, first + 1).start()

    def comm(step):
        if step == 1:
            ty(0).wait_recv()
            ty(1).wait_recv()
            for n in OPPOSITE:
                ty(n).start()
            both(A, 0)
            both(B, 0)
            came(S)
            td(A, 0).start()
            td(B, 0).start()
        if step == 4:
            came(A)
            for n in OPPOSITE:
                ty(n).wait_recv()
            both(O, 0)
            both(S, 2)
            both(A, 2)
            td(O, 0).start()
        if step in (7, 10):
            q = {7: B, 10: O}[step]
            came(q)
            both(q, 2)
        if step >= 12:
            tx(step - 12, 2).wait_recv()
            tx(step - 12, 3).wait_recv()
            td(step - 12, 2).start()

    row_id = lax.broadcasted_iota(jnp.int32, (rows, pairs), 0)

    def one_hot(src):
        pos = metav[src, 0:1, :].astype(jnp.int32)
        return (row_id == pos).astype(F32).astype(BF16)

    def meta_wait(src):
        remote(meta_ref.at[0], metav.at[src], ms.at[0], mr.at[src], dev_p).wait_recv()

    def phase_one(wg, wu, tb, xg, hb, left, wl, tl, hl):
        load_g = pltpu.make_async_copy(wg_ref, wg, wl.at[0])
        load_u = pltpu.make_async_copy(wu_ref, wu, wl.at[1])
        load_g.start()
        load_u.start()

        def store(i):
            dxm, q = order_of(i)
            return pltpu.make_async_copy(hb, h_ref.at[y, (x + dxm) % nx, place(y, q)], hl.at[0])

        def batch(i, carry):
            @pl.when(i > 0)
            def _():
                store(i - 1).wait()

            for step in range(1, 16):
                if SEND_BEFORE[step] or SEND_AFTER[step] or step in (1, 4, 7, 10) or step >= 12:
                    @pl.when(i == step)
                    def _(step=step):
                        send(SEND_BEFORE[step])
                        comm(step)
                        send(SEND_AFTER[step])

            dxm, q = order_of(i)
            xs, ys = (x + dxm) % nx, place(y, q)
            mine = pltpu.make_async_copy(x_ref, tb.at[0], tl.at[0])
            other = pltpu.make_async_copy(tok_ref.at[xs, ys, c], tb.at[0], tl.at[0])
            theirs = pltpu.make_async_copy(tok_ref.at[xs, ys, 1 - c], tb.at[1], tl.at[1])

            @pl.when(i == 0)
            def _():
                mine.start()

            @pl.when(i > 0)
            def _():
                other.start()
                meta_wait(lin(xs, ys, c))

            remote(tok_ref.at[xs, ys, c], tok_ref.at[xs, ys, c], td_s.at[q, dxm], td_r.at[q, dxm], dev_p).wait_recv()
            theirs.start()
            meta_wait(lin(xs, ys, 1 - c))
            for s in (0, 1):
                (other, theirs)[s].wait()
                hot = one_hot(lin(xs, ys, either(s)))
                step = min(512, width)
                for lo in range(0, width, step):
                    got = lax.dot_general(hot, tb[s, :, lo:lo + step], (((0,), (0,)), ((), ())), preferred_element_type=F32)
                    xg[:, s, :, lo:lo + step] = got.astype(BF16).reshape(el, per, step)

            @pl.when(i == 0)
            def _():
                load_g.wait()
                load_u.wait()

            for e in range(el):
                lhs = xg[e].reshape(2 * per, width)
                a = lax.dot_general(lhs, wg[e], (((1,), (1,)), ((), ())), preferred_element_type=F32)
                b = lax.dot_general(lhs, wu[e], (((1,), (1,)), ((), ())), preferred_element_type=F32)
                hid = a * jax.nn.sigmoid(a) * b
                for s in (0, 1):
                    hb[either(s), e] = hid[s * per:(s + 1) * per, :LANES].astype(BF16)
                left[e] = hid[:, LANES:]
            packed = jnp.concatenate([left[e] for e in range(el)], axis=1).astype(BF16)
            for m in range(el * rest // LANES):
                for s in (0, 1):
                    hb[either(s), whole + m] = packed[s * per:(s + 1) * per, m * LANES:(m + 1) * LANES]
            store(i).start()
            return carry

        lax.fori_loop(0, 16, batch, 0)
        store(15).wait()

    pl.run_scoped(
        phase_one,
        pltpu.VMEM((el, ff, width), BF16),
        pltpu.VMEM((el, ff, width), BF16),
        pltpu.VMEM((2, rows, width), BF16),
        pltpu.VMEM((el, 2, per, width), BF16),
        pltpu.VMEM((2,) + h_ref.shape[4:], BF16),
        pltpu.VMEM((el, 2 * per, rest), F32),
        pltpu.SemaphoreType.DMA((2,)),
        pltpu.SemaphoreType.DMA((2,)),
        pltpu.SemaphoreType.DMA((1,)),
    )

    def window(e):
        return e * rest // 128 * 128, -(-(e + 1) * rest // 128) * 128

    def offset(e, q):
        before = sum(LANES + window(m)[1] - window(m)[0] for m in range(e))
        return 4 * before + q * (LANES + window(e)[1] - window(e)[0])

    deep = offset(el, S)

    units = len(UNITS)

    def phase_two(wv, hv, gc, o3, pb, pp, sb, fb, wl, hvl, pp_s, rs_s, of_s, ol):
        lane = gc.shape[3]

        def clear(i, carry):
            wv[i // 8, pl.ds(pl.multiple_of(i % 8 * (deep // 8), 16), deep // 8)] = jnp.zeros((deep // 8, cw), BF16)
            return carry

        lax.fori_loop(0, 8 * kc, clear, 0)

        def blocks(j):
            return ((x + 2 * nx - 1 - j) % nx, (x + 1 + j) % nx), (y, ya)

        def w_loads(k):
            copies = []
            for q in (S, A, B, O):
                for e in range(el):
                    if q == S:
                        src = wd_ref.at[e, :, pl.ds(pl.multiple_of(colb + k * cw, cw), cw)]
                    else:
                        src = w_ref.at[k, yq[q], e]
                    low, high = window(e)
                    at = offset(e, q)
                    copies.append(pltpu.make_async_copy(src.at[pl.ds(0, LANES)], wv.at[k, pl.ds(at, LANES)], wl.at[k]))
                    copies.append(pltpu.make_async_copy(
                        src.at[pl.ds(LANES, rest)], wv.at[k, pl.ds(at + LANES + e * rest - low, rest)], wl.at[k]))
            return copies

        def load_w(k):
            for g in range(PIECES):
                wb(k, g).wait_recv()
                wf(k, g).wait_recv()
            for copy in w_loads(k):
                copy.start()

        def h_loads(n, j):
            xs, ys = blocks(j)
            copies = []
            for d in (0, 1):
                for rel in (0, 1):
                    for q in (S, A, B, O):
                        copies.append(pltpu.make_async_copy(
                            h_ref.at[yq[q], xs[d], ys[d], either(rel)], hv.at[n % 2, q, :, 2 * d + rel], hvl.at[n % 2, q, 2 * d + rel]))
            return copies

        def first_use(j):
            minus, plus = (3 - j) % 4, (1 + j) % 4
            hd(BATCH[(minus, A)]).wait_recv()
            hd(BATCH[(plus, S)]).wait_recv()
            hf(BATCH[(minus, O)]).wait_recv()
            hf(BATCH[(plus, B)]).wait_recv()

        def partner_copy(n, d):
            return remote(pp.at[n % 2, d], db.at[n % 2, d], pp_s.at[n % 2, d], db_r.at[n % 2, d], dev_p)

        def ring_copy(slot, d, k, j):
            return remote(sb.at[slot, d], rb.at[d, k, j], rs_s.at[slot, d], rs_r.at[d, k, j], (dev_xp, dev_xm)[d])

        def out_copies(slot, k):
            cols = out_ref.at[:, pl.ds(pl.multiple_of(colb + k * cw, cw), cw)]
            return (
                pltpu.make_async_copy(fb.at[slot, 0], cols, ol.at[slot]),
                remote(fb.at[slot, 1], cols, of_s.at[slot], of_r.at[k], dev_a),
            )

        def make(n):
            k, j = look_up([u[0] for u in UNITS], n), look_up([u[1] for u in UNITS], n)
            xs, ys = blocks(j)
            for at in range(units):
                new_chunk = UNITS[at][0] not in [u[0] for u in UNITS[:at]]
                first = at in FIRST_STEP.values()
                if (not first and SEND_MAKE[at]) or new_chunk:
                    @pl.when(n == at)
                    def _(at=at, new_chunk=new_chunk, first=first):
                        if not first:
                            send(SEND_MAKE[at], load_w)
                        if new_chunk:
                            pltpu.make_async_copy(w_ref.at[UNITS[at][0]], w_ref.at[UNITS[at][0]], wl.at[UNITS[at][0]]).wait()
            for d in (0, 1):
                for rel in (0, 1):
                    gate = metav[lin(xs[d], ys[d], either(rel)), 1:2, :]
                    gc[:, 2 * d + rel] = jnp.transpose(jnp.broadcast_to(gate, (lane, pairs))).reshape(el, per, lane)
            for copy in h_loads(n, j):
                copy.wait()

            for e in range(el):
                low, high = window(e)
                parts = []
                for q in (S, A, B, O):
                    parts.append(hv[n % 2, q, e].reshape(4 * per, LANES))
                    for at in range(low, high, 128):
                        parts.append(hv[n % 2, q, whole + at // LANES, :, :, at % LANES:at % LANES + 128].reshape(4 * per, 128))
                size = 4 * (LANES + high - low)
                o = jnp.dot(jnp.concatenate(parts, axis=1), wv[k, offset(e, S):offset(e, S) + size], preferred_element_type=F32)
                g = gc[e].reshape(4 * per, lane)
                v = o * jnp.concatenate([g] * (cw // lane), axis=1)
                hi = v.astype(BF16)
                over = v - hi.astype(F32)
                mid = over.astype(BF16)
                low_part = (over - mid.astype(F32)).astype(BF16)
                o3[:, 0, e] = hi.reshape(4, per, cw)
                o3[:, 1, e] = mid.reshape(4, per, cw)
                o3[:, 2, e] = low_part.reshape(4, per, cw)

            @pl.when(n >= 2)
            def _():
                for d in (0, 1):
                    partner_copy(n - 2, d).wait_send()
                pl.semaphore_wait(credit, 1)

            for rel in (1, 0):
                for d in (0, 1):
                    hot = one_hot(lin(xs[d], ys[d], either(rel)))
                    total = jnp.dot(hot, o3[2 * d + rel, 0].reshape(pairs, cw), preferred_element_type=F32)
                    total += jnp.dot(hot, o3[2 * d + rel, 1].reshape(pairs, cw), preferred_element_type=F32)
                    total += jnp.dot(hot, o3[2 * d + rel, 2].reshape(pairs, cw), preferred_element_type=F32)
                    if rel == 1:
                        pp[n % 2, d] = total
                        partner_copy(n, d).start()
                    else:
                        pb[n % 2, d] = total

        def join(n):
            k, j = look_up([u[0] for u in UNITS], n), look_up([u[1] for u in UNITS], n)
            count = look_up([sum(1 for m in SENDS if m < at) for at in range(units)], n)
            slot = count % 4
            for at in range(units):
                if SEND_JOIN[at]:
                    @pl.when(n == at)
                    def _(at=at):
                        send(SEND_JOIN[at], load_w)
            for d in (0, 1):
                partner_copy(n, d).wait_recv()

            @pl.when((j < 3) & (count >= 4))
            def _():
                for d in (0, 1):
                    ring_copy(slot, d, k, 0).wait_send()

            for d in (0, 1):
                @pl.when(j == 0)
                def _():
                    sb[slot, d] = pb[n % 2, d] + db[n % 2, d]

                @pl.when((j > 0) & (j < 3))
                def _():
                    ring_copy(slot, d, k, j - 1).wait_recv()
                    sb[slot, d] = pb[n % 2, d] + db[n % 2, d] + rb[d, k, j - 1]

                @pl.when(j < 3)
                def _():
                    ring_copy(slot, d, k, j).start()

            for order, at in enumerate(FINALS):
                @pl.when(n == at)
                def _(order=order, at=at):
                    kk = UNITS[at][0]
                    if order >= 2:
                        local, away = out_copies(order % 2, kk)
                        local.wait()
                        away.wait_send()
                    for d in (0, 1):
                        ring_copy(0, d, kk, 2).wait_recv()
                        fb[order % 2, d] = (pb[at % 2, d] + db[at % 2, d] + rb[d, kk, 2]).astype(BF16)
                    local, away = out_copies(order % 2, kk)
                    local.start()
                    away.start()

            @pl.when(n < units - 2)
            def _():
                pl.semaphore_signal(credit, inc=1, device_id=dev_p, device_id_type=MESH)

        send([action for action in SEND_END if action[0] == 'lw'], load_w)
        send(SEND_MAKE[0], load_w)
        first_use(UNITS[0][1])
        for copy in h_loads(0, UNITS[0][1]):
            copy.start()
        seen = [int(at + 1 < units and FIRST_STEP[UNITS[at + 1][1]] <= at) for at in range(units)]

        def operation(at, carry):
            n = look_up([o[1] for o in ORDER], at)

            @pl.when(look_up([o[0] for o in ORDER], at) == 0)
            def _():
                for step, first in FIRST_STEP.items():
                    if first > 0:
                        @pl.when(n == first)
                        def _(step=step, first=first):
                            send(SEND_MAKE[first], load_w)
                            first_use(step)
                            for copy in h_loads(first, step):
                                copy.start()

                make(n)

                @pl.when(look_up(seen, n) == 1)
                def _():
                    for copy in h_loads(n + 1, look_up([u[1] for u in UNITS[1:]], n)):
                        copy.start()

            @pl.when(look_up([o[0] for o in ORDER], at) == 1)
            def _():
                join(n)

            return carry

        lax.fori_loop(0, len(ORDER), operation, 0)
        for d in (0, 1):
            for n in (units - 2, units - 1):
                partner_copy(n, d).wait_send()
            for slot in range(4):
                ring_copy(slot, d, 0, 0).wait_send()
        for slot in (0, 1):
            local, away = out_copies(slot, 0)
            local.wait()
            away.wait_send()
        for k in range(kc):
            out_copies(0, k)[1].wait_recv()

    lane = min(128, cw)
    send([action for action in SEND_END if action[0] != 'lw'])

    pl.run_scoped(
        phase_two,
        pltpu.VMEM((kc, deep, cw), BF16),
        pltpu.VMEM((2, 4, h_ref.shape[4], 4, per, LANES), BF16),
        pltpu.VMEM((el, 4, per, lane), F32),
        pltpu.VMEM((4, 3, el, per, cw), BF16),
        pltpu.VMEM((2, 2, rows, cw), F32),
        pltpu.VMEM((2, 2, rows, cw), F32),
        pltpu.VMEM((4, 2, rows, cw), F32),
        pltpu.VMEM((2, 2, rows, cw), BF16),
        pltpu.SemaphoreType.DMA((kc,)),
        pltpu.SemaphoreType.DMA((2, 4, 4)),
        pltpu.SemaphoreType.DMA((2, 2)),
        pltpu.SemaphoreType.DMA((4, 2)),
        pltpu.SemaphoreType.DMA((2,)),
        pltpu.SemaphoreType.DMA((2,)),
    )

    def meta_done(d, carry):
        meta_copy(d).wait_send()
        return carry

    lax.fori_loop(1, ny * eps, meta_done, 0)
    for n in (0, 1) + OPPOSITE:
        ty(n).wait_send()
    for q in (S, A, B, O):
        for n in range(4):
            tx(q, n).wait_send()
        for dxm in range(4):
            td(q, dxm).wait_send()
    for k in range(kc):
        for g in range(PIECES):
            wa(k, g).wait_send()
            wb(k, g).wait_send()
            wf(k, g).wait_send()
    for i in range(16):
        hd(i).wait_send()
        if order_of(i)[1] >= 2:
            hf(i).wait_send()


def solution(mesh):
    ny, eps = mesh.shape['tp'], mesh.shape['ep']
    nx = eps // 2
    row_spec = P(('dp', 'ep', 'tp'), None)
    w_in_spec = P('ep', None, 'tp')
    w_out_spec = P('ep', 'tp', None)

    def local_moe(x, ids, gates, w_gate, w_up, w_down):
        rows, width = x.shape
        el, _, ff = w_gate.shape
        experts = el * eps
        per = rows * ids.shape[1] // experts
        pairs = el * per
        cw = width // 2 // CHUNKS
        position, value = routing_tables(ids, gates, experts, per)
        meta = jnp.stack([position.reshape(eps, pairs), value.reshape(eps, pairs)], axis=1)
        meta = jnp.pad(meta, ((0, 0), (0, 6), (0, 0)))
        hbm = pl.BlockSpec(memory_space=pl.ANY)
        vmem = pl.BlockSpec(memory_space=pltpu.VMEM)
        dma = pltpu.SemaphoreType.DMA
        outs = pl.pallas_call(
            functools.partial(moe_kernel, nx, ny),
            name='moe_kernel',
            out_shape=[
                jax.ShapeDtypeStruct((rows, width), BF16),
                jax.ShapeDtypeStruct((nx, ny, 2, rows, width), BF16),
                jax.ShapeDtypeStruct((ny, nx, ny, 2, el * ff // LANES, per, LANES), BF16),
                jax.ShapeDtypeStruct((CHUNKS, ny, el, ff, cw), BF16),
            ],
            in_specs=[hbm, vmem, hbm, hbm, hbm],
            out_specs=[hbm] * 4,
            scratch_shapes=[
                pltpu.VMEM((ny * eps, 8, pairs), F32),
                pltpu.VMEM((2, CHUNKS, 3, rows, cw), F32),
                pltpu.VMEM((2, 2, rows, cw), F32),
                dma((ny * eps,)), dma((ny * eps,)),
                dma((4,)), dma((4,)),
                dma((4, 4)), dma((4, 4)),
                dma((4, 4)), dma((4, 4)),
                dma((16,)), dma((16,)), dma((16,)), dma((16,)),
            ] + [dma((CHUNKS, PIECES))] * 6 + [
                dma((2, CHUNKS, 3)), dma((2, 2)), dma((CHUNKS,)),
                pltpu.SemaphoreType.REGULAR,
            ],
            compiler_params=pltpu.CompilerParams(collective_id=0, has_side_effects=True, vmem_limit_bytes=67 * 1000 * 1000),
        )(x, meta, jnp.transpose(w_gate, (0, 2, 1)), jnp.transpose(w_up, (0, 2, 1)), w_down)
        return outs[0]

    return jax.shard_map(
        local_moe, mesh=mesh, in_specs=(row_spec, row_spec, row_spec, w_in_spec, w_in_spec, w_out_spec),
        out_specs=row_spec, check_vma=False)
```

```python
import functools

import jax
import jax.numpy as jnp
from jax import lax
from jax.experimental import pallas as pl
from jax.experimental.pallas import tpu as pltpu
from jax.sharding import PartitionSpec as P

MESH = pl.DeviceIdType.MESH
CHUNKS = 4
LANES = 256
PIECES = 2
BF16 = jnp.bfloat16
F32 = jnp.float32

S, A, B, O = 0, 1, 2, 3

UNITS = ((1, 0), (2, 0), (0, 0), (1, 1), (0, 1), (2, 1), (1, 2), (3, 0), (2, 2), (3, 1), (0, 2), (1, 3), (3, 2), (2, 3), (0, 3), (3, 3), )
ORDER = ((0, 0), (0, 1), (1, 0), (0, 2), (1, 1), (1, 2), (0, 3), (0, 4), (1, 3), (0, 5), (1, 4), (0, 6), (1, 5), (1, 6), (0, 7), (0, 8), (1, 7), (0, 9), (1, 8), (0, 10), (1, 9), (0, 11), (1, 10), (0, 12), (1, 11), (0, 13), (1, 12), (0, 14), (1, 13), (0, 15), (1, 14), (1, 15), )
OPPOSITE_VIA_A = 3
OPPOSITE = (2, 3)
SEND_START = (('wa', 1, 0), ('wb', 2, 1), ('wb', 0, 1), ('wb', 2, 0), )
SEND_BEFORE = (
    (),
    (),
    (('hd', 1, 1), ('wf', 1, 0), ('wb', 1, 0), ('wb', 1, 1), ),
    (('hd', 2, 0), ('wa', 0, 1), ('wa', 2, 1), ('wa', 2, 0), ('wa', 0, 0), ('wa', 1, 1), ('wa', 3, 0), ('wa', 3, 1), ),
    (),
    (),
    (('hd', 5, 1), ('hd', 1, 0), ('wf', 0, 1), ),
    (),
    (('hd', 7, 0), ('hd', 7, 1), ),
    (('hd', 8, 0), ('hd', 8, 1), ('wf', 2, 1), ('wf', 2, 0), ),
    (),
    (('hf', 8, 1), ('hf', 7, 1), ('hd', 5, 0), ('hf', 7, 0), ('hf', 8, 0), ('hd', 10, 1), ('hd', 10, 0), ),
    (('hd', 11, 0), ('hd', 11, 1), ('wf', 0, 0), ('wf', 1, 1), ('wb', 0, 0), ),
    (),
    (('hf', 11, 0), ('hd', 12, 0), ('hf', 10, 0), ('hf', 11, 1), ('hd', 13, 1), ('hd', 12, 1), ('hd', 13, 0), ('hf', 10, 1), ),
    (('hd', 14, 0), ('hd', 14, 1), ),
)
SEND_AFTER = (
    (),
    (),
    (),
    (),
    (),
    (),
    (),
    (),
    (),
    (),
    (),
    (),
    (),
    (),
    (),
    (),
)
SEND_END = (('hf', 14, 0), ('hd', 15, 1), ('hd', 15, 0), ('wf', 3, 1), ('wf', 3, 0), ('wb', 3, 1), ('wb', 3, 0), ('hd', 6, 0), ('hd', 9, 1), ('hd', 6, 1), ('hd', 9, 0), ('lw', 0), ('lw', 1), ('lw', 2), )
SEND_MAKE = (
    (),
    (('hf', 14, 1), ),
    (),
    (),
    (),
    (),
    (),
    (('lw', 3), ),
    (('hf', 6, 0), ),
    (),
    (),
    (),
    (),
    (),
    (),
    (),
)
SEND_JOIN = (
    (('hf', 15, 1), ),
    (('hf', 15, 0), ('hd', 4, 0), ('hd', 2, 1), ('hd', 3, 0), ('hd', 0, 0), ('hd', 4, 1), ('hd', 0, 1), ('hd', 3, 1), ),
    (),
    (),
    (),
    (),
    (),
    (('hf', 9, 1), ),
    (('hf', 6, 1), ),
    (('hf', 9, 0), ),
    (),
    (),
    (),
    (),
    (),
    (),
)


def order_of(i):
    last, r = i // 12, i % 3
    return (1 - last) * (r + r // 2) + 2 * last, (1 - last) * (i // 3) + last * (i - 12)


BATCH = {order_of(i): i for i in range(16)}
FIRST_STEP = {}
for place_in_order, (chunk_of, step_of) in enumerate(UNITS):
    FIRST_STEP.setdefault(step_of, place_in_order)
SENDS = [n for n, (_, j) in enumerate(UNITS) if j < 3]
FINALS = [n for n, (_, j) in enumerate(UNITS) if j == 3]


def place(y, q):
    high, low = y // 2, y % 2
    return 2 * ((high + q // 2) % 2) + (low + (q + 1) // 2) % 2


def look_up(table, n):
    value = jnp.int32(table[0])
    for at in range(1, len(table)):
        if table[at] != table[0]:
            value = jnp.where(n == at, table[at], value)
    return value


def routing_tables(ids_ref, gate_ref, meta_ref, slot_ref, weight_ref, per):
    top, rows = ids_ref.shape
    experts = slot_ref.shape[0]
    devices, _, pairs = meta_ref.shape
    group = experts // devices
    expert = lax.broadcasted_iota(jnp.int32, (experts, rows), 0)
    chosen = jnp.zeros((experts, rows), F32)
    weight = jnp.zeros((experts, rows), F32)
    for j in range(top):
        here = expert == ids_ref[j:j + 1, :]
        chosen = jnp.where(here, 1.0, chosen)
        weight = jnp.where(here, gate_ref[j:j + 1, :], weight)
    earlier = lax.broadcasted_iota(jnp.int32, (rows, rows), 0) < lax.broadcasted_iota(jnp.int32, (rows, rows), 1)
    rank = jnp.dot(chosen.astype(BF16), earlier.astype(F32).astype(BF16), preferred_element_type=F32)
    slot_ref[...] = jnp.where(chosen > 0.0, rank, -1.0)
    weight_ref[...] = weight
    lane = lax.broadcasted_iota(jnp.int32, (group, pairs), 1)
    sub = lax.broadcasted_iota(jnp.int32, (group, pairs), 0)
    mine = ((lane >= sub * per) & (lane < (sub + 1) * per)).astype(F32).astype(BF16)
    place_in_expert = lax.broadcasted_iota(jnp.int32, (rows, pairs), 1)
    for m in range(1, group):
        place_in_expert = jnp.where(lax.broadcasted_iota(jnp.int32, (rows, pairs), 1) >= m * per,
                                    lax.broadcasted_iota(jnp.int32, (rows, pairs), 1) - m * per, place_in_expert)
    place_in_expert = place_in_expert.astype(F32)
    row = lax.broadcasted_iota(jnp.int32, (8, rows), 1)
    high = (row // 2).astype(F32).astype(BF16)
    low = (row % 2).astype(F32).astype(BF16)
    top_row = lax.broadcasted_iota(jnp.int32, (8, pairs), 0)

    def spread(part):
        return lax.dot_general(part, mine, (((0,), (0,)), ((), ())), preferred_element_type=F32)

    def table(d, carry):
        at = pl.ds(pl.multiple_of(d * group, group), group)
        hit = (spread(slot_ref[at, :].astype(BF16)) == place_in_expert).astype(F32)
        hot = hit.astype(BF16)
        position = 2.0 * jnp.dot(high, hot, preferred_element_type=F32) + jnp.dot(low, hot, preferred_element_type=F32)
        w = weight_ref[at, :]
        first = w.astype(BF16)
        over = w - first.astype(F32)
        second = over.astype(BF16)
        third = (over - second.astype(F32)).astype(BF16)
        value = jnp.sum((spread(first) + spread(second) + spread(third)) * hit, axis=0, keepdims=True)
        meta_ref[d] = jnp.where(top_row == 0, position, jnp.broadcast_to(value, (8, pairs)))
        return carry

    lax.fori_loop(0, devices, table, 0)


def moe_kernel(nx, ny, x_ref, ids_ref, gate_ref, wg_ref, wu_ref, wd_ref, out_ref, tok_ref, h_ref, w_ref,
               metav, meta_ref, slot_ref, weight_ref, rb, db, ms, mr, ty_s, ty_r, tx_s, tx_r, td_s, td_r, hd_s, hd_r, hf_s, hf_r,
               wa_s, wa_r, wb_s, wb_r, wf_s, wf_r, rs_r, db_r, of_r, credit):
    rows, width = x_ref.shape
    half = rows // 2
    el, ff, _ = wg_ref.shape
    per = h_ref.shape[5]
    rest = ff - LANES * (ff // LANES)
    whole = el * (ff // LANES)
    assert ff // LANES == 1 and (el * rest) % LANES == 0 and rest <= 128
    pairs = el * per
    kc, cw = w_ref.shape[0], w_ref.shape[4]
    ep_piece = el // PIECES
    eps = 2 * nx
    y = lax.axis_index('tp')
    ep = lax.axis_index('ep')
    x, c = ep // 2, ep % 2
    ya, yb, yo = place(y, A), place(y, B), place(y, O)
    yq = (y, ya, yb, yo)
    xp, xm = (x + 1) % nx, (x + nx - 1) % nx
    colb = ((y + y // 2) % 2) * (kc * cw)
    cola = ((ya + ya // 2) % 2) * (kc * cw)
    me = y * eps + ep

    dev_a = {'tp': ya, 'ep': ep}
    dev_b = {'tp': yb, 'ep': ep}
    dev_p = {'tp': y, 'ep': 2 * x + 1 - c}
    dev_xp = {'tp': y, 'ep': 2 * xp + c}
    dev_xm = {'tp': y, 'ep': 2 * xm + c}

    def remote(src, dst, send, recv, dev):
        return pltpu.make_async_remote_copy(src_ref=src, dst_ref=dst, send_sem=send, recv_sem=recv, device_id=dev, device_id_type=MESH)

    def lin(xs, ys, cs):
        return ys * eps + 2 * xs + cs

    def either(rel):
        return c if rel == 0 else 1 - c

    barrier = pltpu.get_barrier_semaphore()

    def peer_of(d):
        other = (me + d) % (ny * eps)
        return other // eps, other % eps

    def greet(d, carry):
        py, pe = peer_of(d)
        pl.semaphore_signal(barrier, inc=1, device_id={'tp': py, 'ep': pe}, device_id_type=MESH)
        return carry

    lax.fori_loop(1, ny * eps, greet, 0)
    pl.semaphore_wait(barrier, ny * eps - 1)

    def meta_copy(d):
        py, pe = peer_of(d)
        return remote(meta_ref.at[pe], metav.at[me], ms.at[d], mr.at[me], {'tp': py, 'ep': pe})

    def meta_send(d, carry):
        meta_copy(d).start()
        return carry

    def own(dxm, q):
        return tok_ref.at[(x + dxm) % nx, yq[q], c]

    def rows_of(ref, part, cut=None):
        cut = half if cut is None else cut
        return ref.at[pl.ds(part * cut, (cut, rows - cut)[part])]

    def ty(n):
        if n < 2:
            return remote(x_ref, tok_ref.at[x, y, c], ty_s.at[n], ty_r.at[n], (dev_a, dev_b)[n])
        block = rows_of(own(0, (B, A)[n - 2]), n - 2, rows * OPPOSITE_VIA_A // 4)
        return remote(block, block, ty_s.at[n], ty_r.at[n], (dev_a, dev_b)[n - 2])

    def tx(q, n):
        if n < 2:
            return remote(x_ref if q == S else own(0, q), own(0, q), tx_s.at[q, n], tx_r.at[q, n], (dev_xp, dev_xm)[n])
        block = rows_of(own((3, 1)[n - 2], q), n - 2)
        return remote(block, block, tx_s.at[q, n], tx_r.at[q, n], (dev_xp, dev_xm)[n - 2])

    def td(q, dxm):
        return remote(x_ref if (q == S and dxm == 0) else own(dxm, q), own(dxm, q), td_s.at[q, dxm], td_r.at[q, dxm], dev_p)

    def wa(k, g):
        src = wd_ref.at[pl.ds(g * ep_piece, ep_piece), :, pl.ds(pl.multiple_of(cola + k * cw, cw), cw)]
        return remote(src, w_ref.at[k, y, pl.ds(g * ep_piece, ep_piece)], wa_s.at[k, g], wa_r.at[k, g], dev_a)

    def wb(k, g):
        src = wd_ref.at[pl.ds(g * ep_piece, ep_piece), :, pl.ds(pl.multiple_of(colb + k * cw, cw), cw)]
        return remote(src, w_ref.at[k, y, pl.ds(g * ep_piece, ep_piece)], wb_s.at[k, g], wb_r.at[k, g], dev_b)

    def wf(k, g):
        block = w_ref.at[k, ya, pl.ds(g * ep_piece, ep_piece)]
        return remote(block, block, wf_s.at[k, g], wf_r.at[k, g], dev_b)

    def hd(i, s):
        dxm, q = order_of(i)
        block = h_ref.at[y, (x + dxm) % nx, yq[q], either(s)]
        return remote(block, block, hd_s.at[i, s], hd_r.at[i, s], dev_a if q < 2 else dev_b)

    def hf(i, s):
        dxm, q = order_of(i)
        block = h_ref.at[yb, (x + dxm) % nx, place(yb, q), either(s)]
        return remote(block, block, hf_s.at[i, s], hf_r.at[i, s], dev_a)

    def send(actions, load_w=None):
        for action in actions:
            kind, at = action[0], action[1:]
            if kind == 'wf':
                wa(*at).wait_recv()
            if kind == 'hf':
                hd(*at).wait_recv()
            if kind == 'lw':
                load_w(*at)
            else:
                {'wa': wa, 'wb': wb, 'wf': wf, 'hd': hd, 'hf': hf}[kind](*at).start()

    for n in (0, 1):
        ty(n).start()
        tx(S, n).start()
    td(S, 0).start()
    routing_tables(ids_ref, gate_ref, meta_ref, slot_ref, weight_ref, per)
    lax.fori_loop(1, ny * eps, meta_send, 0)
    metav[me] = meta_ref[ep]
    send(SEND_START)

    def came(q):
        for n in (0, 1):
            tx(q, n).wait_recv()
        td(q, 1).start()
        td(q, 3).start()

    def both(q, first):
        tx(q, first).start()
        tx(q, first + 1).start()

    def comm(step):
        if step == 1:
            ty(0).wait_recv()
            ty(1).wait_recv()
            for n in OPPOSITE:
                ty(n).start()
            both(A, 0)
            both(B, 0)
            came(S)
            td(A, 0).start()
            td(B, 0).start()
        if step == 4:
            came(A)
            for n in OPPOSITE:
                ty(n).wait_recv()
            both(O, 0)
            both(S, 2)
            both(A, 2)
            td(O, 0).start()
        if step in (7, 10):
            q = {7: B, 10: O}[step]
            came(q)
            both(q, 2)
        if step >= 12:
            tx(step - 12, 2).wait_recv()
            tx(step - 12, 3).wait_recv()
            td(step - 12, 2).start()

    row_id = lax.broadcasted_iota(jnp.int32, (rows, pairs), 0)

    def one_hot(src):
        pos = metav[src, 0:1, :].astype(jnp.int32)
        return (row_id == pos).astype(F32).astype(BF16)

    def meta_wait(src):
        remote(meta_ref.at[0], metav.at[src], ms.at[0], mr.at[src], dev_p).wait_recv()

    def phase_one(wg, wu, tb, xg, hb, left, wl, tl, hl):
        load_g = pltpu.make_async_copy(wg_ref, wg, wl.at[0])
        load_u = pltpu.make_async_copy(wu_ref, wu, wl.at[1])
        load_g.start()
        load_u.start()

        def store(i):
            dxm, q = order_of(i)
            return pltpu.make_async_copy(hb, h_ref.at[y, (x + dxm) % nx, place(y, q)], hl.at[0])

        def batch(i, carry):
            @pl.when(i > 0)
            def _():
                store(i - 1).wait()

            for step in range(1, 16):
                if SEND_BEFORE[step] or SEND_AFTER[step] or step in (1, 4, 7, 10) or step >= 12:
                    @pl.when(i == step)
                    def _(step=step):
                        send(SEND_BEFORE[step])
                        comm(step)
                        send(SEND_AFTER[step])

            dxm, q = order_of(i)
            xs, ys = (x + dxm) % nx, place(y, q)
            mine = pltpu.make_async_copy(x_ref, tb.at[0], tl.at[0])
            other = pltpu.make_async_copy(tok_ref.at[xs, ys, c], tb.at[0], tl.at[0])
            theirs = pltpu.make_async_copy(tok_ref.at[xs, ys, 1 - c], tb.at[1], tl.at[1])

            @pl.when(i == 0)
            def _():
                mine.start()

            @pl.when(i > 0)
            def _():
                other.start()
                meta_wait(lin(xs, ys, c))

            for s in (0, 1):
                if s == 1:
                    block = tok_ref.at[xs, ys, c]
                    remote(block, block, td_s.at[q, dxm], td_r.at[q, dxm], dev_p).wait_recv()
                    theirs.start()
                    meta_wait(lin(xs, ys, 1 - c))
                (other, theirs)[s].wait()
                hot = one_hot(lin(xs, ys, either(s)))
                step = min(512, width)
                for lo in range(0, width, step):
                    got = lax.dot_general(hot, tb[s, :, lo:lo + step], (((0,), (0,)), ((), ())), preferred_element_type=F32)
                    xg[:, s, :, lo:lo + step] = got.astype(BF16).reshape(el, per, step)

            @pl.when(i == 0)
            def _():
                load_g.wait()
                load_u.wait()

            for e in range(el):
                lhs = xg[e].reshape(2 * per, width)
                a = lax.dot_general(lhs, wg[e], (((1,), (1,)), ((), ())), preferred_element_type=F32)
                b = lax.dot_general(lhs, wu[e], (((1,), (1,)), ((), ())), preferred_element_type=F32)
                hid = a * jax.nn.sigmoid(a) * b
                for s in (0, 1):
                    hb[either(s), e] = hid[s * per:(s + 1) * per, :LANES].astype(BF16)
                left[e] = hid[:, LANES:]
            packed = jnp.concatenate([left[e] for e in range(el)], axis=1).astype(BF16)
            for m in range(el * rest // LANES):
                for s in (0, 1):
                    hb[either(s), whole + m] = packed[s * per:(s + 1) * per, m * LANES:(m + 1) * LANES]
            store(i).start()
            return carry

        lax.fori_loop(0, 16, batch, 0)
        store(15).wait()

    pl.run_scoped(
        phase_one,
        pltpu.VMEM((el, ff, width), BF16),
        pltpu.VMEM((el, ff, width), BF16),
        pltpu.VMEM((2, rows, width), BF16),
        pltpu.VMEM((el, 2, per, width), BF16),
        pltpu.VMEM((2,) + h_ref.shape[4:], BF16),
        pltpu.VMEM((el, 2 * per, rest), F32),
        pltpu.SemaphoreType.DMA((2,)),
        pltpu.SemaphoreType.DMA((2,)),
        pltpu.SemaphoreType.DMA((1,)),
    )

    def window(e):
        return e * rest // 128 * 128, -(-(e + 1) * rest // 128) * 128

    def offset(e, q):
        before = sum(LANES + window(m)[1] - window(m)[0] for m in range(e))
        return 4 * before + q * (LANES + window(e)[1] - window(e)[0])

    deep = offset(el, S)

    units = len(UNITS)

    def phase_two(wv, hv, gc, o3, pb, pp, sb, fb, wl, hvl, pp_s, rs_s, of_s, ol):
        lane = gc.shape[3]

        def clear(k, carry):
            for e in range(el):
                low, high = window(e)
                for q in (S, A, B, O):
                    at = offset(e, q) + LANES
                    for start, stop in ((0, e * rest - low), ((e + 1) * rest - low, high - low)):
                        if stop > start:
                            wv[k, at + start:at + stop] = jnp.zeros((stop - start, cw), BF16)
            return carry

        lax.fori_loop(0, kc, clear, 0)

        def blocks(j):
            return ((x + 2 * nx - 1 - j) % nx, (x + 1 + j) % nx), (y, ya)

        def w_loads(k):
            copies = []
            for q in (S, A, B, O):
                for e in range(el):
                    if q == S:
                        src = wd_ref.at[e, :, pl.ds(pl.multiple_of(colb + k * cw, cw), cw)]
                    else:
                        src = w_ref.at[k, yq[q], e]
                    low, high = window(e)
                    at = offset(e, q)
                    copies.append(pltpu.make_async_copy(src.at[pl.ds(0, LANES)], wv.at[k, pl.ds(at, LANES)], wl.at[k]))
                    copies.append(pltpu.make_async_copy(
                        src.at[pl.ds(LANES, rest)], wv.at[k, pl.ds(at + LANES + e * rest - low, rest)], wl.at[k]))
            return copies

        def load_w(k):
            for g in range(PIECES):
                wb(k, g).wait_recv()
                wf(k, g).wait_recv()
            for copy in w_loads(k):
                copy.start()

        def h_loads(n, j):
            xs, ys = blocks(j)
            copies = []
            for d in (0, 1):
                for rel in (0, 1):
                    for q in (S, A, B, O):
                        copies.append(pltpu.make_async_copy(
                            h_ref.at[yq[q], xs[d], ys[d], either(rel)], hv.at[n % 2, q, :, 2 * d + rel], hvl.at[n % 2, q, 2 * d + rel]))
            return copies

        def first_use(j):
            minus, plus = (3 - j) % 4, (1 + j) % 4
            for s in (0, 1):
                hd(BATCH[(minus, A)], s).wait_recv()
                hd(BATCH[(plus, S)], s).wait_recv()
                hf(BATCH[(minus, O)], s).wait_recv()
                hf(BATCH[(plus, B)], s).wait_recv()

        def partner_copy(n, d):
            return remote(pp.at[n % 2, d], db.at[n % 2, d], pp_s.at[n % 2, d], db_r.at[n % 2, d], dev_p)

        def ring_copy(slot, d, k, j):
            return remote(sb.at[slot, d], rb.at[d, k, j], rs_s.at[slot, d], rs_r.at[d, k, j], (dev_xp, dev_xm)[d])

        def out_copies(slot, k):
            cols = out_ref.at[:, pl.ds(pl.multiple_of(colb + k * cw, cw), cw)]
            return (
                pltpu.make_async_copy(fb.at[slot, 0], cols, ol.at[slot]),
                remote(fb.at[slot, 1], cols, of_s.at[slot], of_r.at[k], dev_a),
            )

        def make(n):
            k, j = look_up([u[0] for u in UNITS], n), look_up([u[1] for u in UNITS], n)
            xs, ys = blocks(j)
            for at in range(units):
                new_chunk = UNITS[at][0] not in [u[0] for u in UNITS[:at]]
                first = at in FIRST_STEP.values()
                if (not first and SEND_MAKE[at]) or new_chunk:
                    @pl.when(n == at)
                    def _(at=at, new_chunk=new_chunk, first=first):
                        if not first:
                            send(SEND_MAKE[at], load_w)
                        if new_chunk:
                            pltpu.make_async_copy(w_ref.at[UNITS[at][0]], w_ref.at[UNITS[at][0]], wl.at[UNITS[at][0]]).wait()
            for d in (0, 1):
                for rel in (0, 1):
                    gate = metav[lin(xs[d], ys[d], either(rel)), 1:2, :]
                    gc[:, 2 * d + rel] = jnp.transpose(jnp.broadcast_to(gate, (lane, pairs))).reshape(el, per, lane)
            for copy in h_loads(n, j):
                copy.wait()

            for e in range(el):
                low, high = window(e)
                parts = []
                for q in (S, A, B, O):
                    parts.append(hv[n % 2, q, e].reshape(4 * per, LANES))
                    for at in range(low, high, 128):
                        parts.append(hv[n % 2, q, whole + at // LANES, :, :, at % LANES:at % LANES + 128].reshape(4 * per, 128))
                size = 4 * (LANES + high - low)
                o = jnp.dot(jnp.concatenate(parts, axis=1), wv[k, offset(e, S):offset(e, S) + size], preferred_element_type=F32)
                g = gc[e].reshape(4 * per, lane)
                v = o * jnp.concatenate([g] * (cw // lane), axis=1)
                hi = v.astype(BF16)
                over = v - hi.astype(F32)
                mid = over.astype(BF16)
                low_part = (over - mid.astype(F32)).astype(BF16)
                o3[:, 0, e] = hi.reshape(4, per, cw)
                o3[:, 1, e] = mid.reshape(4, per, cw)
                o3[:, 2, e] = low_part.reshape(4, per, cw)

            @pl.when(n >= 2)
            def _():
                for d in (0, 1):
                    partner_copy(n - 2, d).wait_send()
                pl.semaphore_wait(credit, 1)

            for rel in (1, 0):
                for d in (0, 1):
                    hot = one_hot(lin(xs[d], ys[d], either(rel)))
                    total = jnp.dot(hot, o3[2 * d + rel, 0].reshape(pairs, cw), preferred_element_type=F32)
                    total += jnp.dot(hot, o3[2 * d + rel, 1].reshape(pairs, cw), preferred_element_type=F32)
                    total += jnp.dot(hot, o3[2 * d + rel, 2].reshape(pairs, cw), preferred_element_type=F32)
                    if rel == 1:
                        pp[n % 2, d] = total
                        partner_copy(n, d).start()
                    else:
                        pb[n % 2, d] = total

        def join(n):
            k, j = look_up([u[0] for u in UNITS], n), look_up([u[1] for u in UNITS], n)
            count = look_up([sum(1 for m in SENDS if m < at) for at in range(units)], n)
            slot = count % 4
            for at in range(units):
                if SEND_JOIN[at]:
                    @pl.when(n == at)
                    def _(at=at):
                        send(SEND_JOIN[at], load_w)
            for d in (0, 1):
                partner_copy(n, d).wait_recv()

            @pl.when((j < 3) & (count >= 4))
            def _():
                for d in (0, 1):
                    ring_copy(slot, d, k, 0).wait_send()

            for d in (0, 1):
                @pl.when(j == 0)
                def _():
                    sb[slot, d] = pb[n % 2, d] + db[n % 2, d]

                @pl.when((j > 0) & (j < 3))
                def _():
                    ring_copy(slot, d, k, j - 1).wait_recv()
                    sb[slot, d] = pb[n % 2, d] + db[n % 2, d] + rb[d, k, j - 1]

                @pl.when(j < 3)
                def _():
                    ring_copy(slot, d, k, j).start()

            for order, at in enumerate(FINALS):
                @pl.when(n == at)
                def _(order=order, at=at):
                    kk = UNITS[at][0]
                    if order >= 2:
                        local, away = out_copies(order % 2, kk)
                        local.wait()
                        away.wait_send()
                    for d in (0, 1):
                        ring_copy(0, d, kk, 2).wait_recv()
                        fb[order % 2, d] = (pb[at % 2, d] + db[at % 2, d] + rb[d, kk, 2]).astype(BF16)
                    local, away = out_copies(order % 2, kk)
                    local.start()
                    away.start()

            @pl.when(n < units - 2)
            def _():
                pl.semaphore_signal(credit, inc=1, device_id=dev_p, device_id_type=MESH)

        send([action for action in SEND_END if action[0] == 'lw'], load_w)
        send(SEND_MAKE[0], load_w)
        first_use(UNITS[0][1])
        for copy in h_loads(0, UNITS[0][1]):
            copy.start()
        seen = [int(at + 1 < units and FIRST_STEP[UNITS[at + 1][1]] <= at) for at in range(units)]

        def operation(at, carry):
            n = look_up([o[1] for o in ORDER], at)

            @pl.when(look_up([o[0] for o in ORDER], at) == 0)
            def _():
                for step, first in FIRST_STEP.items():
                    if first > 0:
                        @pl.when(n == first)
                        def _(step=step, first=first):
                            send(SEND_MAKE[first], load_w)
                            first_use(step)
                            for copy in h_loads(first, step):
                                copy.start()

                make(n)

                @pl.when(look_up(seen, n) == 1)
                def _():
                    for copy in h_loads(n + 1, look_up([u[1] for u in UNITS[1:]], n)):
                        copy.start()

            @pl.when(look_up([o[0] for o in ORDER], at) == 1)
            def _():
                join(n)

            return carry

        lax.fori_loop(0, len(ORDER), operation, 0)
        for d in (0, 1):
            for n in (units - 2, units - 1):
                partner_copy(n, d).wait_send()
            for slot in range(4):
                ring_copy(slot, d, 0, 0).wait_send()
        for slot in (0, 1):
            local, away = out_copies(slot, 0)
            local.wait()
            away.wait_send()
        for k in range(kc):
            out_copies(0, k)[1].wait_recv()

    lane = min(128, cw)
    send([action for action in SEND_END if action[0] != 'lw'])

    pl.run_scoped(
        phase_two,
        pltpu.VMEM((kc, deep, cw), BF16),
        pltpu.VMEM((2, 4, h_ref.shape[4], 4, per, LANES), BF16),
        pltpu.VMEM((el, 4, per, lane), F32),
        pltpu.VMEM((4, 3, el, per, cw), BF16),
        pltpu.VMEM((2, 2, rows, cw), F32),
        pltpu.VMEM((2, 2, rows, cw), F32),
        pltpu.VMEM((4, 2, rows, cw), F32),
        pltpu.VMEM((2, 2, rows, cw), BF16),
        pltpu.SemaphoreType.DMA((kc,)),
        pltpu.SemaphoreType.DMA((2, 4, 4)),
        pltpu.SemaphoreType.DMA((2, 2)),
        pltpu.SemaphoreType.DMA((4, 2)),
        pltpu.SemaphoreType.DMA((2,)),
        pltpu.SemaphoreType.DMA((2,)),
    )

    def meta_done(d, carry):
        meta_copy(d).wait_send()
        return carry

    lax.fori_loop(1, ny * eps, meta_done, 0)
    for n in (0, 1) + OPPOSITE:
        ty(n).wait_send()
    for q in (S, A, B, O):
        for n in range(4):
            tx(q, n).wait_send()
        for dxm in range(4):
            td(q, dxm).wait_send()
    for k in range(kc):
        for g in range(PIECES):
            wa(k, g).wait_send()
            wb(k, g).wait_send()
            wf(k, g).wait_send()
    for i in range(16):
        for s in (0, 1):
            hd(i, s).wait_send()
            if order_of(i)[1] >= 2:
                hf(i, s).wait_send()


def solution(mesh):
    ny, eps = mesh.shape['tp'], mesh.shape['ep']
    nx = eps // 2
    row_spec = P(('dp', 'ep', 'tp'), None)
    w_in_spec = P('ep', None, 'tp')
    w_out_spec = P('ep', 'tp', None)

    def local_moe(x, ids, gates, w_gate, w_up, w_down):
        rows, width = x.shape
        el, _, ff = w_gate.shape
        experts = el * eps
        per = rows * ids.shape[1] // experts
        pairs = el * per
        cw = width // 2 // CHUNKS
        hbm = pl.BlockSpec(memory_space=pl.ANY)
        vmem = pl.BlockSpec(memory_space=pltpu.VMEM)
        dma = pltpu.SemaphoreType.DMA
        outs = pl.pallas_call(
            functools.partial(moe_kernel, nx, ny),
            name='moe_kernel',
            out_shape=[
                jax.ShapeDtypeStruct((rows, width), BF16),
                jax.ShapeDtypeStruct((nx, ny, 2, rows, width), BF16),
                jax.ShapeDtypeStruct((ny, nx, ny, 2, el * ff // LANES, per, LANES), BF16),
                jax.ShapeDtypeStruct((CHUNKS, ny, el, ff, cw), BF16),
            ],
            in_specs=[hbm, vmem, vmem, hbm, hbm, hbm],
            out_specs=[hbm] * 4,
            scratch_shapes=[
                pltpu.VMEM((ny * eps, 8, pairs), F32),
                pltpu.VMEM((eps, 8, pairs), F32),
                pltpu.VMEM((experts, rows), F32),
                pltpu.VMEM((experts, rows), F32),
                pltpu.VMEM((2, CHUNKS, 3, rows, cw), F32),
                pltpu.VMEM((2, 2, rows, cw), F32),
                dma((ny * eps,)), dma((ny * eps,)),
                dma((4,)), dma((4,)),
                dma((4, 4)), dma((4, 4)),
                dma((4, 4)), dma((4, 4)),
                dma((16, 2)), dma((16, 2)), dma((16, 2)), dma((16, 2)),
            ] + [dma((CHUNKS, PIECES))] * 6 + [
                dma((2, CHUNKS, 3)), dma((2, 2)), dma((CHUNKS,)),
                pltpu.SemaphoreType.REGULAR,
            ],
            compiler_params=pltpu.CompilerParams(collective_id=0, has_side_effects=True, vmem_limit_bytes=67 * 1000 * 1000),
        )(x, ids.T, gates.T, jnp.transpose(w_gate, (0, 2, 1)), jnp.transpose(w_up, (0, 2, 1)), w_down)
        return outs[0]

    return jax.shard_map(
        local_moe, mesh=mesh, in_specs=(row_spec, row_spec, row_spec, w_in_spec, w_in_spec, w_out_spec),
        out_specs=row_spec, check_vma=False)
```

```python
import functools

import jax
import jax.numpy as jnp
from jax import lax
from jax.experimental import pallas as pl
from jax.experimental.pallas import tpu as pltpu
from jax.sharding import PartitionSpec as P

MESH = pl.DeviceIdType.MESH
CHUNKS = 4
LANES = 256
PIECES = 2
BF16 = jnp.bfloat16
F32 = jnp.float32

S, A, B, O = 0, 1, 2, 3

UNITS = ((2, 0), (1, 0), (0, 0), (2, 1), (0, 1), (1, 1), (0, 2), (3, 0), (1, 2), (3, 1), (2, 2), (1, 3), (3, 2), (0, 3), (2, 3), (3, 3), )
ORDER = ((0, 0), (0, 1), (1, 0), (0, 2), (1, 1), (1, 2), (0, 3), (0, 4), (1, 3), (1, 4), (0, 5), (0, 6), (1, 5), (1, 6), (0, 7), (0, 8), (1, 7), (0, 9), (1, 8), (0, 10), (1, 9), (1, 10), (0, 11), (0, 12), (1, 11), (0, 13), (1, 12), (0, 14), (1, 13), (0, 15), (1, 14), (1, 15), )
OPPOSITE_VIA_A = 4
OPPOSITE = (2,)
SEND_START = (('wa', 1, 1), ('wb', 3, 1), ('wb', 1, 0), )
SEND_BEFORE = (
    (),
    (),
    (('hd', 1), ('wa', 2, 0), ('wa', 0, 1), ('wa', 2, 1), ('wa', 3, 0), ('wa', 1, 0), ('wa', 0, 0), ('wf', 1, 1), ('wb', 2, 0), ('wb', 0, 0), ('wb', 0, 1), ('wb', 1, 1), ('wb', 2, 1), ),
    (),
    (),
    (),
    (),
    (('wf', 2, 0), ),
    (),
    (('hd', 8), ('hd', 7), ('wf', 0, 1), ),
    (),
    (('hf', 8), ('wa', 3, 1), ('hd', 5), ('wf', 1, 0), ),
    (('hd', 11), ('hd', 10), ('wf', 0, 0), ('wf', 2, 1), ),
    (('hd', 12), ('hf', 7), ),
    (('hf', 11), ('hd', 13), ),
    (('hf', 10), ('hd', 14), ),
)
SEND_AFTER = (
    (),
    (),
    (),
    (),
    (),
    (),
    (),
    (),
    (),
    (),
    (),
    (),
    (),
    (),
    (),
    (),
)
SEND_END = (('hd', 15), ('wf', 3, 1), ('hd', 9), ('wf', 3, 0), ('wb', 3, 0), ('hd', 6), ('lw', 0), ('lw', 1), ('lw', 2), )
SEND_MAKE = (
    (),
    (('hf', 14), ),
    (),
    (),
    (),
    (),
    (),
    (('lw', 3), ),
    (),
    (),
    (),
    (),
    (),
    (),
    (),
    (),
)
SEND_JOIN = (
    (),
    (('hf', 15), ('hd', 2), ('hd', 4), ('hd', 0), ('hd', 3), ),
    (),
    (('hf', 9), ),
    (),
    (),
    (),
    (('hf', 6), ),
    (),
    (),
    (),
    (),
    (),
    (),
    (),
    (),
)


def order_of(i):
    last, r = i // 12, i % 3
    return (1 - last) * (r + r // 2) + 2 * last, (1 - last) * (i // 3) + last * (i - 12)


BATCH = {order_of(i): i for i in range(16)}
FIRST_STEP = {}
for place_in_order, (chunk_of, step_of) in enumerate(UNITS):
    FIRST_STEP.setdefault(step_of, place_in_order)
SENDS = [n for n, (_, j) in enumerate(UNITS) if j < 3]
FINALS = [n for n, (_, j) in enumerate(UNITS) if j == 3]


def place(y, q):
    high, low = y // 2, y % 2
    return 2 * ((high + q // 2) % 2) + (low + (q + 1) // 2) % 2


def look_up(table, n):
    value = jnp.int32(table[0])
    for at in range(1, len(table)):
        if table[at] != table[0]:
            value = jnp.where(n == at, table[at], value)
    return value


def routing_tables(ids_ref, gate_ref, meta_ref, slot_ref, weight_ref, per):
    top, rows = ids_ref.shape
    experts = slot_ref.shape[0]
    devices, _, pairs = meta_ref.shape
    group = experts // devices
    expert = lax.broadcasted_iota(jnp.int32, (experts, rows), 0)
    chosen = jnp.zeros((experts, rows), F32)
    weight = jnp.zeros((experts, rows), F32)
    for j in range(top):
        here = expert == ids_ref[j:j + 1, :]
        chosen = jnp.where(here, 1.0, chosen)
        weight = jnp.where(here, gate_ref[j:j + 1, :], weight)
    earlier = lax.broadcasted_iota(jnp.int32, (rows, rows), 0) < lax.broadcasted_iota(jnp.int32, (rows, rows), 1)
    rank = jnp.dot(chosen.astype(BF16), earlier.astype(F32).astype(BF16), preferred_element_type=F32)
    slot_ref[...] = jnp.where(chosen > 0.0, rank, -1.0)
    weight_ref[...] = weight
    lane = lax.broadcasted_iota(jnp.int32, (group, pairs), 1)
    sub = lax.broadcasted_iota(jnp.int32, (group, pairs), 0)
    mine = ((lane >= sub * per) & (lane < (sub + 1) * per)).astype(F32).astype(BF16)
    place_in_expert = lax.broadcasted_iota(jnp.int32, (rows, pairs), 1)
    for m in range(1, group):
        place_in_expert = jnp.where(lax.broadcasted_iota(jnp.int32, (rows, pairs), 1) >= m * per,
                                    lax.broadcasted_iota(jnp.int32, (rows, pairs), 1) - m * per, place_in_expert)
    place_in_expert = place_in_expert.astype(F32)
    row = lax.broadcasted_iota(jnp.int32, (8, rows), 1)
    high = (row // 2).astype(F32).astype(BF16)
    low = (row % 2).astype(F32).astype(BF16)
    top_row = lax.broadcasted_iota(jnp.int32, (8, pairs), 0)

    def spread(part):
        return lax.dot_general(part, mine, (((0,), (0,)), ((), ())), preferred_element_type=F32)

    def table(d, carry):
        at = pl.ds(pl.multiple_of(d * group, group), group)
        hit = (spread(slot_ref[at, :].astype(BF16)) == place_in_expert).astype(F32)
        hot = hit.astype(BF16)
        position = 2.0 * jnp.dot(high, hot, preferred_element_type=F32) + jnp.dot(low, hot, preferred_element_type=F32)
        w = weight_ref[at, :]
        first = w.astype(BF16)
        over = w - first.astype(F32)
        second = over.astype(BF16)
        third = (over - second.astype(F32)).astype(BF16)
        value = jnp.sum((spread(first) + spread(second) + spread(third)) * hit, axis=0, keepdims=True)
        meta_ref[d] = jnp.where(top_row == 0, position, jnp.broadcast_to(value, (8, pairs)))
        return carry

    lax.fori_loop(0, devices, table, 0)


def moe_kernel(nx, ny, x_ref, ids_ref, gate_ref, wg_ref, wu_ref, wd_ref, out_ref, tok_ref, h_ref, w_ref,
               metav, meta_ref, slot_ref, weight_ref, rb, db, ms, mr, ty_s, ty_r, tx_s, tx_r, td_s, td_r, hd_s, hd_r, hf_s, hf_r,
               wa_s, wa_r, wb_s, wb_r, wf_s, wf_r, rs_r, db_r, of_r, credit):
    rows, width = x_ref.shape
    half = rows // 2
    el, ff, _ = wg_ref.shape
    per = h_ref.shape[5]
    rest = ff - LANES * (ff // LANES)
    whole = el * (ff // LANES)
    assert ff // LANES == 1 and (el * rest) % LANES == 0 and rest <= 128
    pairs = el * per
    kc, cw = w_ref.shape[0], w_ref.shape[4]
    ep_piece = el // PIECES
    eps = 2 * nx
    y = lax.axis_index('tp')
    ep = lax.axis_index('ep')
    x, c = ep // 2, ep % 2
    ya, yb, yo = place(y, A), place(y, B), place(y, O)
    yq = (y, ya, yb, yo)
    xp, xm = (x + 1) % nx, (x + nx - 1) % nx
    colb = ((y + y // 2) % 2) * (kc * cw)
    cola = ((ya + ya // 2) % 2) * (kc * cw)
    me = y * eps + ep

    dev_a = {'tp': ya, 'ep': ep}
    dev_b = {'tp': yb, 'ep': ep}
    dev_p = {'tp': y, 'ep': 2 * x + 1 - c}
    dev_xp = {'tp': y, 'ep': 2 * xp + c}
    dev_xm = {'tp': y, 'ep': 2 * xm + c}

    def remote(src, dst, send, recv, dev):
        return pltpu.make_async_remote_copy(src_ref=src, dst_ref=dst, send_sem=send, recv_sem=recv, device_id=dev, device_id_type=MESH)

    def lin(xs, ys, cs):
        return ys * eps + 2 * xs + cs

    def either(rel):
        return c if rel == 0 else 1 - c

    barrier = pltpu.get_barrier_semaphore()

    def peer_of(d):
        other = (me + d) % (ny * eps)
        return other // eps, other % eps

    def greet(d, carry):
        py, pe = peer_of(d)
        pl.semaphore_signal(barrier, inc=1, device_id={'tp': py, 'ep': pe}, device_id_type=MESH)
        return carry

    lax.fori_loop(1, ny * eps, greet, 0)
    pl.semaphore_wait(barrier, ny * eps - 1)

    def meta_copy(d):
        py, pe = peer_of(d)
        return remote(meta_ref.at[pe], metav.at[me], ms.at[d], mr.at[me], {'tp': py, 'ep': pe})

    def meta_send(d, carry):
        meta_copy(d).start()
        return carry

    def own(dxm, q):
        return tok_ref.at[(x + dxm) % nx, yq[q], c]

    def rows_of(ref, part, cut=None):
        cut = half if cut is None else cut
        return ref.at[pl.ds(part * cut, (cut, rows - cut)[part])]

    def ty(n):
        if n < 2:
            return remote(x_ref, tok_ref.at[x, y, c], ty_s.at[n], ty_r.at[n], (dev_a, dev_b)[n])
        block = rows_of(own(0, (B, A)[n - 2]), n - 2, rows * OPPOSITE_VIA_A // 4)
        return remote(block, block, ty_s.at[n], ty_r.at[n], (dev_a, dev_b)[n - 2])

    def tx(q, n):
        if n < 2:
            return remote(x_ref if q == S else own(0, q), own(0, q), tx_s.at[q, n], tx_r.at[q, n], (dev_xp, dev_xm)[n])
        block = rows_of(own((3, 1)[n - 2], q), n - 2)
        return remote(block, block, tx_s.at[q, n], tx_r.at[q, n], (dev_xp, dev_xm)[n - 2])

    def td(q, dxm):
        return remote(x_ref if (q == S and dxm == 0) else own(dxm, q), own(dxm, q), td_s.at[q, dxm], td_r.at[q, dxm], dev_p)

    def wa(k, g):
        src = wd_ref.at[pl.ds(g * ep_piece, ep_piece), :, pl.ds(pl.multiple_of(cola + k * cw, cw), cw)]
        return remote(src, w_ref.at[k, y, pl.ds(g * ep_piece, ep_piece)], wa_s.at[k, g], wa_r.at[k, g], dev_a)

    def wb(k, g):
        src = wd_ref.at[pl.ds(g * ep_piece, ep_piece), :, pl.ds(pl.multiple_of(colb + k * cw, cw), cw)]
        return remote(src, w_ref.at[k, y, pl.ds(g * ep_piece, ep_piece)], wb_s.at[k, g], wb_r.at[k, g], dev_b)

    def wf(k, g):
        block = w_ref.at[k, ya, pl.ds(g * ep_piece, ep_piece)]
        return remote(block, block, wf_s.at[k, g], wf_r.at[k, g], dev_b)

    def hd(i):
        dxm, q = order_of(i)
        block = h_ref.at[y, (x + dxm) % nx, yq[q]]
        return remote(block, block, hd_s.at[i], hd_r.at[i], dev_a if q < 2 else dev_b)

    def hf(i):
        dxm, q = order_of(i)
        block = h_ref.at[yb, (x + dxm) % nx, place(yb, q)]
        return remote(block, block, hf_s.at[i], hf_r.at[i], dev_a)

    def send(actions, load_w=None):
        for action in actions:
            kind, at = action[0], action[1:]
            if kind == 'wf':
                wa(*at).wait_recv()
            if kind == 'hf':
                hd(*at).wait_recv()
            if kind == 'lw':
                load_w(*at)
            else:
                {'wa': wa, 'wb': wb, 'wf': wf, 'hd': hd, 'hf': hf}[kind](*at).start()

    for n in (0, 1):
        ty(n).start()
        tx(S, n).start()
    td(S, 0).start()
    routing_tables(ids_ref, gate_ref, meta_ref, slot_ref, weight_ref, per)
    lax.fori_loop(1, ny * eps, meta_send, 0)
    metav[me] = meta_ref[ep]
    send(SEND_START)

    def came(q):
        for n in (0, 1):
            tx(q, n).wait_recv()
        td(q, 1).start()
        td(q, 3).start()

    def both(q, first):
        tx(q, first).start()
        tx(q, first + 1).start()

    def comm(step):
        if step == 1:
            ty(0).wait_recv()
            ty(1).wait_recv()
            for n in OPPOSITE:
                ty(n).start()
            both(A, 0)
            both(B, 0)
            came(S)
            td(A, 0).start()
            td(B, 0).start()
        if step == 4:
            came(A)
            for n in OPPOSITE:
                ty(n).wait_recv()
            both(O, 0)
            both(S, 2)
            both(A, 2)
            td(O, 0).start()
        if step in (7, 10):
            q = {7: B, 10: O}[step]
            came(q)
            both(q, 2)
        if step >= 12:
            tx(step - 12, 2).wait_recv()
            tx(step - 12, 3).wait_recv()
            td(step - 12, 2).start()

    row_id = lax.broadcasted_iota(jnp.int32, (rows, pairs), 0)

    def one_hot(src):
        pos = metav[src, 0:1, :].astype(jnp.int32)
        return (row_id == pos).astype(F32).astype(BF16)

    def meta_wait(src):
        remote(meta_ref.at[0], metav.at[src], ms.at[0], mr.at[src], dev_p).wait_recv()

    def phase_one(wg, wu, tb, xg, hb, left, wl, tl, hl):
        load_g = pltpu.make_async_copy(wg_ref, wg, wl.at[0])
        load_u = pltpu.make_async_copy(wu_ref, wu, wl.at[1])
        load_g.start()
        load_u.start()

        def store(i):
            dxm, q = order_of(i)
            return pltpu.make_async_copy(hb, h_ref.at[y, (x + dxm) % nx, place(y, q)], hl.at[0])

        def batch(i, carry):
            @pl.when(i > 0)
            def _():
                store(i - 1).wait()

            for step in range(1, 16):
                if SEND_BEFORE[step] or SEND_AFTER[step] or step in (1, 4, 7, 10) or step >= 12:
                    @pl.when(i == step)
                    def _(step=step):
                        send(SEND_BEFORE[step])
                        comm(step)
                        send(SEND_AFTER[step])

            dxm, q = order_of(i)
            xs, ys = (x + dxm) % nx, place(y, q)
            mine = pltpu.make_async_copy(x_ref, tb.at[0], tl.at[0])
            other = pltpu.make_async_copy(tok_ref.at[xs, ys, c], tb.at[0], tl.at[0])
            theirs = pltpu.make_async_copy(tok_ref.at[xs, ys, 1 - c], tb.at[1], tl.at[1])

            @pl.when(i == 0)
            def _():
                mine.start()

            @pl.when(i > 0)
            def _():
                other.start()
                meta_wait(lin(xs, ys, c))

            for s in (0, 1):
                if s == 1:
                    block = tok_ref.at[xs, ys, c]
                    remote(block, block, td_s.at[q, dxm], td_r.at[q, dxm], dev_p).wait_recv()
                    theirs.start()
                    meta_wait(lin(xs, ys, 1 - c))
                (other, theirs)[s].wait()
                hot = one_hot(lin(xs, ys, either(s)))
                step = min(512, width)
                for lo in range(0, width, step):
                    got = lax.dot_general(hot, tb[s, :, lo:lo + step], (((0,), (0,)), ((), ())), preferred_element_type=F32)
                    xg[:, s, :, lo:lo + step] = got.astype(BF16).reshape(el, per, step)

            @pl.when(i == 0)
            def _():
                load_g.wait()
                load_u.wait()

            for e in range(el):
                lhs = xg[e].reshape(2 * per, width)
                a = lax.dot_general(lhs, wg[e], (((1,), (1,)), ((), ())), preferred_element_type=F32)
                b = lax.dot_general(lhs, wu[e], (((1,), (1,)), ((), ())), preferred_element_type=F32)
                hid = a * jax.nn.sigmoid(a) * b
                for s in (0, 1):
                    hb[either(s), e] = hid[s * per:(s + 1) * per, :LANES].astype(BF16)
                left[e] = hid[:, LANES:]
            packed = jnp.concatenate([left[e] for e in range(el)], axis=1).astype(BF16)
            for m in range(el * rest // LANES):
                for s in (0, 1):
                    hb[either(s), whole + m] = packed[s * per:(s + 1) * per, m * LANES:(m + 1) * LANES]
            store(i).start()
            return carry

        lax.fori_loop(0, 16, batch, 0)
        store(15).wait()

    pl.run_scoped(
        phase_one,
        pltpu.VMEM((el, ff, width), BF16),
        pltpu.VMEM((el, ff, width), BF16),
        pltpu.VMEM((2, rows, width), BF16),
        pltpu.VMEM((el, 2, per, width), BF16),
        pltpu.VMEM((2,) + h_ref.shape[4:], BF16),
        pltpu.VMEM((el, 2 * per, rest), F32),
        pltpu.SemaphoreType.DMA((2,)),
        pltpu.SemaphoreType.DMA((2,)),
        pltpu.SemaphoreType.DMA((1,)),
    )

    def window(e):
        return e * rest // 128 * 128, -(-(e + 1) * rest // 128) * 128

    def offset(e, q):
        before = sum(LANES + window(m)[1] - window(m)[0] for m in range(e))
        return 4 * before + q * (LANES + window(e)[1] - window(e)[0])

    deep = offset(el, S)

    units = len(UNITS)

    def phase_two(wv, hv, gc, o3, pb, pp, sb, fb, wl, hvl, pp_s, rs_s, of_s, ol):
        lane = gc.shape[3]

        def clear(k, carry):
            for e in range(el):
                low, high = window(e)
                for q in (S, A, B, O):
                    at = offset(e, q) + LANES
                    for start, stop in ((0, e * rest - low), ((e + 1) * rest - low, high - low)):
                        if stop > start:
                            wv[k, at + start:at + stop] = jnp.zeros((stop - start, cw), BF16)
            return carry

        lax.fori_loop(0, kc, clear, 0)

        def blocks(j):
            return ((x + 2 * nx - 1 - j) % nx, (x + 1 + j) % nx), (y, ya)

        def w_loads(k):
            copies = []
            for q in (S, A, B, O):
                for e in range(el):
                    if q == S:
                        src = wd_ref.at[e, :, pl.ds(pl.multiple_of(colb + k * cw, cw), cw)]
                    else:
                        src = w_ref.at[k, yq[q], e]
                    low, high = window(e)
                    at = offset(e, q)
                    copies.append(pltpu.make_async_copy(src.at[pl.ds(0, LANES)], wv.at[k, pl.ds(at, LANES)], wl.at[k]))
                    copies.append(pltpu.make_async_copy(
                        src.at[pl.ds(LANES, rest)], wv.at[k, pl.ds(at + LANES + e * rest - low, rest)], wl.at[k]))
            return copies

        def load_w(k):
            for g in range(PIECES):
                wb(k, g).wait_recv()
                wf(k, g).wait_recv()
            for copy in w_loads(k):
                copy.start()

        def h_loads(n, j):
            xs, ys = blocks(j)
            copies = []
            for d in (0, 1):
                for rel in (0, 1):
                    for q in (S, A, B, O):
                        copies.append(pltpu.make_async_copy(
                            h_ref.at[yq[q], xs[d], ys[d], either(rel)], hv.at[n % 2, q, :, 2 * d + rel], hvl.at[n % 2, q, 2 * d + rel]))
            return copies

        def first_use(j):
            minus, plus = (3 - j) % 4, (1 + j) % 4
            hd(BATCH[(minus, A)]).wait_recv()
            hd(BATCH[(plus, S)]).wait_recv()
            hf(BATCH[(minus, O)]).wait_recv()
            hf(BATCH[(plus, B)]).wait_recv()

        def partner_copy(n, d):
            return remote(pp.at[n % 2, d], db.at[n % 2, d], pp_s.at[n % 2, d], db_r.at[n % 2, d], dev_p)

        def ring_copy(slot, d, k, j):
            return remote(sb.at[slot, d], rb.at[d, k, j], rs_s.at[slot, d], rs_r.at[d, k, j], (dev_xp, dev_xm)[d])

        def out_copies(slot, k):
            cols = out_ref.at[:, pl.ds(pl.multiple_of(colb + k * cw, cw), cw)]
            return (
                pltpu.make_async_copy(fb.at[slot, 0], cols, ol.at[slot]),
                remote(fb.at[slot, 1], cols, of_s.at[slot], of_r.at[k], dev_a),
            )

        def make(n):
            k, j = look_up([u[0] for u in UNITS], n), look_up([u[1] for u in UNITS], n)
            xs, ys = blocks(j)
            for at in range(units):
                new_chunk = UNITS[at][0] not in [u[0] for u in UNITS[:at]]
                first = at in FIRST_STEP.values()
                if (not first and SEND_MAKE[at]) or new_chunk:
                    @pl.when(n == at)
                    def _(at=at, new_chunk=new_chunk, first=first):
                        if not first:
                            send(SEND_MAKE[at], load_w)
                        if new_chunk:
                            pltpu.make_async_copy(w_ref.at[UNITS[at][0]], w_ref.at[UNITS[at][0]], wl.at[UNITS[at][0]]).wait()
            for d in (0, 1):
                for rel in (0, 1):
                    gate = metav[lin(xs[d], ys[d], either(rel)), 1:2, :]
                    gc[:, 2 * d + rel] = jnp.transpose(jnp.broadcast_to(gate, (lane, pairs))).reshape(el, per, lane)
            for copy in h_loads(n, j):
                copy.wait()

            for e in range(el):
                low, high = window(e)
                parts = []
                for q in (S, A, B, O):
                    parts.append(hv[n % 2, q, e].reshape(4 * per, LANES))
                    for at in range(low, high, 128):
                        parts.append(hv[n % 2, q, whole + at // LANES, :, :, at % LANES:at % LANES + 128].reshape(4 * per, 128))
                size = 4 * (LANES + high - low)
                o = jnp.dot(jnp.concatenate(parts, axis=1), wv[k, offset(e, S):offset(e, S) + size], preferred_element_type=F32)
                g = gc[e].reshape(4 * per, lane)
                v = o * jnp.concatenate([g] * (cw // lane), axis=1)
                hi = v.astype(BF16)
                over = v - hi.astype(F32)
                mid = over.astype(BF16)
                low_part = (over - mid.astype(F32)).astype(BF16)
                o3[:, 0, e] = hi.reshape(4, per, cw)
                o3[:, 1, e] = mid.reshape(4, per, cw)
                o3[:, 2, e] = low_part.reshape(4, per, cw)

            @pl.when(n >= 2)
            def _():
                for d in (0, 1):
                    partner_copy(n - 2, d).wait_send()
                pl.semaphore_wait(credit, 1)

            for rel in (1, 0):
                for d in (0, 1):
                    hot = one_hot(lin(xs[d], ys[d], either(rel)))
                    total = jnp.dot(hot, o3[2 * d + rel, 0].reshape(pairs, cw), preferred_element_type=F32)
                    total += jnp.dot(hot, o3[2 * d + rel, 1].reshape(pairs, cw), preferred_element_type=F32)
                    total += jnp.dot(hot, o3[2 * d + rel, 2].reshape(pairs, cw), preferred_element_type=F32)
                    if rel == 1:
                        pp[n % 2, d] = total
                        partner_copy(n, d).start()
                    else:
                        pb[n % 2, d] = total

        def join(n):
            k, j = look_up([u[0] for u in UNITS], n), look_up([u[1] for u in UNITS], n)
            count = look_up([sum(1 for m in SENDS if m < at) for at in range(units)], n)
            slot = count % 4
            for at in range(units):
                if SEND_JOIN[at]:
                    @pl.when(n == at)
                    def _(at=at):
                        send(SEND_JOIN[at], load_w)
            for d in (0, 1):
                partner_copy(n, d).wait_recv()

            @pl.when((j < 3) & (count >= 4))
            def _():
                for d in (0, 1):
                    ring_copy(slot, d, k, 0).wait_send()

            for d in (0, 1):
                @pl.when(j == 0)
                def _():
                    sb[slot, d] = pb[n % 2, d] + db[n % 2, d]

                @pl.when((j > 0) & (j < 3))
                def _():
                    ring_copy(slot, d, k, j - 1).wait_recv()
                    sb[slot, d] = pb[n % 2, d] + db[n % 2, d] + rb[d, k, j - 1]

                @pl.when(j < 3)
                def _():
                    ring_copy(slot, d, k, j).start()

            for order, at in enumerate(FINALS):
                @pl.when(n == at)
                def _(order=order, at=at):
                    kk = UNITS[at][0]
                    if order >= 2:
                        local, away = out_copies(order % 2, kk)
                        local.wait()
                        away.wait_send()
                    for d in (0, 1):
                        ring_copy(0, d, kk, 2).wait_recv()
                        fb[order % 2, d] = (pb[at % 2, d] + db[at % 2, d] + rb[d, kk, 2]).astype(BF16)
                    local, away = out_copies(order % 2, kk)
                    local.start()
                    away.start()

            @pl.when(n < units - 2)
            def _():
                pl.semaphore_signal(credit, inc=1, device_id=dev_p, device_id_type=MESH)

        send([action for action in SEND_END if action[0] == 'lw'], load_w)
        send(SEND_MAKE[0], load_w)
        first_use(UNITS[0][1])
        for copy in h_loads(0, UNITS[0][1]):
            copy.start()
        seen = [int(at + 1 < units and FIRST_STEP[UNITS[at + 1][1]] <= at) for at in range(units)]

        def operation(at, carry):
            n = look_up([o[1] for o in ORDER], at)

            @pl.when(look_up([o[0] for o in ORDER], at) == 0)
            def _():
                for step, first in FIRST_STEP.items():
                    if first > 0:
                        @pl.when(n == first)
                        def _(step=step, first=first):
                            send(SEND_MAKE[first], load_w)
                            first_use(step)
                            for copy in h_loads(first, step):
                                copy.start()

                make(n)

                @pl.when(look_up(seen, n) == 1)
                def _():
                    for copy in h_loads(n + 1, look_up([u[1] for u in UNITS[1:]], n)):
                        copy.start()

            @pl.when(look_up([o[0] for o in ORDER], at) == 1)
            def _():
                join(n)

            return carry

        lax.fori_loop(0, len(ORDER), operation, 0)
        for d in (0, 1):
            for n in (units - 2, units - 1):
                partner_copy(n, d).wait_send()
            for slot in range(4):
                ring_copy(slot, d, 0, 0).wait_send()
        for slot in (0, 1):
            local, away = out_copies(slot, 0)
            local.wait()
            away.wait_send()
        for k in range(kc):
            out_copies(0, k)[1].wait_recv()

    lane = min(128, cw)
    send([action for action in SEND_END if action[0] != 'lw'])

    pl.run_scoped(
        phase_two,
        pltpu.VMEM((kc, deep, cw), BF16),
        pltpu.VMEM((2, 4, h_ref.shape[4], 4, per, LANES), BF16),
        pltpu.VMEM((el, 4, per, lane), F32),
        pltpu.VMEM((4, 3, el, per, cw), BF16),
        pltpu.VMEM((2, 2, rows, cw), F32),
        pltpu.VMEM((2, 2, rows, cw), F32),
        pltpu.VMEM((4, 2, rows, cw), F32),
        pltpu.VMEM((2, 2, rows, cw), BF16),
        pltpu.SemaphoreType.DMA((kc,)),
        pltpu.SemaphoreType.DMA((2, 4, 4)),
        pltpu.SemaphoreType.DMA((2, 2)),
        pltpu.SemaphoreType.DMA((4, 2)),
        pltpu.SemaphoreType.DMA((2,)),
        pltpu.SemaphoreType.DMA((2,)),
    )

    def meta_done(d, carry):
        meta_copy(d).wait_send()
        return carry

    lax.fori_loop(1, ny * eps, meta_done, 0)
    for n in (0, 1) + OPPOSITE:
        ty(n).wait_send()
    for q in (S, A, B, O):
        for n in range(4):
            tx(q, n).wait_send()
        for dxm in range(4):
            td(q, dxm).wait_send()
    for k in range(kc):
        for g in range(PIECES):
            wa(k, g).wait_send()
            wb(k, g).wait_send()
            wf(k, g).wait_send()
    for i in range(16):
        hd(i).wait_send()
        if order_of(i)[1] >= 2:
            hf(i).wait_send()


def solution(mesh):
    ny, eps = mesh.shape['tp'], mesh.shape['ep']
    nx = eps // 2
    row_spec = P(('dp', 'ep', 'tp'), None)
    w_in_spec = P('ep', None, 'tp')
    w_out_spec = P('ep', 'tp', None)

    def local_moe(x, ids, gates, w_gate, w_up, w_down):
        rows, width = x.shape
        el, _, ff = w_gate.shape
        experts = el * eps
        per = rows * ids.shape[1] // experts
        pairs = el * per
        cw = width // 2 // CHUNKS
        hbm = pl.BlockSpec(memory_space=pl.ANY)
        vmem = pl.BlockSpec(memory_space=pltpu.VMEM)
        dma = pltpu.SemaphoreType.DMA
        outs = pl.pallas_call(
            functools.partial(moe_kernel, nx, ny),
            name='moe_kernel',
            out_shape=[
                jax.ShapeDtypeStruct((rows, width), BF16),
                jax.ShapeDtypeStruct((nx, ny, 2, rows, width), BF16),
                jax.ShapeDtypeStruct((ny, nx, ny, 2, el * ff // LANES, per, LANES), BF16),
                jax.ShapeDtypeStruct((CHUNKS, ny, el, ff, cw), BF16),
            ],
            in_specs=[hbm, vmem, vmem, hbm, hbm, hbm],
            out_specs=[hbm] * 4,
            scratch_shapes=[
                pltpu.VMEM((ny * eps, 8, pairs), F32),
                pltpu.VMEM((eps, 8, pairs), F32),
                pltpu.VMEM((experts, rows), F32),
                pltpu.VMEM((experts, rows), F32),
                pltpu.VMEM((2, CHUNKS, 3, rows, cw), F32),
                pltpu.VMEM((2, 2, rows, cw), F32),
                dma((ny * eps,)), dma((ny * eps,)),
                dma((4,)), dma((4,)),
                dma((4, 4)), dma((4, 4)),
                dma((4, 4)), dma((4, 4)),
                dma((16,)), dma((16,)), dma((16,)), dma((16,)),
            ] + [dma((CHUNKS, PIECES))] * 6 + [
                dma((2, CHUNKS, 3)), dma((2, 2)), dma((CHUNKS,)),
                pltpu.SemaphoreType.REGULAR,
            ],
            compiler_params=pltpu.CompilerParams(collective_id=0, has_side_effects=True, vmem_limit_bytes=67 * 1000 * 1000),
        )(x, ids.T, gates.T, jnp.transpose(w_gate, (0, 2, 1)), jnp.transpose(w_up, (0, 2, 1)), w_down)
        return outs[0]

    return jax.shard_map(
        local_moe, mesh=mesh, in_specs=(row_spec, row_spec, row_spec, w_in_spec, w_in_spec, w_out_spec),
        out_specs=row_spec, check_vma=False)
```

```python
import functools

import jax
import jax.numpy as jnp
from jax import lax
from jax.experimental import pallas as pl
from jax.experimental.pallas import tpu as pltpu
from jax.sharding import PartitionSpec as P

MESH = pl.DeviceIdType.MESH
CHUNKS = 4
LANES = 256
PIECES = 2
BF16 = jnp.bfloat16
F32 = jnp.float32

S, A, B, O = 0, 1, 2, 3

UNITS = ((2, 0), (1, 0), (0, 0), (2, 1), (0, 1), (1, 1), (0, 2), (3, 0), (1, 2), (3, 1), (2, 2), (1, 3), (3, 2), (0, 3), (2, 3), (3, 3), )
ORDER = ((0, 0), (0, 1), (1, 0), (0, 2), (1, 1), (1, 2), (0, 3), (0, 4), (1, 3), (1, 4), (0, 5), (0, 6), (1, 5), (1, 6), (0, 7), (0, 8), (1, 7), (0, 9), (1, 8), (0, 10), (1, 9), (1, 10), (0, 11), (0, 12), (1, 11), (0, 13), (1, 12), (0, 14), (1, 13), (0, 15), (1, 14), (1, 15), )
OPPOSITE_VIA_A = 4
OPPOSITE = (2,)
SEND_START = (('wa', 1, 1), ('wb', 3, 1), ('wb', 1, 0), )
SEND_BEFORE = (
    (),
    (),
    (('hd', 1), ('wa', 2, 0), ('wa', 0, 1), ('wa', 2, 1), ('wa', 3, 0), ('wa', 1, 0), ('wa', 0, 0), ('wf', 1, 1), ('wb', 2, 0), ('wb', 0, 0), ('wb', 0, 1), ('wb', 1, 1), ('wb', 2, 1), ),
    (),
    (),
    (),
    (),
    (('wf', 2, 0), ),
    (),
    (('hd', 8), ('hd', 7), ('wf', 0, 1), ),
    (),
    (('hf', 8), ('wa', 3, 1), ('hd', 5), ('wf', 1, 0), ),
    (('hd', 11), ('hd', 10), ('wf', 0, 0), ('wf', 2, 1), ),
    (('hd', 12), ('hf', 7), ),
    (('hf', 11), ('hd', 13), ),
    (('hf', 10), ('hd', 14), ),
)
SEND_AFTER = (
    (),
    (),
    (),
    (),
    (),
    (),
    (),
    (),
    (),
    (),
    (),
    (),
    (),
    (),
    (),
    (),
)
SEND_END = (('hd', 15), ('wf', 3, 1), ('hd', 9), ('wf', 3, 0), ('wb', 3, 0), ('hd', 6), ('lw', 0), ('lw', 1), ('lw', 2), )
SEND_MAKE = (
    (),
    (('hf', 14), ),
    (),
    (),
    (),
    (),
    (),
    (('lw', 3), ),
    (),
    (),
    (),
    (),
    (),
    (),
    (),
    (),
)
SEND_JOIN = (
    (),
    (('hf', 15), ('hd', 2), ('hd', 4), ('hd', 0), ('hd', 3), ),
    (),
    (('hf', 9), ),
    (),
    (),
    (),
    (('hf', 6), ),
    (),
    (),
    (),
    (),
    (),
    (),
    (),
    (),
)


def order_of(i):
    last, r = i // 12, i % 3
    return (1 - last) * (r + r // 2) + 2 * last, (1 - last) * (i // 3) + last * (i - 12)


BATCH = {order_of(i): i for i in range(16)}
FIRST_STEP = {}
for place_in_order, (chunk_of, step_of) in enumerate(UNITS):
    FIRST_STEP.setdefault(step_of, place_in_order)
SENDS = [n for n, (_, j) in enumerate(UNITS) if j < 3]
FINALS = [n for n, (_, j) in enumerate(UNITS) if j == 3]


def place(y, q):
    high, low = y // 2, y % 2
    return 2 * ((high + q // 2) % 2) + (low + (q + 1) // 2) % 2


def look_up(table, n):
    value = jnp.int32(table[0])
    for at in range(1, len(table)):
        if table[at] != table[0]:
            value = jnp.where(n == at, table[at], value)
    return value


def routing_tables(ids_ref, gate_ref, meta_ref, slot_ref, weight_ref, per):
    top, rows = ids_ref.shape
    experts = slot_ref.shape[0]
    devices, _, pairs = meta_ref.shape
    group = experts // devices
    expert = lax.broadcasted_iota(jnp.int32, (experts, rows), 0)
    chosen = jnp.zeros((experts, rows), F32)
    weight = jnp.zeros((experts, rows), F32)
    for j in range(top):
        here = expert == ids_ref[j:j + 1, :]
        chosen = jnp.where(here, 1.0, chosen)
        weight = jnp.where(here, gate_ref[j:j + 1, :], weight)
    earlier = lax.broadcasted_iota(jnp.int32, (rows, rows), 0) < lax.broadcasted_iota(jnp.int32, (rows, rows), 1)
    rank = jnp.dot(chosen.astype(BF16), earlier.astype(F32).astype(BF16), preferred_element_type=F32)
    slot_ref[...] = jnp.where(chosen > 0.0, rank, -1.0)
    weight_ref[...] = weight
    lane = lax.broadcasted_iota(jnp.int32, (group, pairs), 1)
    sub = lax.broadcasted_iota(jnp.int32, (group, pairs), 0)
    mine = ((lane >= sub * per) & (lane < (sub + 1) * per)).astype(F32).astype(BF16)
    place_in_expert = lax.broadcasted_iota(jnp.int32, (rows, pairs), 1)
    for m in range(1, group):
        place_in_expert = jnp.where(lax.broadcasted_iota(jnp.int32, (rows, pairs), 1) >= m * per,
                                    lax.broadcasted_iota(jnp.int32, (rows, pairs), 1) - m * per, place_in_expert)
    place_in_expert = place_in_expert.astype(F32)
    row = lax.broadcasted_iota(jnp.int32, (8, rows), 1)
    high = (row // 2).astype(F32).astype(BF16)
    low = (row % 2).astype(F32).astype(BF16)
    top_row = lax.broadcasted_iota(jnp.int32, (8, pairs), 0)

    def spread(part):
        return lax.dot_general(part, mine, (((0,), (0,)), ((), ())), preferred_element_type=F32)

    def table(d, carry):
        at = pl.ds(pl.multiple_of(d * group, group), group)
        hit = (spread(slot_ref[at, :].astype(BF16)) == place_in_expert).astype(F32)
        hot = hit.astype(BF16)
        position = 2.0 * jnp.dot(high, hot, preferred_element_type=F32) + jnp.dot(low, hot, preferred_element_type=F32)
        w = weight_ref[at, :]
        first = w.astype(BF16)
        over = w - first.astype(F32)
        second = over.astype(BF16)
        third = (over - second.astype(F32)).astype(BF16)
        value = jnp.sum((spread(first) + spread(second) + spread(third)) * hit, axis=0, keepdims=True)
        meta_ref[d] = jnp.where(top_row == 0, position, jnp.broadcast_to(value, (8, pairs)))
        return carry

    lax.fori_loop(0, devices, table, 0)


def moe_kernel(nx, ny, x_ref, ids_ref, gate_ref, wg_ref, wu_ref, wd_ref, out_ref, tok_ref, h_ref, w_ref,
               metav, meta_ref, slot_ref, weight_ref, rb, db, ms, mr, ty_s, ty_r, tx_s, tx_r, td_s, td_r, te_s, te_r, hd_s, hd_r, hf_s, hf_r,
               wa_s, wa_r, wb_s, wb_r, wf_s, wf_r, rs_r, db_r, of_r, credit):
    rows, width = x_ref.shape
    half = rows // 2
    el, ff, _ = wg_ref.shape
    per = h_ref.shape[5]
    rest = ff - LANES * (ff // LANES)
    whole = el * (ff // LANES)
    assert ff // LANES == 1 and (el * rest) % LANES == 0 and rest <= 128
    pairs = el * per
    kc, cw = w_ref.shape[0], w_ref.shape[4]
    ep_piece = el // PIECES
    eps = 2 * nx
    y = lax.axis_index('tp')
    ep = lax.axis_index('ep')
    x, c = ep // 2, ep % 2
    ya, yb, yo = place(y, A), place(y, B), place(y, O)
    yq = (y, ya, yb, yo)
    xp, xm = (x + 1) % nx, (x + nx - 1) % nx
    colb = ((y + y // 2) % 2) * (kc * cw)
    cola = ((ya + ya // 2) % 2) * (kc * cw)
    me = y * eps + ep

    dev_a = {'tp': ya, 'ep': ep}
    dev_b = {'tp': yb, 'ep': ep}
    dev_p = {'tp': y, 'ep': 2 * x + 1 - c}
    dev_xp = {'tp': y, 'ep': 2 * xp + c}
    dev_xm = {'tp': y, 'ep': 2 * xm + c}

    def remote(src, dst, send, recv, dev):
        return pltpu.make_async_remote_copy(src_ref=src, dst_ref=dst, send_sem=send, recv_sem=recv, device_id=dev, device_id_type=MESH)

    def lin(xs, ys, cs):
        return ys * eps + 2 * xs + cs

    def either(rel):
        return c if rel == 0 else 1 - c

    barrier = pltpu.get_barrier_semaphore()

    def peer_of(d):
        other = (me + d) % (ny * eps)
        return other // eps, other % eps

    def greet(d, carry):
        py, pe = peer_of(d)
        pl.semaphore_signal(barrier, inc=1, device_id={'tp': py, 'ep': pe}, device_id_type=MESH)
        return carry

    lax.fori_loop(1, ny * eps, greet, 0)
    pl.semaphore_wait(barrier, ny * eps - 1)

    def meta_copy(d):
        py, pe = peer_of(d)
        return remote(meta_ref.at[pe], metav.at[me], ms.at[d], mr.at[me], {'tp': py, 'ep': pe})

    def meta_send(d, carry):
        meta_copy(d).start()
        return carry

    def own(dxm, q):
        return tok_ref.at[(x + dxm) % nx, yq[q], c]

    def rows_of(ref, part, cut=None):
        cut = half if cut is None else cut
        return ref.at[pl.ds(part * cut, (cut, rows - cut)[part])]

    def ty(n):
        if n < 2:
            return remote(x_ref, tok_ref.at[x, y, c], ty_s.at[n], ty_r.at[n], (dev_a, dev_b)[n])
        block = rows_of(own(0, (B, A)[n - 2]), n - 2, rows * OPPOSITE_VIA_A // 4)
        return remote(block, block, ty_s.at[n], ty_r.at[n], (dev_a, dev_b)[n - 2])

    def tx(q, n):
        if n < 2:
            return remote(x_ref if q == S else own(0, q), own(0, q), tx_s.at[q, n], tx_r.at[q, n], (dev_xp, dev_xm)[n])
        block = rows_of(own((3, 1)[n % 2], q), n % 2)
        if q == O:
            block = block.at[pl.ds((n // 2 - 1) * (half // 2), half // 2)]
        return remote(block, block, tx_s.at[q, n], tx_r.at[q, n], (dev_xp, dev_xm)[n % 2])

    def td(q, dxm):
        return remote(x_ref if (q == S and dxm == 0) else own(dxm, q), own(dxm, q), td_s.at[q, dxm], td_r.at[q, dxm], dev_p)

    def td_last(n):
        block = rows_of(own(2, O), n % 2).at[pl.ds(n // 2 * (half // 2), half // 2)]
        return remote(block, block, te_s.at[n], te_r.at[n], dev_p)

    def wa(k, g):
        src = wd_ref.at[pl.ds(g * ep_piece, ep_piece), :, pl.ds(pl.multiple_of(cola + k * cw, cw), cw)]
        return remote(src, w_ref.at[k, y, pl.ds(g * ep_piece, ep_piece)], wa_s.at[k, g], wa_r.at[k, g], dev_a)

    def wb(k, g):
        src = wd_ref.at[pl.ds(g * ep_piece, ep_piece), :, pl.ds(pl.multiple_of(colb + k * cw, cw), cw)]
        return remote(src, w_ref.at[k, y, pl.ds(g * ep_piece, ep_piece)], wb_s.at[k, g], wb_r.at[k, g], dev_b)

    def wf(k, g):
        block = w_ref.at[k, ya, pl.ds(g * ep_piece, ep_piece)]
        return remote(block, block, wf_s.at[k, g], wf_r.at[k, g], dev_b)

    def hd(i):
        dxm, q = order_of(i)
        block = h_ref.at[y, (x + dxm) % nx, yq[q]]
        return remote(block, block, hd_s.at[i], hd_r.at[i], dev_a if q < 2 else dev_b)

    def hf(i):
        dxm, q = order_of(i)
        block = h_ref.at[yb, (x + dxm) % nx, place(yb, q)]
        return remote(block, block, hf_s.at[i], hf_r.at[i], dev_a)

    def send(actions, load_w=None):
        for action in actions:
            kind, at = action[0], action[1:]
            if kind == 'wf':
                wa(*at).wait_recv()
            if kind == 'hf':
                hd(*at).wait_recv()
            if kind == 'lw':
                load_w(*at)
            else:
                {'wa': wa, 'wb': wb, 'wf': wf, 'hd': hd, 'hf': hf}[kind](*at).start()

    for n in (0, 1):
        ty(n).start()
        tx(S, n).start()
    td(S, 0).start()
    routing_tables(ids_ref, gate_ref, meta_ref, slot_ref, weight_ref, per)
    lax.fori_loop(1, ny * eps, meta_send, 0)
    metav[me] = meta_ref[ep]
    send(SEND_START)

    def came(q):
        for n in (0, 1):
            tx(q, n).wait_recv()
        td(q, 1).start()
        td(q, 3).start()

    def both(q, first):
        tx(q, first).start()
        tx(q, first + 1).start()

    def comm(step):
        if step == 1:
            ty(0).wait_recv()
            ty(1).wait_recv()
            for n in OPPOSITE:
                ty(n).start()
            both(A, 0)
            both(B, 0)
            came(S)
            td(A, 0).start()
            td(B, 0).start()
        if step == 4:
            came(A)
            for n in OPPOSITE:
                ty(n).wait_recv()
            both(O, 0)
            both(S, 2)
            both(A, 2)
            td(O, 0).start()
        if step in (7, 10):
            q = {7: B, 10: O}[step]
            came(q)
            both(q, 2)
            if q == O:
                both(q, 4)
        if 12 <= step < 15:
            tx(step - 12, 2).wait_recv()
            tx(step - 12, 3).wait_recv()
            td(step - 12, 2).start()
        if step == 15:
            for n in range(4):
                tx(O, 2 + n).wait_recv()
                td_last(n).start()

    row_id = lax.broadcasted_iota(jnp.int32, (rows, pairs), 0)

    def one_hot(src):
        pos = metav[src, 0:1, :].astype(jnp.int32)
        return (row_id == pos).astype(F32).astype(BF16)

    def meta_wait(src):
        remote(meta_ref.at[0], metav.at[src], ms.at[0], mr.at[src], dev_p).wait_recv()

    def phase_one(wg, wu, tb, xg, hb, left, wl, tl, hl):
        load_g = pltpu.make_async_copy(wg_ref, wg, wl.at[0])
        load_u = pltpu.make_async_copy(wu_ref, wu, wl.at[1])
        load_g.start()
        load_u.start()

        def store(i):
            dxm, q = order_of(i)
            return pltpu.make_async_copy(hb, h_ref.at[y, (x + dxm) % nx, place(y, q)], hl.at[0])

        def batch(i, carry):
            @pl.when(i > 0)
            def _():
                store(i - 1).wait()

            for step in range(1, 16):
                if SEND_BEFORE[step] or SEND_AFTER[step] or step in (1, 4, 7, 10) or step >= 12:
                    @pl.when(i == step)
                    def _(step=step):
                        send(SEND_BEFORE[step])
                        comm(step)
                        send(SEND_AFTER[step])

            dxm, q = order_of(i)
            xs, ys = (x + dxm) % nx, place(y, q)
            mine = pltpu.make_async_copy(x_ref, tb.at[0], tl.at[0])
            other = pltpu.make_async_copy(tok_ref.at[xs, ys, c], tb.at[0], tl.at[0])
            theirs = pltpu.make_async_copy(tok_ref.at[xs, ys, 1 - c], tb.at[1], tl.at[1])

            @pl.when(i == 0)
            def _():
                mine.start()

            @pl.when(i > 0)
            def _():
                other.start()
                meta_wait(lin(xs, ys, c))

            for s in (0, 1):
                if s == 1:
                    @pl.when(i < 15)
                    def _():
                        block = tok_ref.at[xs, ys, c]
                        remote(block, block, td_s.at[q, dxm], td_r.at[q, dxm], dev_p).wait_recv()

                    @pl.when(i == 15)
                    def _():
                        for n in range(4):
                            td_last(n).wait_recv()

                    theirs.start()
                    meta_wait(lin(xs, ys, 1 - c))
                (other, theirs)[s].wait()
                hot = one_hot(lin(xs, ys, either(s)))
                step = min(512, width)
                for lo in range(0, width, step):
                    got = lax.dot_general(hot, tb[s, :, lo:lo + step], (((0,), (0,)), ((), ())), preferred_element_type=F32)
                    xg[:, s, :, lo:lo + step] = got.astype(BF16).reshape(el, per, step)

            @pl.when(i == 0)
            def _():
                load_g.wait()
                load_u.wait()

            for e in range(el):
                lhs = xg[e].reshape(2 * per, width)
                a = lax.dot_general(lhs, wg[e], (((1,), (1,)), ((), ())), preferred_element_type=F32)
                b = lax.dot_general(lhs, wu[e], (((1,), (1,)), ((), ())), preferred_element_type=F32)
                hid = a * jax.nn.sigmoid(a) * b
                for s in (0, 1):
                    hb[either(s), e] = hid[s * per:(s + 1) * per, :LANES].astype(BF16)
                left[e] = hid[:, LANES:]
            packed = jnp.concatenate([left[e] for e in range(el)], axis=1).astype(BF16)
            for m in range(el * rest // LANES):
                for s in (0, 1):
                    hb[either(s), whole + m] = packed[s * per:(s + 1) * per, m * LANES:(m + 1) * LANES]
            store(i).start()
            return carry

        lax.fori_loop(0, 16, batch, 0)
        store(15).wait()

    pl.run_scoped(
        phase_one,
        pltpu.VMEM((el, ff, width), BF16),
        pltpu.VMEM((el, ff, width), BF16),
        pltpu.VMEM((2, rows, width), BF16),
        pltpu.VMEM((el, 2, per, width), BF16),
        pltpu.VMEM((2,) + h_ref.shape[4:], BF16),
        pltpu.VMEM((el, 2 * per, rest), F32),
        pltpu.SemaphoreType.DMA((2,)),
        pltpu.SemaphoreType.DMA((2,)),
        pltpu.SemaphoreType.DMA((1,)),
    )

    def all_sent():
        def meta_done(d, carry):
            meta_copy(d).wait_send()
            return carry

        lax.fori_loop(1, ny * eps, meta_done, 0)
        for n in (0, 1) + OPPOSITE:
            ty(n).wait_send()
        for q in (S, A, B, O):
            for n in range(6 if q == O else 4):
                tx(q, n).wait_send()
            for dxm in range(4):
                if (dxm, q) != (2, O):
                    td(q, dxm).wait_send()
        for n in range(4):
            td_last(n).wait_send()
        for k in range(kc):
            for g in range(PIECES):
                wa(k, g).wait_send()
                wb(k, g).wait_send()
                wf(k, g).wait_send()
        for i in range(16):
            hd(i).wait_send()
            if order_of(i)[1] >= 2:
                hf(i).wait_send()

    def window(e):
        return e * rest // 128 * 128, -(-(e + 1) * rest // 128) * 128

    def offset(e, q):
        before = sum(LANES + window(m)[1] - window(m)[0] for m in range(e))
        return 4 * before + q * (LANES + window(e)[1] - window(e)[0])

    deep = offset(el, S)

    units = len(UNITS)

    def phase_two(wv, hv, gc, o3, pb, pp, sb, fb, wl, hvl, pp_s, rs_s, of_s, ol):
        lane = gc.shape[3]

        def clear(k):
            for e in range(el):
                low, high = window(e)
                for q in (S, A, B, O):
                    at = offset(e, q) + LANES
                    for start, stop in ((0, e * rest - low), ((e + 1) * rest - low, high - low)):
                        if stop > start:
                            wv[k, at + start:at + stop] = jnp.zeros((stop - start, cw), BF16)

        def blocks(j):
            return ((x + 2 * nx - 1 - j) % nx, (x + 1 + j) % nx), (y, ya)

        def w_loads(k):
            copies = []
            for q in (S, A, B, O):
                for e in range(el):
                    if q == S:
                        src = wd_ref.at[e, :, pl.ds(pl.multiple_of(colb + k * cw, cw), cw)]
                    else:
                        src = w_ref.at[k, yq[q], e]
                    low, high = window(e)
                    at = offset(e, q)
                    copies.append(pltpu.make_async_copy(src.at[pl.ds(0, LANES)], wv.at[k, pl.ds(at, LANES)], wl.at[k]))
                    copies.append(pltpu.make_async_copy(
                        src.at[pl.ds(LANES, rest)], wv.at[k, pl.ds(at + LANES + e * rest - low, rest)], wl.at[k]))
            return copies

        def load_w(k):
            for g in range(PIECES):
                wb(k, g).wait_recv()
                wf(k, g).wait_recv()
            for copy in w_loads(k):
                copy.start()
            clear(k)

        def h_loads(n, j):
            xs, ys = blocks(j)
            copies = []
            for d in (0, 1):
                for rel in (0, 1):
                    for q in (S, A, B, O):
                        copies.append(pltpu.make_async_copy(
                            h_ref.at[yq[q], xs[d], ys[d], either(rel)], hv.at[n % 2, q, :, 2 * d + rel], hvl.at[n % 2, q, 2 * d + rel]))
            return copies

        def first_use(j):
            minus, plus = (3 - j) % 4, (1 + j) % 4
            hd(BATCH[(minus, A)]).wait_recv()
            hd(BATCH[(plus, S)]).wait_recv()
            hf(BATCH[(minus, O)]).wait_recv()
            hf(BATCH[(plus, B)]).wait_recv()

        def partner_copy(n, d):
            return remote(pp.at[n % 2, d], db.at[n % 2, d], pp_s.at[n % 2, d], db_r.at[n % 2, d], dev_p)

        def ring_copy(slot, d, k, j):
            return remote(sb.at[slot, d], rb.at[d, k, j], rs_s.at[slot, d], rs_r.at[d, k, j], (dev_xp, dev_xm)[d])

        def out_copies(slot, k):
            cols = out_ref.at[:, pl.ds(pl.multiple_of(colb + k * cw, cw), cw)]
            return (
                pltpu.make_async_copy(fb.at[slot, 0], cols, ol.at[slot]),
                remote(fb.at[slot, 1], cols, of_s.at[slot], of_r.at[k], dev_a),
            )

        def make(n):
            k, j = look_up([u[0] for u in UNITS], n), look_up([u[1] for u in UNITS], n)
            xs, ys = blocks(j)
            for at in range(units):
                new_chunk = UNITS[at][0] not in [u[0] for u in UNITS[:at]]
                first = at in FIRST_STEP.values()
                if (not first and SEND_MAKE[at]) or new_chunk:
                    @pl.when(n == at)
                    def _(at=at, new_chunk=new_chunk, first=first):
                        if not first:
                            send(SEND_MAKE[at], load_w)
                        if new_chunk:
                            pltpu.make_async_copy(w_ref.at[UNITS[at][0]], w_ref.at[UNITS[at][0]], wl.at[UNITS[at][0]]).wait()
            for d in (0, 1):
                for rel in (0, 1):
                    gate = metav[lin(xs[d], ys[d], either(rel)), 1:2, :]
                    gc[:, 2 * d + rel] = jnp.transpose(jnp.broadcast_to(gate, (lane, pairs))).reshape(el, per, lane)
            for copy in h_loads(n, j):
                copy.wait()

            @pl.when(n == 0)
            def _():
                later = [action for action in SEND_END + SEND_MAKE[0] if action[0] == 'lw' and action[1] != UNITS[0][0]]
                send(later, load_w)

            for e in range(el):
                low, high = window(e)
                parts = []
                for q in (S, A, B, O):
                    parts.append(hv[n % 2, q, e].reshape(4 * per, LANES))
                    for at in range(low, high, 128):
                        parts.append(hv[n % 2, q, whole + at // LANES, :, :, at % LANES:at % LANES + 128].reshape(4 * per, 128))
                size = 4 * (LANES + high - low)
                o = jnp.dot(jnp.concatenate(parts, axis=1), wv[k, offset(e, S):offset(e, S) + size], preferred_element_type=F32)
                g = gc[e].reshape(4 * per, lane)
                v = o * jnp.concatenate([g] * (cw // lane), axis=1)
                hi = v.astype(BF16)
                over = v - hi.astype(F32)
                mid = over.astype(BF16)
                low_part = (over - mid.astype(F32)).astype(BF16)
                o3[:, 0, e] = hi.reshape(4, per, cw)
                o3[:, 1, e] = mid.reshape(4, per, cw)
                o3[:, 2, e] = low_part.reshape(4, per, cw)

            @pl.when(n >= 2)
            def _():
                for d in (0, 1):
                    partner_copy(n - 2, d).wait_send()
                pl.semaphore_wait(credit, 1)

            for rel in (1, 0):
                for d in (0, 1):
                    hot = one_hot(lin(xs[d], ys[d], either(rel)))
                    total = jnp.dot(hot, o3[2 * d + rel, 0].reshape(pairs, cw), preferred_element_type=F32)
                    total += jnp.dot(hot, o3[2 * d + rel, 1].reshape(pairs, cw), preferred_element_type=F32)
                    total += jnp.dot(hot, o3[2 * d + rel, 2].reshape(pairs, cw), preferred_element_type=F32)
                    if rel == 1:
                        pp[n % 2, d] = total
                        partner_copy(n, d).start()
                    else:
                        pb[n % 2, d] = total

        def join(n):
            k, j = look_up([u[0] for u in UNITS], n), look_up([u[1] for u in UNITS], n)
            count = look_up([sum(1 for m in SENDS if m < at) for at in range(units)], n)
            slot = count % 4
            for at in range(units):
                if SEND_JOIN[at]:
                    @pl.when(n == at)
                    def _(at=at):
                        send(SEND_JOIN[at], load_w)
            for d in (0, 1):
                partner_copy(n, d).wait_recv()

            @pl.when((j < 3) & (count >= 4))
            def _():
                for d in (0, 1):
                    ring_copy(slot, d, k, 0).wait_send()

            for d in (0, 1):
                @pl.when(j == 0)
                def _():
                    sb[slot, d] = pb[n % 2, d] + db[n % 2, d]

                @pl.when((j > 0) & (j < 3))
                def _():
                    ring_copy(slot, d, k, j - 1).wait_recv()
                    sb[slot, d] = pb[n % 2, d] + db[n % 2, d] + rb[d, k, j - 1]

                @pl.when(j < 3)
                def _():
                    ring_copy(slot, d, k, j).start()

            for order, at in enumerate(FINALS):
                @pl.when(n == at)
                def _(order=order, at=at):
                    kk = UNITS[at][0]
                    if order >= 2:
                        local, away = out_copies(order % 2, kk)
                        local.wait()
                        away.wait_send()
                    local, away = out_copies(order % 2, kk)
                    for d in (1, 0):
                        ring_copy(0, d, kk, 2).wait_recv()
                        fb[order % 2, d] = (pb[at % 2, d] + db[at % 2, d] + rb[d, kk, 2]).astype(BF16)
                        (local, away)[d].start()

            @pl.when(n < units - 2)
            def _():
                pl.semaphore_signal(credit, inc=1, device_id=dev_p, device_id_type=MESH)

        send([action for action in SEND_MAKE[0] if action[0] != 'lw'])
        load_w(UNITS[0][0])
        first_use(UNITS[0][1])
        for copy in h_loads(0, UNITS[0][1]):
            copy.start()
        seen = [int(at + 1 < units and FIRST_STEP[UNITS[at + 1][1]] <= at) for at in range(units)]

        def operation(at, carry):
            n = look_up([o[1] for o in ORDER], at)

            @pl.when(look_up([o[0] for o in ORDER], at) == 0)
            def _():
                for step, first in FIRST_STEP.items():
                    if first > 0:
                        @pl.when(n == first)
                        def _(step=step, first=first):
                            send(SEND_MAKE[first], load_w)
                            first_use(step)
                            for copy in h_loads(first, step):
                                copy.start()

                make(n)

                @pl.when(look_up(seen, n) == 1)
                def _():
                    for copy in h_loads(n + 1, look_up([u[1] for u in UNITS[1:]], n)):
                        copy.start()

            @pl.when(look_up([o[0] for o in ORDER], at) == 1)
            def _():
                join(n)

            return carry

        lax.fori_loop(0, len(ORDER), operation, 0)
        for d in (0, 1):
            for n in (units - 2, units - 1):
                partner_copy(n, d).wait_send()
            for slot in range(4):
                ring_copy(slot, d, 0, 0).wait_send()
        for slot in (0, 1):
            local, away = out_copies(slot, 0)
            local.wait()
            away.wait_send()
        all_sent()
        for k in range(kc):
            out_copies(0, k)[1].wait_recv()

    lane = min(128, cw)
    send([action for action in SEND_END if action[0] != 'lw'])

    pl.run_scoped(
        phase_two,
        pltpu.VMEM((kc, deep, cw), BF16),
        pltpu.VMEM((2, 4, h_ref.shape[4], 4, per, LANES), BF16),
        pltpu.VMEM((el, 4, per, lane), F32),
        pltpu.VMEM((4, 3, el, per, cw), BF16),
        pltpu.VMEM((2, 2, rows, cw), F32),
        pltpu.VMEM((2, 2, rows, cw), F32),
        pltpu.VMEM((4, 2, rows, cw), F32),
        pltpu.VMEM((2, 2, rows, cw), BF16),
        pltpu.SemaphoreType.DMA((kc,)),
        pltpu.SemaphoreType.DMA((2, 4, 4)),
        pltpu.SemaphoreType.DMA((2, 2)),
        pltpu.SemaphoreType.DMA((4, 2)),
        pltpu.SemaphoreType.DMA((2,)),
        pltpu.SemaphoreType.DMA((2,)),
    )


def solution(mesh):
    ny, eps = mesh.shape['tp'], mesh.shape['ep']
    nx = eps // 2
    row_spec = P(('dp', 'ep', 'tp'), None)
    w_in_spec = P('ep', None, 'tp')
    w_out_spec = P('ep', 'tp', None)

    def local_moe(x, ids, gates, w_gate, w_up, w_down):
        rows, width = x.shape
        el, _, ff = w_gate.shape
        experts = el * eps
        per = rows * ids.shape[1] // experts
        pairs = el * per
        cw = width // 2 // CHUNKS
        hbm = pl.BlockSpec(memory_space=pl.ANY)
        vmem = pl.BlockSpec(memory_space=pltpu.VMEM)
        dma = pltpu.SemaphoreType.DMA
        outs = pl.pallas_call(
            functools.partial(moe_kernel, nx, ny),
            name='moe_kernel',
            out_shape=[
                jax.ShapeDtypeStruct((rows, width), BF16),
                jax.ShapeDtypeStruct((nx, ny, 2, rows, width), BF16),
                jax.ShapeDtypeStruct((ny, nx, ny, 2, el * ff // LANES, per, LANES), BF16),
                jax.ShapeDtypeStruct((CHUNKS, ny, el, ff, cw), BF16),
            ],
            in_specs=[hbm, vmem, vmem, hbm, hbm, hbm],
            out_specs=[hbm] * 4,
            scratch_shapes=[
                pltpu.VMEM((ny * eps, 8, pairs), F32),
                pltpu.VMEM((eps, 8, pairs), F32),
                pltpu.VMEM((experts, rows), F32),
                pltpu.VMEM((experts, rows), F32),
                pltpu.VMEM((2, CHUNKS, 3, rows, cw), F32),
                pltpu.VMEM((2, 2, rows, cw), F32),
                dma((ny * eps,)), dma((ny * eps,)),
                dma((4,)), dma((4,)),
                dma((4, 6)), dma((4, 6)),
                dma((4, 4)), dma((4, 4)), dma((4,)), dma((4,)),
                dma((16,)), dma((16,)), dma((16,)), dma((16,)),
            ] + [dma((CHUNKS, PIECES))] * 6 + [
                dma((2, CHUNKS, 3)), dma((2, 2)), dma((CHUNKS,)),
                pltpu.SemaphoreType.REGULAR,
            ],
            compiler_params=pltpu.CompilerParams(collective_id=0, has_side_effects=True, vmem_limit_bytes=67 * 1000 * 1000),
        )(x, ids.T, gates.T, jnp.transpose(w_gate, (0, 2, 1)), jnp.transpose(w_up, (0, 2, 1)), w_down)
        return outs[0]

    return jax.shard_map(
        local_moe, mesh=mesh, in_specs=(row_spec, row_spec, row_spec, w_in_spec, w_in_spec, w_out_spec),
        out_specs=row_spec, check_vma=False)
```

```python
import functools

import jax
import jax.numpy as jnp
from jax import lax
from jax.experimental import pallas as pl
from jax.experimental.pallas import tpu as pltpu
from jax.sharding import PartitionSpec as P

MESH = pl.DeviceIdType.MESH
CHUNKS = 4
LANES = 256
PIECES = 2
BF16 = jnp.bfloat16
F32 = jnp.float32

S, A, B, O = 0, 1, 2, 3

UNITS = ((0, 0), (1, 0), (2, 0), (0, 1), (1, 1), (2, 1), (0, 2), (3, 0), (2, 2), (3, 1), (1, 2), (3, 2), (2, 3), (1, 3), (0, 3), (3, 3), )
ORDER = ((0, 0), (1, 0), (0, 1), (0, 2), (1, 1), (1, 2), (0, 3), (0, 4), (1, 3), (1, 4), (0, 5), (0, 6), (1, 5), (1, 6), (0, 7), (1, 7), (0, 8), (0, 9), (1, 8), (0, 10), (1, 9), (1, 10), (0, 11), (0, 12), (1, 11), (0, 13), (1, 12), (0, 14), (1, 13), (0, 15), (1, 14), (1, 15), )
OPPOSITE_VIA_A = 4
OPPOSITE = (2,)
SEND_START = (('wa', 2, 1), ('wb', 2, 1), )
SEND_BEFORE = (
    (),
    (),
    (('wf', 2, 1), ('wb', 1, 0), ('wb', 0, 1), ('wb', 2, 0), ('wb', 1, 1), ('wb', 0, 0), ),
    (('hd', 2), ('wa', 3, 0), ('wa', 2, 0), ('wa', 0, 0), ('wa', 1, 0), ),
    (),
    (),
    (('hd', 5), ('wa', 0, 1), ('wa', 1, 1), ('hd', 1), ),
    (),
    (('wf', 2, 0), ),
    (('hd', 8), ('hd', 7), ),
    (),
    (('hf', 7), ('hf', 8), ('hd', 10), ),
    (('hd', 11), ),
    (),
    (('hd', 13), ('hd', 12), ),
    (('hf', 11), ('hf', 10), ('hd', 14), ),
)
SEND_AFTER = (
    (),
    (),
    (),
    (),
    (),
    (),
    (),
    (),
    (),
    (),
    (('wf', 1, 0), ('wf', 0, 0), ),
    (),
    (),
    (('wf', 1, 1), ('wf', 0, 1), ),
    (),
    (),
)
SEND_END = (('hd', 15), ('wb', 3, 1), ('wf', 3, 0), ('wb', 3, 0), ('lw', 0), ('lw', 1), ('lw', 2), )
SEND_MAKE = (
    (),
    (),
    (('hf', 15), ('wa', 3, 1), ('hd', 4), ('hd', 0), ('hd', 3), ),
    (),
    (),
    (('wf', 3, 1), ('hd', 6), ('hd', 9), ),
    (),
    (('lw', 3), ),
    (('hf', 6), ),
    (),
    (),
    (),
    (),
    (),
    (),
    (),
)
SEND_JOIN = (
    (('hf', 14), ),
    (),
    (),
    (),
    (),
    (),
    (),
    (),
    (),
    (('hf', 9), ),
    (),
    (),
    (),
    (),
    (),
    (),
)


def order_of(i):
    last, r = i // 12, i % 3
    return (1 - last) * (r + r // 2) + 2 * last, (1 - last) * (i // 3) + last * (i - 12)


BATCH = {order_of(i): i for i in range(16)}
FIRST_STEP = {}
for place_in_order, (chunk_of, step_of) in enumerate(UNITS):
    FIRST_STEP.setdefault(step_of, place_in_order)
SENDS = [n for n, (_, j) in enumerate(UNITS) if j < 3]
FINALS = [n for n, (_, j) in enumerate(UNITS) if j == 3]


def place(y, q):
    high, low = y // 2, y % 2
    return 2 * ((high + q // 2) % 2) + (low + (q + 1) // 2) % 2


def look_up(table, n):
    value = jnp.int32(table[0])
    for at in range(1, len(table)):
        if table[at] != table[0]:
            value = jnp.where(n == at, table[at], value)
    return value


def routing_tables(ids_ref, gate_ref, meta_ref, slot_ref, weight_ref, per):
    top, rows = ids_ref.shape
    experts = slot_ref.shape[0]
    devices, _, pairs = meta_ref.shape
    group = experts // devices
    expert = lax.broadcasted_iota(jnp.int32, (experts, rows), 0)
    chosen = jnp.zeros((experts, rows), F32)
    weight = jnp.zeros((experts, rows), F32)
    for j in range(top):
        here = expert == ids_ref[j:j + 1, :]
        chosen = jnp.where(here, 1.0, chosen)
        weight = jnp.where(here, gate_ref[j:j + 1, :], weight)
    earlier = lax.broadcasted_iota(jnp.int32, (rows, rows), 0) < lax.broadcasted_iota(jnp.int32, (rows, rows), 1)
    rank = jnp.dot(chosen.astype(BF16), earlier.astype(F32).astype(BF16), preferred_element_type=F32)
    slot_ref[...] = jnp.where(chosen > 0.0, rank, -1.0)
    weight_ref[...] = weight
    lane = lax.broadcasted_iota(jnp.int32, (group, pairs), 1)
    sub = lax.broadcasted_iota(jnp.int32, (group, pairs), 0)
    mine = ((lane >= sub * per) & (lane < (sub + 1) * per)).astype(F32).astype(BF16)
    place_in_expert = lax.broadcasted_iota(jnp.int32, (rows, pairs), 1)
    for m in range(1, group):
        place_in_expert = jnp.where(lax.broadcasted_iota(jnp.int32, (rows, pairs), 1) >= m * per,
                                    lax.broadcasted_iota(jnp.int32, (rows, pairs), 1) - m * per, place_in_expert)
    place_in_expert = place_in_expert.astype(F32)
    row = lax.broadcasted_iota(jnp.int32, (8, rows), 1)
    high = (row // 2).astype(F32).astype(BF16)
    low = (row % 2).astype(F32).astype(BF16)
    top_row = lax.broadcasted_iota(jnp.int32, (8, pairs), 0)

    def spread(part):
        return lax.dot_general(part, mine, (((0,), (0,)), ((), ())), preferred_element_type=F32)

    def table(d, carry):
        at = pl.ds(pl.multiple_of(d * group, group), group)
        hit = (spread(slot_ref[at, :].astype(BF16)) == place_in_expert).astype(F32)
        hot = hit.astype(BF16)
        position = 2.0 * jnp.dot(high, hot, preferred_element_type=F32) + jnp.dot(low, hot, preferred_element_type=F32)
        w = weight_ref[at, :]
        first = w.astype(BF16)
        over = w - first.astype(F32)
        second = over.astype(BF16)
        third = (over - second.astype(F32)).astype(BF16)
        value = jnp.sum((spread(first) + spread(second) + spread(third)) * hit, axis=0, keepdims=True)
        meta_ref[d] = jnp.where(top_row == 0, position, jnp.broadcast_to(value, (8, pairs)))
        return carry

    lax.fori_loop(0, devices, table, 0)


def moe_kernel(nx, ny, x_ref, ids_ref, gate_ref, wg_ref, wu_ref, wd_ref, out_ref, tok_ref, h_ref, w_ref,
               metav, meta_ref, slot_ref, weight_ref, rb, db, ms, mr, ty_s, ty_r, tx_s, tx_r, td_s, td_r, te_s, te_r, hd_s, hd_r, hf_s, hf_r,
               wa_s, wa_r, wb_s, wb_r, wf_s, wf_r, rs_r, db_r, of_r, credit):
    rows, width = x_ref.shape
    half = rows // 2
    el, ff, _ = wg_ref.shape
    per = h_ref.shape[5]
    rest = ff - LANES * (ff // LANES)
    whole = el * (ff // LANES)
    assert ff // LANES == 1 and (el * rest) % LANES == 0 and rest <= 128
    pairs = el * per
    kc, cw = w_ref.shape[0], w_ref.shape[4]
    ep_piece = el // PIECES
    eps = 2 * nx
    y = lax.axis_index('tp')
    ep = lax.axis_index('ep')
    x, c = ep // 2, ep % 2
    ya, yb, yo = place(y, A), place(y, B), place(y, O)
    yq = (y, ya, yb, yo)
    xp, xm = (x + 1) % nx, (x + nx - 1) % nx
    colb = ((y + y // 2) % 2) * (kc * cw)
    cola = ((ya + ya // 2) % 2) * (kc * cw)
    me = y * eps + ep

    dev_a = {'tp': ya, 'ep': ep}
    dev_b = {'tp': yb, 'ep': ep}
    dev_p = {'tp': y, 'ep': 2 * x + 1 - c}
    dev_xp = {'tp': y, 'ep': 2 * xp + c}
    dev_xm = {'tp': y, 'ep': 2 * xm + c}

    def remote(src, dst, send, recv, dev):
        return pltpu.make_async_remote_copy(src_ref=src, dst_ref=dst, send_sem=send, recv_sem=recv, device_id=dev, device_id_type=MESH)

    def lin(xs, ys, cs):
        return ys * eps + 2 * xs + cs

    def either(rel):
        return c if rel == 0 else 1 - c

    barrier = pltpu.get_barrier_semaphore()

    def peer_of(d):
        other = (me + d) % (ny * eps)
        return other // eps, other % eps

    def greet(d, carry):
        py, pe = peer_of(d)
        pl.semaphore_signal(barrier, inc=1, device_id={'tp': py, 'ep': pe}, device_id_type=MESH)
        return carry

    lax.fori_loop(1, ny * eps, greet, 0)
    pl.semaphore_wait(barrier, ny * eps - 1)

    def meta_copy(d):
        py, pe = peer_of(d)
        return remote(meta_ref.at[pe], metav.at[me], ms.at[d], mr.at[me], {'tp': py, 'ep': pe})

    def meta_send(d, carry):
        meta_copy(d).start()
        return carry

    def own(dxm, q):
        return tok_ref.at[(x + dxm) % nx, yq[q], c]

    def rows_of(ref, part, cut=None):
        cut = half if cut is None else cut
        return ref.at[pl.ds(part * cut, (cut, rows - cut)[part])]

    def ty(n):
        if n < 2:
            return remote(x_ref, tok_ref.at[x, y, c], ty_s.at[n], ty_r.at[n], (dev_a, dev_b)[n])
        block = rows_of(own(0, (B, A)[n - 2]), n - 2, rows * OPPOSITE_VIA_A // 4)
        return remote(block, block, ty_s.at[n], ty_r.at[n], (dev_a, dev_b)[n - 2])

    def tx(q, n):
        if n < 2:
            return remote(x_ref if q == S else own(0, q), own(0, q), tx_s.at[q, n], tx_r.at[q, n], (dev_xp, dev_xm)[n])
        block = rows_of(own((3, 1)[n % 2], q), n % 2)
        if q == O:
            block = block.at[pl.ds((n // 2 - 1) * (half // 2), half // 2)]
        return remote(block, block, tx_s.at[q, n], tx_r.at[q, n], (dev_xp, dev_xm)[n % 2])

    def td(q, dxm):
        return remote(x_ref if (q == S and dxm == 0) else own(dxm, q), own(dxm, q), td_s.at[q, dxm], td_r.at[q, dxm], dev_p)

    def td_last(n):
        block = rows_of(own(2, O), n % 2).at[pl.ds(n // 2 * (half // 2), half // 2)]
        return remote(block, block, te_s.at[n], te_r.at[n], dev_p)

    def wa(k, g):
        src = wd_ref.at[pl.ds(g * ep_piece, ep_piece), :, pl.ds(pl.multiple_of(cola + k * cw, cw), cw)]
        return remote(src, w_ref.at[k, y, pl.ds(g * ep_piece, ep_piece)], wa_s.at[k, g], wa_r.at[k, g], dev_a)

    def wb(k, g):
        src = wd_ref.at[pl.ds(g * ep_piece, ep_piece), :, pl.ds(pl.multiple_of(colb + k * cw, cw), cw)]
        return remote(src, w_ref.at[k, y, pl.ds(g * ep_piece, ep_piece)], wb_s.at[k, g], wb_r.at[k, g], dev_b)

    def wf(k, g):
        block = w_ref.at[k, ya, pl.ds(g * ep_piece, ep_piece)]
        return remote(block, block, wf_s.at[k, g], wf_r.at[k, g], dev_b)

    def hd(i):
        dxm, q = order_of(i)
        block = h_ref.at[y, (x + dxm) % nx, yq[q]]
        return remote(block, block, hd_s.at[i], hd_r.at[i], dev_a if q < 2 else dev_b)

    def hf(i):
        dxm, q = order_of(i)
        block = h_ref.at[yb, (x + dxm) % nx, place(yb, q)]
        return remote(block, block, hf_s.at[i], hf_r.at[i], dev_a)

    def send(actions, load_w=None):
        for action in actions:
            kind, at = action[0], action[1:]
            if kind == 'wf':
                wa(*at).wait_recv()
            if kind == 'hf':
                hd(*at).wait_recv()
            if kind == 'lw':
                load_w(*at)
            else:
                {'wa': wa, 'wb': wb, 'wf': wf, 'hd': hd, 'hf': hf}[kind](*at).start()

    for n in (0, 1):
        ty(n).start()
        tx(S, n).start()
    td(S, 0).start()
    routing_tables(ids_ref, gate_ref, meta_ref, slot_ref, weight_ref, per)
    lax.fori_loop(1, ny * eps, meta_send, 0)
    metav[me] = meta_ref[ep]
    send(SEND_START)

    def came(q):
        for n in (0, 1):
            tx(q, n).wait_recv()
        td(q, 1).start()
        td(q, 3).start()

    def both(q, first):
        tx(q, first).start()
        tx(q, first + 1).start()

    def comm(step):
        if step == 1:
            ty(0).wait_recv()
            ty(1).wait_recv()
            for n in OPPOSITE:
                ty(n).start()
            both(A, 0)
            both(B, 0)
            came(S)
            td(A, 0).start()
            td(B, 0).start()
        if step == 4:
            came(A)
            for n in OPPOSITE:
                ty(n).wait_recv()
            both(O, 0)
            both(S, 2)
            both(A, 2)
            td(O, 0).start()
        if step in (7, 10):
            q = {7: B, 10: O}[step]
            came(q)
            both(q, 2)
            if q == O:
                both(q, 4)
        if 12 <= step < 15:
            tx(step - 12, 2).wait_recv()
            tx(step - 12, 3).wait_recv()
            td(step - 12, 2).start()
        if step == 15:
            for n in range(4):
                tx(O, 2 + n).wait_recv()
                td_last(n).start()

    row_id = lax.broadcasted_iota(jnp.int32, (rows, pairs), 0)

    def one_hot(src):
        pos = metav[src, 0:1, :].astype(jnp.int32)
        return (row_id == pos).astype(F32).astype(BF16)

    def meta_wait(src):
        remote(meta_ref.at[0], metav.at[src], ms.at[0], mr.at[src], dev_p).wait_recv()

    def phase_one(wg, wu, tb, xg, hb, left, wl, tl, hl):
        load_g = pltpu.make_async_copy(wg_ref, wg, wl.at[0])
        load_u = pltpu.make_async_copy(wu_ref, wu, wl.at[1])
        load_g.start()
        load_u.start()

        def store(i):
            dxm, q = order_of(i)
            return pltpu.make_async_copy(hb, h_ref.at[y, (x + dxm) % nx, place(y, q)], hl.at[0])

        def batch(i, carry):
            @pl.when(i > 0)
            def _():
                store(i - 1).wait()

            for step in range(1, 16):
                if SEND_BEFORE[step] or SEND_AFTER[step] or step in (1, 4, 7, 10) or step >= 12:
                    @pl.when(i == step)
                    def _(step=step):
                        send(SEND_BEFORE[step])
                        comm(step)
                        send(SEND_AFTER[step])

            dxm, q = order_of(i)
            xs, ys = (x + dxm) % nx, place(y, q)
            mine = pltpu.make_async_copy(x_ref, tb.at[0], tl.at[0])
            other = pltpu.make_async_copy(tok_ref.at[xs, ys, c], tb.at[0], tl.at[0])
            theirs = pltpu.make_async_copy(tok_ref.at[xs, ys, 1 - c], tb.at[1], tl.at[1])

            @pl.when(i == 0)
            def _():
                mine.start()

            @pl.when(i > 0)
            def _():
                other.start()
                meta_wait(lin(xs, ys, c))

            for s in (0, 1):
                if s == 1:
                    @pl.when(i < 15)
                    def _():
                        block = tok_ref.at[xs, ys, c]
                        remote(block, block, td_s.at[q, dxm], td_r.at[q, dxm], dev_p).wait_recv()

                    @pl.when(i == 15)
                    def _():
                        for n in range(4):
                            td_last(n).wait_recv()

                    theirs.start()
                    meta_wait(lin(xs, ys, 1 - c))
                (other, theirs)[s].wait()
                hot = one_hot(lin(xs, ys, either(s)))
                step = min(512, width)
                for lo in range(0, width, step):
                    got = lax.dot_general(hot, tb[s, :, lo:lo + step], (((0,), (0,)), ((), ())), preferred_element_type=F32)
                    xg[:, s, :, lo:lo + step] = got.astype(BF16).reshape(el, per, step)

            @pl.when(i == 0)
            def _():
                load_g.wait()
                load_u.wait()

            for e in range(el):
                lhs = xg[e].reshape(2 * per, width)
                a = lax.dot_general(lhs, wg[e], (((1,), (1,)), ((), ())), preferred_element_type=F32)
                b = lax.dot_general(lhs, wu[e], (((1,), (1,)), ((), ())), preferred_element_type=F32)
                hid = a * jax.nn.sigmoid(a) * b
                for s in (0, 1):
                    hb[either(s), e] = hid[s * per:(s + 1) * per, :LANES].astype(BF16)
                left[e] = hid[:, LANES:]
            packed = jnp.concatenate([left[e] for e in range(el)], axis=1).astype(BF16)
            for m in range(el * rest // LANES):
                for s in (0, 1):
                    hb[either(s), whole + m] = packed[s * per:(s + 1) * per, m * LANES:(m + 1) * LANES]
            store(i).start()
            return carry

        lax.fori_loop(0, 16, batch, 0)
        store(15).wait()

    pl.run_scoped(
        phase_one,
        pltpu.VMEM((el, ff, width), BF16),
        pltpu.VMEM((el, ff, width), BF16),
        pltpu.VMEM((2, rows, width), BF16),
        pltpu.VMEM((el, 2, per, width), BF16),
        pltpu.VMEM((2,) + h_ref.shape[4:], BF16),
        pltpu.VMEM((el, 2 * per, rest), F32),
        pltpu.SemaphoreType.DMA((2,)),
        pltpu.SemaphoreType.DMA((2,)),
        pltpu.SemaphoreType.DMA((1,)),
    )

    def all_sent():
        def meta_done(d, carry):
            meta_copy(d).wait_send()
            return carry

        lax.fori_loop(1, ny * eps, meta_done, 0)
        for n in (0, 1) + OPPOSITE:
            ty(n).wait_send()
        for q in (S, A, B, O):
            for n in range(6 if q == O else 4):
                tx(q, n).wait_send()
            for dxm in range(4):
                if (dxm, q) != (2, O):
                    td(q, dxm).wait_send()
        for n in range(4):
            td_last(n).wait_send()
        for k in range(kc):
            for g in range(PIECES):
                wa(k, g).wait_send()
                wb(k, g).wait_send()
                wf(k, g).wait_send()
        for i in range(16):
            hd(i).wait_send()
            if order_of(i)[1] >= 2:
                hf(i).wait_send()

    def window(e):
        return e * rest // 128 * 128, -(-(e + 1) * rest // 128) * 128

    def offset(e, q):
        before = sum(LANES + window(m)[1] - window(m)[0] for m in range(e))
        return 4 * before + q * (LANES + window(e)[1] - window(e)[0])

    deep = offset(el, S)

    units = len(UNITS)

    def phase_two(wv, hv, gc, o3, pb, pp, sb, fb, wl, hvl, pp_s, rs_s, of_s, ol):
        lane = gc.shape[3]

        def clear(k):
            for e in range(el):
                low, high = window(e)
                for q in (S, A, B, O):
                    at = offset(e, q) + LANES
                    for start, stop in ((0, e * rest - low), ((e + 1) * rest - low, high - low)):
                        if stop > start:
                            wv[k, at + start:at + stop] = jnp.zeros((stop - start, cw), BF16)

        def blocks(j):
            return ((x + 2 * nx - 1 - j) % nx, (x + 1 + j) % nx), (y, ya)

        def w_loads(k):
            copies = []
            for q in (S, A, B, O):
                for e in range(el):
                    if q == S:
                        src = wd_ref.at[e, :, pl.ds(pl.multiple_of(colb + k * cw, cw), cw)]
                    else:
                        src = w_ref.at[k, yq[q], e]
                    low, high = window(e)
                    at = offset(e, q)
                    copies.append(pltpu.make_async_copy(src.at[pl.ds(0, LANES)], wv.at[k, pl.ds(at, LANES)], wl.at[k]))
                    copies.append(pltpu.make_async_copy(
                        src.at[pl.ds(LANES, rest)], wv.at[k, pl.ds(at + LANES + e * rest - low, rest)], wl.at[k]))
            return copies

        def load_w(k):
            for g in range(PIECES):
                wb(k, g).wait_recv()
                wf(k, g).wait_recv()
            for copy in w_loads(k):
                copy.start()
            clear(k)

        def h_loads(n, j):
            xs, ys = blocks(j)
            copies = []
            for d in (0, 1):
                for rel in (0, 1):
                    for q in (S, A, B, O):
                        copies.append(pltpu.make_async_copy(
                            h_ref.at[yq[q], xs[d], ys[d], either(rel)], hv.at[n % 2, q, :, 2 * d + rel], hvl.at[n % 2, q, 2 * d + rel]))
            return copies

        def first_use(j):
            minus, plus = (3 - j) % 4, (1 + j) % 4
            hd(BATCH[(minus, A)]).wait_recv()
            hd(BATCH[(plus, S)]).wait_recv()
            hf(BATCH[(minus, O)]).wait_recv()
            hf(BATCH[(plus, B)]).wait_recv()

        def partner_copy(n, d):
            return remote(pp.at[n % 2, d], db.at[n % 2, d], pp_s.at[n % 2, d], db_r.at[n % 2, d], dev_p)

        def ring_copy(slot, d, k, j):
            return remote(sb.at[slot, d], rb.at[d, k, j], rs_s.at[slot, d], rs_r.at[d, k, j], (dev_xp, dev_xm)[d])

        def out_copies(slot, k):
            cols = out_ref.at[:, pl.ds(pl.multiple_of(colb + k * cw, cw), cw)]
            return (
                pltpu.make_async_copy(fb.at[slot, 0], cols, ol.at[slot]),
                remote(fb.at[slot, 1], cols, of_s.at[slot], of_r.at[k], dev_a),
            )

        def make(n):
            k, j = look_up([u[0] for u in UNITS], n), look_up([u[1] for u in UNITS], n)
            xs, ys = blocks(j)
            for at in range(units):
                new_chunk = UNITS[at][0] not in [u[0] for u in UNITS[:at]]
                first = at in FIRST_STEP.values()
                if (not first and SEND_MAKE[at]) or new_chunk:
                    @pl.when(n == at)
                    def _(at=at, new_chunk=new_chunk, first=first):
                        if not first:
                            send(SEND_MAKE[at], load_w)
                        if new_chunk:
                            pltpu.make_async_copy(w_ref.at[UNITS[at][0]], w_ref.at[UNITS[at][0]], wl.at[UNITS[at][0]]).wait()
            for d in (0, 1):
                for rel in (0, 1):
                    gate = metav[lin(xs[d], ys[d], either(rel)), 1:2, :]
                    gc[:, 2 * d + rel] = jnp.transpose(jnp.broadcast_to(gate, (lane, pairs))).reshape(el, per, lane)
            for copy in h_loads(n, j):
                copy.wait()

            @pl.when(n == 0)
            def _():
                later = [action for action in SEND_END + SEND_MAKE[0] if action[0] == 'lw' and action[1] != UNITS[0][0]]
                send(later, load_w)

            for e in range(el):
                low, high = window(e)
                parts = []
                for q in (S, A, B, O):
                    parts.append(hv[n % 2, q, e].reshape(4 * per, LANES))
                    for at in range(low, high, 128):
                        parts.append(hv[n % 2, q, whole + at // LANES, :, :, at % LANES:at % LANES + 128].reshape(4 * per, 128))
                size = 4 * (LANES + high - low)
                o = jnp.dot(jnp.concatenate(parts, axis=1), wv[k, offset(e, S):offset(e, S) + size], preferred_element_type=F32)
                g = gc[e].reshape(4 * per, lane)
                v = o * jnp.concatenate([g] * (cw // lane), axis=1)
                hi = v.astype(BF16)
                over = v - hi.astype(F32)
                mid = over.astype(BF16)
                low_part = (over - mid.astype(F32)).astype(BF16)
                o3[:, 0, e] = hi.reshape(4, per, cw)
                o3[:, 1, e] = mid.reshape(4, per, cw)
                o3[:, 2, e] = low_part.reshape(4, per, cw)

            @pl.when(n >= 2)
            def _():
                for d in (0, 1):
                    partner_copy(n - 2, d).wait_send()
                pl.semaphore_wait(credit, 1)

            for rel in (1, 0):
                for d in (0, 1):
                    hot = one_hot(lin(xs[d], ys[d], either(rel)))
                    total = jnp.dot(hot, o3[2 * d + rel, 0].reshape(pairs, cw), preferred_element_type=F32)
                    total += jnp.dot(hot, o3[2 * d + rel, 1].reshape(pairs, cw), preferred_element_type=F32)
                    total += jnp.dot(hot, o3[2 * d + rel, 2].reshape(pairs, cw), preferred_element_type=F32)
                    if rel == 1:
                        pp[n % 2, d] = total
                        partner_copy(n, d).start()
                    else:
                        pb[n % 2, d] = total

        def join(n):
            k, j = look_up([u[0] for u in UNITS], n), look_up([u[1] for u in UNITS], n)
            count = look_up([sum(1 for m in SENDS if m < at) for at in range(units)], n)
            slot = count % 4
            for at in range(units):
                if SEND_JOIN[at]:
                    @pl.when(n == at)
                    def _(at=at):
                        send(SEND_JOIN[at], load_w)
            for d in (0, 1):
                partner_copy(n, d).wait_recv()

            @pl.when((j < 3) & (count >= 4))
            def _():
                for d in (0, 1):
                    ring_copy(slot, d, k, 0).wait_send()

            for d in (0, 1):
                @pl.when(j == 0)
                def _():
                    sb[slot, d] = pb[n % 2, d] + db[n % 2, d]

                @pl.when((j > 0) & (j < 3))
                def _():
                    ring_copy(slot, d, k, j - 1).wait_recv()
                    sb[slot, d] = pb[n % 2, d] + db[n % 2, d] + rb[d, k, j - 1]

                @pl.when(j < 3)
                def _():
                    ring_copy(slot, d, k, j).start()

            for order, at in enumerate(FINALS):
                @pl.when(n == at)
                def _(order=order, at=at):
                    kk = UNITS[at][0]
                    if order >= 2:
                        local, away = out_copies(order % 2, kk)
                        local.wait()
                        away.wait_send()
                    local, away = out_copies(order % 2, kk)
                    for d in (1, 0):
                        ring_copy(0, d, kk, 2).wait_recv()
                        fb[order % 2, d] = (pb[at % 2, d] + db[at % 2, d] + rb[d, kk, 2]).astype(BF16)
                        (local, away)[d].start()

            @pl.when(n < units - 2)
            def _():
                pl.semaphore_signal(credit, inc=1, device_id=dev_p, device_id_type=MESH)

        send([action for action in SEND_MAKE[0] if action[0] != 'lw'])
        load_w(UNITS[0][0])
        first_use(UNITS[0][1])
        for copy in h_loads(0, UNITS[0][1]):
            copy.start()
        seen = [int(at + 1 < units and FIRST_STEP[UNITS[at + 1][1]] <= at) for at in range(units)]

        def operation(at, carry):
            n = look_up([o[1] for o in ORDER], at)

            @pl.when(look_up([o[0] for o in ORDER], at) == 0)
            def _():
                for step, first in FIRST_STEP.items():
                    if first > 0:
                        @pl.when(n == first)
                        def _(step=step, first=first):
                            send(SEND_MAKE[first], load_w)
                            first_use(step)
                            for copy in h_loads(first, step):
                                copy.start()

                make(n)

                @pl.when(look_up(seen, n) == 1)
                def _():
                    for copy in h_loads(n + 1, look_up([u[1] for u in UNITS[1:]], n)):
                        copy.start()

            @pl.when(look_up([o[0] for o in ORDER], at) == 1)
            def _():
                join(n)

            return carry

        lax.fori_loop(0, len(ORDER), operation, 0)
        for d in (0, 1):
            for n in (units - 2, units - 1):
                partner_copy(n, d).wait_send()
            for slot in range(4):
                ring_copy(slot, d, 0, 0).wait_send()
        for slot in (0, 1):
            local, away = out_copies(slot, 0)
            local.wait()
            away.wait_send()
        all_sent()
        for k in range(kc):
            out_copies(0, k)[1].wait_recv()

    lane = min(128, cw)
    send([action for action in SEND_END if action[0] != 'lw'])

    pl.run_scoped(
        phase_two,
        pltpu.VMEM((kc, deep, cw), BF16),
        pltpu.VMEM((2, 4, h_ref.shape[4], 4, per, LANES), BF16),
        pltpu.VMEM((el, 4, per, lane), F32),
        pltpu.VMEM((4, 3, el, per, cw), BF16),
        pltpu.VMEM((2, 2, rows, cw), F32),
        pltpu.VMEM((2, 2, rows, cw), F32),
        pltpu.VMEM((4, 2, rows, cw), F32),
        pltpu.VMEM((2, 2, rows, cw), BF16),
        pltpu.SemaphoreType.DMA((kc,)),
        pltpu.SemaphoreType.DMA((2, 4, 4)),
        pltpu.SemaphoreType.DMA((2, 2)),
        pltpu.SemaphoreType.DMA((4, 2)),
        pltpu.SemaphoreType.DMA((2,)),
        pltpu.SemaphoreType.DMA((2,)),
    )


def solution(mesh):
    ny, eps = mesh.shape['tp'], mesh.shape['ep']
    nx = eps // 2
    row_spec = P(('dp', 'ep', 'tp'), None)
    w_in_spec = P('ep', None, 'tp')
    w_out_spec = P('ep', 'tp', None)

    def local_moe(x, ids, gates, w_gate, w_up, w_down):
        rows, width = x.shape
        el, _, ff = w_gate.shape
        experts = el * eps
        per = rows * ids.shape[1] // experts
        pairs = el * per
        cw = width // 2 // CHUNKS
        hbm = pl.BlockSpec(memory_space=pl.ANY)
        vmem = pl.BlockSpec(memory_space=pltpu.VMEM)
        dma = pltpu.SemaphoreType.DMA
        outs = pl.pallas_call(
            functools.partial(moe_kernel, nx, ny),
            name='moe_kernel',
            out_shape=[
                jax.ShapeDtypeStruct((rows, width), BF16),
                jax.ShapeDtypeStruct((nx, ny, 2, rows, width), BF16),
                jax.ShapeDtypeStruct((ny, nx, ny, 2, el * ff // LANES, per, LANES), BF16),
                jax.ShapeDtypeStruct((CHUNKS, ny, el, ff, cw), BF16),
            ],
            in_specs=[hbm, vmem, vmem, hbm, hbm, hbm],
            out_specs=[hbm] * 4,
            scratch_shapes=[
                pltpu.VMEM((ny * eps, 8, pairs), F32),
                pltpu.VMEM((eps, 8, pairs), F32),
                pltpu.VMEM((experts, rows), F32),
                pltpu.VMEM((experts, rows), F32),
                pltpu.VMEM((2, CHUNKS, 3, rows, cw), F32),
                pltpu.VMEM((2, 2, rows, cw), F32),
                dma((ny * eps,)), dma((ny * eps,)),
                dma((4,)), dma((4,)),
                dma((4, 6)), dma((4, 6)),
                dma((4, 4)), dma((4, 4)), dma((4,)), dma((4,)),
                dma((16,)), dma((16,)), dma((16,)), dma((16,)),
            ] + [dma((CHUNKS, PIECES))] * 6 + [
                dma((2, CHUNKS, 3)), dma((2, 2)), dma((CHUNKS,)),
                pltpu.SemaphoreType.REGULAR,
            ],
            compiler_params=pltpu.CompilerParams(collective_id=0, has_side_effects=True, vmem_limit_bytes=67 * 1000 * 1000),
        )(x, ids.T, gates.T, jnp.transpose(w_gate, (0, 2, 1)), jnp.transpose(w_up, (0, 2, 1)), w_down)
        return outs[0]

    return jax.shard_map(
        local_moe, mesh=mesh, in_specs=(row_spec, row_spec, row_spec, w_in_spec, w_in_spec, w_out_spec),
        out_specs=row_spec, check_vma=False)
```

```python
import functools

import jax
import jax.numpy as jnp
from jax import lax
from jax.experimental import pallas as pl
from jax.experimental.pallas import tpu as pltpu
from jax.sharding import PartitionSpec as P

MESH = pl.DeviceIdType.MESH
CHUNKS = 4
LANES = 256
PIECES = 2
BF16 = jnp.bfloat16
F32 = jnp.float32

S, A, B, O = 0, 1, 2, 3

UNITS = ((1, 0), (0, 0), (2, 0), (0, 1), (2, 1), (1, 1), (0, 2), (3, 0), (2, 2), (3, 1), (1, 2), (2, 3), (3, 2), (0, 3), (1, 3), (3, 3), )
ORDER = ((0, 0), (1, 0), (0, 1), (1, 1), (0, 2), (0, 3), (1, 2), (0, 4), (1, 3), (1, 4), (0, 5), (1, 5), (0, 6), (0, 7), (1, 6), (0, 8), (1, 7), (0, 9), (1, 8), (0, 10), (1, 9), (0, 11), (1, 10), (0, 12), (1, 11), (0, 13), (1, 12), (0, 14), (1, 13), (0, 15), (1, 14), (1, 15), )
OPPOSITE_VIA_A = 4
OPPOSITE = (2,)
SEND_START = (('wa', 2, 1), ('wb', 2, 0), ('wb', 0, 0), ('wb', 1, 0), ('wb', 1, 1), )
SEND_BEFORE = (
    (),
    (),
    (('hd', 1), ('wa', 1, 1), ('wa', 0, 1), ('wa', 0, 0), ('wa', 2, 0), ('wa', 1, 0), ('wa', 3, 0), ),
    (('wf', 2, 1), ('wb', 2, 1), ('wb', 0, 1), ),
    (),
    (),
    (('wf', 1, 1), ),
    (),
    (('hd', 7), ),
    (('hd', 8), ('wf', 0, 0), ('wf', 0, 1), ),
    (),
    (('hf', 8), ('hf', 7), ('hd', 5), ),
    (('hd', 11), ('hd', 10), ('wf', 1, 0), ('wf', 2, 0), ),
    (),
    (('hf', 11), ),
    (('hd', 14), ),
)
SEND_AFTER = (
    (),
    (),
    (),
    (),
    (),
    (),
    (),
    (),
    (),
    (),
    (),
    (),
    (),
    (),
    (('hf', 10), ('hd', 13), ('hd', 12), ),
    (),
)
SEND_END = (('hd', 15), ('wb', 3, 1), ('wf', 3, 0), ('wb', 3, 0), ('lw', 0), ('lw', 1), ('lw', 2), )
SEND_MAKE = (
    (),
    (('hf', 15), ('wa', 3, 1), ('hd', 2), ('hd', 4), ('hd', 3), ('hd', 0), ),
    (),
    (),
    (),
    (),
    (),
    (('lw', 3), ),
    (('hf', 6), ),
    (),
    (),
    (),
    (),
    (),
    (),
    (),
)
SEND_JOIN = (
    (('hf', 14), ),
    (),
    (),
    (),
    (('wf', 3, 1), ('hd', 6), ('hd', 9), ),
    (),
    (),
    (),
    (('hf', 9), ),
    (),
    (),
    (),
    (),
    (),
    (),
    (),
)


def order_of(i):
    last, r = i // 12, i % 3
    return (1 - last) * (r + r // 2) + 2 * last, (1 - last) * (i // 3) + last * (i - 12)


BATCH = {order_of(i): i for i in range(16)}
FIRST_STEP = {}
for place_in_order, (chunk_of, step_of) in enumerate(UNITS):
    FIRST_STEP.setdefault(step_of, place_in_order)
SENDS = [n for n, (_, j) in enumerate(UNITS) if j < 3]
FINALS = [n for n, (_, j) in enumerate(UNITS) if j == 3]


def place(y, q):
    high, low = y // 2, y % 2
    return 2 * ((high + q // 2) % 2) + (low + (q + 1) // 2) % 2


def look_up(table, n):
    value = jnp.int32(table[0])
    for at in range(1, len(table)):
        if table[at] != table[0]:
            value = jnp.where(n == at, table[at], value)
    return value


def routing_tables(ids_ref, gate_ref, meta_ref, slot_ref, weight_ref, per):
    top, rows = ids_ref.shape
    experts = slot_ref.shape[0]
    devices, _, pairs = meta_ref.shape
    group = experts // devices
    expert = lax.broadcasted_iota(jnp.int32, (experts, rows), 0)
    chosen = jnp.zeros((experts, rows), F32)
    weight = jnp.zeros((experts, rows), F32)
    for j in range(top):
        here = expert == ids_ref[j:j + 1, :]
        chosen = jnp.where(here, 1.0, chosen)
        weight = jnp.where(here, gate_ref[j:j + 1, :], weight)
    earlier = lax.broadcasted_iota(jnp.int32, (rows, rows), 0) < lax.broadcasted_iota(jnp.int32, (rows, rows), 1)
    rank = jnp.dot(chosen.astype(BF16), earlier.astype(F32).astype(BF16), preferred_element_type=F32)
    slot_ref[...] = jnp.where(chosen > 0.0, rank, -1.0)
    weight_ref[...] = weight
    lane = lax.broadcasted_iota(jnp.int32, (group, pairs), 1)
    sub = lax.broadcasted_iota(jnp.int32, (group, pairs), 0)
    mine = ((lane >= sub * per) & (lane < (sub + 1) * per)).astype(F32).astype(BF16)
    place_in_expert = lax.broadcasted_iota(jnp.int32, (rows, pairs), 1)
    for m in range(1, group):
        place_in_expert = jnp.where(lax.broadcasted_iota(jnp.int32, (rows, pairs), 1) >= m * per,
                                    lax.broadcasted_iota(jnp.int32, (rows, pairs), 1) - m * per, place_in_expert)
    place_in_expert = place_in_expert.astype(F32)
    row = lax.broadcasted_iota(jnp.int32, (8, rows), 1)
    high = (row // 2).astype(F32).astype(BF16)
    low = (row % 2).astype(F32).astype(BF16)
    top_row = lax.broadcasted_iota(jnp.int32, (8, pairs), 0)

    def spread(part):
        return lax.dot_general(part, mine, (((0,), (0,)), ((), ())), preferred_element_type=F32)

    def table(d, carry):
        at = pl.ds(pl.multiple_of(d * group, group), group)
        hit = (spread(slot_ref[at, :].astype(BF16)) == place_in_expert).astype(F32)
        hot = hit.astype(BF16)
        position = 2.0 * jnp.dot(high, hot, preferred_element_type=F32) + jnp.dot(low, hot, preferred_element_type=F32)
        w = weight_ref[at, :]
        first = w.astype(BF16)
        over = w - first.astype(F32)
        second = over.astype(BF16)
        third = (over - second.astype(F32)).astype(BF16)
        value = jnp.sum((spread(first) + spread(second) + spread(third)) * hit, axis=0, keepdims=True)
        meta_ref[d] = jnp.where(top_row == 0, position, jnp.broadcast_to(value, (8, pairs)))
        return carry

    lax.fori_loop(0, devices, table, 0)


def moe_kernel(nx, ny, x_ref, ids_ref, gate_ref, wg_ref, wu_ref, wd_ref, out_ref, tok_ref, h_ref, w_ref,
               metav, meta_ref, slot_ref, weight_ref, rb, db, ms, mr, ty_s, ty_r, tx_s, tx_r, td_s, td_r, room, o3, hd_s, hd_r, hf_s, hf_r,
               wa_s, wa_r, wb_s, wb_r, wf_s, wf_r, rs_r, db_r, of_r, credit):
    rows, width = x_ref.shape
    half = rows // 2
    el, ff, _ = wg_ref.shape
    per = h_ref.shape[5]
    rest = ff - LANES * (ff // LANES)
    whole = el * (ff // LANES)
    assert ff // LANES == 1 and (el * rest) % LANES == 0 and rest <= 128
    pairs = el * per
    kc, cw = w_ref.shape[0], w_ref.shape[4]
    ep_piece = el // PIECES
    eps = 2 * nx
    y = lax.axis_index('tp')
    ep = lax.axis_index('ep')
    x, c = ep // 2, ep % 2
    ya, yb, yo = place(y, A), place(y, B), place(y, O)
    yq = (y, ya, yb, yo)
    xp, xm = (x + 1) % nx, (x + nx - 1) % nx
    colb = ((y + y // 2) % 2) * (kc * cw)
    cola = ((ya + ya // 2) % 2) * (kc * cw)
    me = y * eps + ep

    dev_a = {'tp': ya, 'ep': ep}
    dev_b = {'tp': yb, 'ep': ep}
    dev_p = {'tp': y, 'ep': 2 * x + 1 - c}
    dev_xp = {'tp': y, 'ep': 2 * xp + c}
    dev_xm = {'tp': y, 'ep': 2 * xm + c}

    def remote(src, dst, send, recv, dev):
        return pltpu.make_async_remote_copy(src_ref=src, dst_ref=dst, send_sem=send, recv_sem=recv, device_id=dev, device_id_type=MESH)

    def lin(xs, ys, cs):
        return ys * eps + 2 * xs + cs

    def either(rel):
        return c if rel == 0 else 1 - c

    barrier = pltpu.get_barrier_semaphore()

    def peer_of(d):
        other = (me + d) % (ny * eps)
        return other // eps, other % eps

    def greet(d, carry):
        py, pe = peer_of(d)
        pl.semaphore_signal(barrier, inc=1, device_id={'tp': py, 'ep': pe}, device_id_type=MESH)
        return carry

    lax.fori_loop(1, ny * eps, greet, 0)
    pl.semaphore_wait(barrier, ny * eps - 1)

    def meta_copy(d):
        py, pe = peer_of(d)
        return remote(meta_ref.at[pe], metav.at[me], ms.at[d], mr.at[me], {'tp': py, 'ep': pe})

    def meta_send(d, carry):
        meta_copy(d).start()
        return carry

    def own(dxm, q):
        return tok_ref.at[(x + dxm) % nx, yq[q], c]

    def rows_of(ref, part, cut=None):
        cut = half if cut is None else cut
        return ref.at[pl.ds(part * cut, (cut, rows - cut)[part])]

    def ty(n):
        if n < 2:
            return remote(x_ref, tok_ref.at[x, y, c], ty_s.at[n], ty_r.at[n], (dev_a, dev_b)[n])
        block = rows_of(own(0, (B, A)[n - 2]), n - 2, rows * OPPOSITE_VIA_A // 4)
        return remote(block, block, ty_s.at[n], ty_r.at[n], (dev_a, dev_b)[n - 2])

    def tx(q, n):
        if n < 2:
            return remote(x_ref if q == S else own(0, q), own(0, q), tx_s.at[q, n], tx_r.at[q, n], (dev_xp, dev_xm)[n])
        block = rows_of(own((3, 1)[n - 2], q), n - 2)
        return remote(block, block, tx_s.at[q, n], tx_r.at[q, n], (dev_xp, dev_xm)[n - 2])


    def wa(k, g):
        src = wd_ref.at[pl.ds(g * ep_piece, ep_piece), :, pl.ds(pl.multiple_of(cola + k * cw, cw), cw)]
        return remote(src, w_ref.at[k, y, pl.ds(g * ep_piece, ep_piece)], wa_s.at[k, g], wa_r.at[k, g], dev_a)

    def wb(k, g):
        src = wd_ref.at[pl.ds(g * ep_piece, ep_piece), :, pl.ds(pl.multiple_of(colb + k * cw, cw), cw)]
        return remote(src, w_ref.at[k, y, pl.ds(g * ep_piece, ep_piece)], wb_s.at[k, g], wb_r.at[k, g], dev_b)

    def wf(k, g):
        block = w_ref.at[k, ya, pl.ds(g * ep_piece, ep_piece)]
        return remote(block, block, wf_s.at[k, g], wf_r.at[k, g], dev_b)

    def hd(i):
        dxm, q = order_of(i)
        block = h_ref.at[y, (x + dxm) % nx, yq[q]]
        return remote(block, block, hd_s.at[i], hd_r.at[i], dev_a if q < 2 else dev_b)

    def hf(i):
        dxm, q = order_of(i)
        block = h_ref.at[yb, (x + dxm) % nx, place(yb, q)]
        return remote(block, block, hf_s.at[i], hf_r.at[i], dev_a)

    def send(actions, load_w=None):
        for action in actions:
            kind, at = action[0], action[1:]
            if kind == 'wf':
                wa(*at).wait_recv()
            if kind == 'hf':
                hd(*at).wait_recv()
            if kind == 'lw':
                load_w(*at)
            else:
                {'wa': wa, 'wb': wb, 'wf': wf, 'hd': hd, 'hf': hf}[kind](*at).start()

    for n in (0, 1):
        ty(n).start()
        tx(S, n).start()
    routing_tables(ids_ref, gate_ref, meta_ref, slot_ref, weight_ref, per)
    lax.fori_loop(1, ny * eps, meta_send, 0)
    metav[me] = meta_ref[ep]
    send(SEND_START)

    def came(q):
        for n in (0, 1):
            tx(q, n).wait_recv()

    def both(q, first):
        tx(q, first).start()
        tx(q, first + 1).start()

    def comm(step):
        if step == 1:
            ty(0).wait_recv()
            ty(1).wait_recv()
            for n in OPPOSITE:
                ty(n).start()
            both(A, 0)
            both(B, 0)
            came(S)
        if step == 4:
            came(A)
            for n in OPPOSITE:
                ty(n).wait_recv()
            both(O, 0)
            both(S, 2)
            both(A, 2)
        if step in (7, 10):
            q = {7: B, 10: O}[step]
            came(q)
            both(q, 2)
        if step >= 12:
            tx(step - 12, 2).wait_recv()
            tx(step - 12, 3).wait_recv()

    row_id = lax.broadcasted_iota(jnp.int32, (rows, pairs), 0)

    def one_hot(src):
        pos = metav[src, 0:1, :].astype(jnp.int32)
        return (row_id == pos).astype(F32).astype(BF16)

    def meta_wait(src):
        remote(meta_ref.at[0], metav.at[src], ms.at[0], mr.at[src], dev_p).wait_recv()

    def phase_one(wg, wu, tb, xg, hb, left, wl, tl, hl):
        load_g = pltpu.make_async_copy(wg_ref, wg, wl.at[0])
        load_u = pltpu.make_async_copy(wu_ref, wu, wl.at[1])
        load_g.start()
        load_u.start()

        def store(i):
            dxm, q = order_of(i)
            return pltpu.make_async_copy(hb, h_ref.at[y, (x + dxm) % nx, place(y, q)], hl.at[0])

        def to_partner(m):
            return remote(tb.at[:, pl.ds(m * cw, cw)], o3.at[pl.ds(m * rows, rows)], td_s.at[m], td_r.at[m], dev_p)

        def batch(i, carry):
            @pl.when(i > 0)
            def _():
                store(i - 1).wait()

            for step in range(1, 16):
                if SEND_BEFORE[step] or SEND_AFTER[step] or step in (1, 4, 7, 10) or step >= 12:
                    @pl.when(i == step)
                    def _(step=step):
                        send(SEND_BEFORE[step])
                        comm(step)
                        send(SEND_AFTER[step])

            dxm, q = order_of(i)
            xs, ys = (x + dxm) % nx, place(y, q)
            mine = pltpu.make_async_copy(x_ref, tb, tl.at[0])
            arrived = pltpu.make_async_copy(tok_ref.at[xs, ys, c], tb, tl.at[0])

            @pl.when(i > 0)
            def _():
                for m in range(width // cw):
                    to_partner(m).wait_send()

            @pl.when(i == 0)
            def _():
                mine.start()

            @pl.when(i > 0)
            def _():
                arrived.start()
                pl.semaphore_wait(room, 1)
                meta_wait(lin(xs, ys, c))

            arrived.wait()
            for m in range(width // cw):
                to_partner(m).start()
            hot = one_hot(lin(xs, ys, c))
            step = min(512, width)
            for lo in range(0, width, step):
                got = lax.dot_general(hot, tb[:, lo:lo + step], (((0,), (0,)), ((), ())), preferred_element_type=F32)
                xg[:, 0, :, lo:lo + step] = got.astype(BF16).reshape(el, per, step)
            meta_wait(lin(xs, ys, 1 - c))
            hot = one_hot(lin(xs, ys, 1 - c))
            for m in range(width // cw):
                to_partner(m).wait_recv()
                got = lax.dot_general(hot, o3[m * rows:(m + 1) * rows, :], (((0,), (0,)), ((), ())), preferred_element_type=F32)
                xg[:, 1, :, m * cw:(m + 1) * cw] = got.astype(BF16).reshape(el, per, cw)

            @pl.when(i < 15)
            def _():
                pl.semaphore_signal(room, inc=1, device_id=dev_p, device_id_type=MESH)

            @pl.when(i == 0)
            def _():
                load_g.wait()
                load_u.wait()

            for e in range(el):
                lhs = xg[e].reshape(2 * per, width)
                a = lax.dot_general(lhs, wg[e], (((1,), (1,)), ((), ())), preferred_element_type=F32)
                b = lax.dot_general(lhs, wu[e], (((1,), (1,)), ((), ())), preferred_element_type=F32)
                hid = a * jax.nn.sigmoid(a) * b
                for s in (0, 1):
                    hb[either(s), e] = hid[s * per:(s + 1) * per, :LANES].astype(BF16)
                left[e] = hid[:, LANES:]
            packed = jnp.concatenate([left[e] for e in range(el)], axis=1).astype(BF16)
            for m in range(el * rest // LANES):
                for s in (0, 1):
                    hb[either(s), whole + m] = packed[s * per:(s + 1) * per, m * LANES:(m + 1) * LANES]
            store(i).start()
            return carry

        lax.fori_loop(0, 16, batch, 0)
        for m in range(width // cw):
            to_partner(m).wait_send()
        store(15).wait()

    pl.run_scoped(
        phase_one,
        pltpu.VMEM((el, ff, width), BF16),
        pltpu.VMEM((el, ff, width), BF16),
        pltpu.VMEM((rows, width), BF16),
        pltpu.VMEM((el, 2, per, width), BF16),
        pltpu.VMEM((2,) + h_ref.shape[4:], BF16),
        pltpu.VMEM((el, 2 * per, rest), F32),
        pltpu.SemaphoreType.DMA((2,)),
        pltpu.SemaphoreType.DMA((2,)),
        pltpu.SemaphoreType.DMA((1,)),
    )

    def all_sent():
        def meta_done(d, carry):
            meta_copy(d).wait_send()
            return carry

        lax.fori_loop(1, ny * eps, meta_done, 0)
        for n in (0, 1) + OPPOSITE:
            ty(n).wait_send()
        for q in (S, A, B, O):
            for n in range(4):
                tx(q, n).wait_send()
        for k in range(kc):
            for g in range(PIECES):
                wa(k, g).wait_send()
                wb(k, g).wait_send()
                wf(k, g).wait_send()
        for i in range(16):
            hd(i).wait_send()
            if order_of(i)[1] >= 2:
                hf(i).wait_send()

    def window(e):
        return e * rest // 128 * 128, -(-(e + 1) * rest // 128) * 128

    def offset(e, q):
        before = sum(LANES + window(m)[1] - window(m)[0] for m in range(e))
        return 4 * before + q * (LANES + window(e)[1] - window(e)[0])

    deep = offset(el, S)

    units = len(UNITS)

    def phase_two(wv, hv, gc, pb, pp, sb, fb, wl, hvl, pp_s, rs_s, of_s, ol):
        lane = gc.shape[3]

        def clear(k):
            for e in range(el):
                low, high = window(e)
                for q in (S, A, B, O):
                    at = offset(e, q) + LANES
                    for start, stop in ((0, e * rest - low), ((e + 1) * rest - low, high - low)):
                        if stop > start:
                            wv[k, at + start:at + stop] = jnp.zeros((stop - start, cw), BF16)

        def blocks(j):
            return ((x + 2 * nx - 1 - j) % nx, (x + 1 + j) % nx), (y, ya)

        def w_loads(k):
            copies = []
            for q in (S, A, B, O):
                for e in range(el):
                    if q == S:
                        src = wd_ref.at[e, :, pl.ds(pl.multiple_of(colb + k * cw, cw), cw)]
                    else:
                        src = w_ref.at[k, yq[q], e]
                    low, high = window(e)
                    at = offset(e, q)
                    copies.append(pltpu.make_async_copy(src.at[pl.ds(0, LANES)], wv.at[k, pl.ds(at, LANES)], wl.at[k]))
                    copies.append(pltpu.make_async_copy(
                        src.at[pl.ds(LANES, rest)], wv.at[k, pl.ds(at + LANES + e * rest - low, rest)], wl.at[k]))
            return copies

        def load_w(k):
            for g in range(PIECES):
                wb(k, g).wait_recv()
                wf(k, g).wait_recv()
            for copy in w_loads(k):
                copy.start()
            clear(k)

        def h_loads(n, j):
            xs, ys = blocks(j)
            copies = []
            for d in (0, 1):
                for rel in (0, 1):
                    for q in (S, A, B, O):
                        copies.append(pltpu.make_async_copy(
                            h_ref.at[yq[q], xs[d], ys[d], either(rel)], hv.at[n % 2, q, :, 2 * d + rel], hvl.at[n % 2, q, 2 * d + rel]))
            return copies

        def first_use(j):
            minus, plus = (3 - j) % 4, (1 + j) % 4
            hd(BATCH[(minus, A)]).wait_recv()
            hd(BATCH[(plus, S)]).wait_recv()
            hf(BATCH[(minus, O)]).wait_recv()
            hf(BATCH[(plus, B)]).wait_recv()

        def partner_copy(n, d):
            return remote(pp.at[n % 2, d], db.at[n % 2, d], pp_s.at[n % 2, d], db_r.at[n % 2, d], dev_p)

        def ring_copy(slot, d, k, j):
            return remote(sb.at[slot, d], rb.at[d, k, j], rs_s.at[slot, d], rs_r.at[d, k, j], (dev_xp, dev_xm)[d])

        def out_copies(slot, k):
            cols = out_ref.at[:, pl.ds(pl.multiple_of(colb + k * cw, cw), cw)]
            return (
                pltpu.make_async_copy(fb.at[slot, 0], cols, ol.at[slot]),
                remote(fb.at[slot, 1], cols, of_s.at[slot], of_r.at[k], dev_a),
            )

        def make(n):
            k, j = look_up([u[0] for u in UNITS], n), look_up([u[1] for u in UNITS], n)
            xs, ys = blocks(j)
            for at in range(units):
                new_chunk = UNITS[at][0] not in [u[0] for u in UNITS[:at]]
                first = at in FIRST_STEP.values()
                if (not first and SEND_MAKE[at]) or new_chunk:
                    @pl.when(n == at)
                    def _(at=at, new_chunk=new_chunk, first=first):
                        if not first:
                            send(SEND_MAKE[at], load_w)
                        if new_chunk:
                            pltpu.make_async_copy(w_ref.at[UNITS[at][0]], w_ref.at[UNITS[at][0]], wl.at[UNITS[at][0]]).wait()
            for d in (0, 1):
                for rel in (0, 1):
                    gate = metav[lin(xs[d], ys[d], either(rel)), 1:2, :]
                    gc[:, 2 * d + rel] = jnp.transpose(jnp.broadcast_to(gate, (lane, pairs))).reshape(el, per, lane)
            for copy in h_loads(n, j):
                copy.wait()

            @pl.when(n == 0)
            def _():
                later = [action for action in SEND_END + SEND_MAKE[0] if action[0] == 'lw' and action[1] != UNITS[0][0]]
                send(later, load_w)

            for e in range(el):
                low, high = window(e)
                parts = []
                for q in (S, A, B, O):
                    parts.append(hv[n % 2, q, e].reshape(4 * per, LANES))
                    for at in range(low, high, 128):
                        parts.append(hv[n % 2, q, whole + at // LANES, :, :, at % LANES:at % LANES + 128].reshape(4 * per, 128))
                size = 4 * (LANES + high - low)
                o = jnp.dot(jnp.concatenate(parts, axis=1), wv[k, offset(e, S):offset(e, S) + size], preferred_element_type=F32)
                g = gc[e].reshape(4 * per, lane)
                v = o * jnp.concatenate([g] * (cw // lane), axis=1)
                hi = v.astype(BF16)
                over = v - hi.astype(F32)
                mid = over.astype(BF16)
                low_part = (over - mid.astype(F32)).astype(BF16)
                for m in range(4):
                    for third, value in enumerate((hi, mid, low_part)):
                        at = (3 * m + third) * pairs + e * per
                        o3[at:at + per, :] = value[m * per:(m + 1) * per]

            @pl.when(n >= 2)
            def _():
                for d in (0, 1):
                    partner_copy(n - 2, d).wait_send()
                pl.semaphore_wait(credit, 1)

            for rel in (1, 0):
                for d in (0, 1):
                    hot = one_hot(lin(xs[d], ys[d], either(rel)))
                    at = 3 * (2 * d + rel) * pairs
                    total = jnp.dot(hot, o3[at:at + pairs, :], preferred_element_type=F32)
                    total += jnp.dot(hot, o3[at + pairs:at + 2 * pairs, :], preferred_element_type=F32)
                    total += jnp.dot(hot, o3[at + 2 * pairs:at + 3 * pairs, :], preferred_element_type=F32)
                    if rel == 1:
                        pp[n % 2, d] = total
                        partner_copy(n, d).start()
                    else:
                        pb[n % 2, d] = total

        def join(n):
            k, j = look_up([u[0] for u in UNITS], n), look_up([u[1] for u in UNITS], n)
            count = look_up([sum(1 for m in SENDS if m < at) for at in range(units)], n)
            slot = count % 4
            for at in range(units):
                if SEND_JOIN[at]:
                    @pl.when(n == at)
                    def _(at=at):
                        send(SEND_JOIN[at], load_w)
            for d in (0, 1):
                partner_copy(n, d).wait_recv()

            @pl.when((j < 3) & (count >= 4))
            def _():
                for d in (0, 1):
                    ring_copy(slot, d, k, 0).wait_send()

            for d in (0, 1):
                @pl.when(j == 0)
                def _():
                    sb[slot, d] = pb[n % 2, d] + db[n % 2, d]

                @pl.when((j > 0) & (j < 3))
                def _():
                    ring_copy(slot, d, k, j - 1).wait_recv()
                    sb[slot, d] = pb[n % 2, d] + db[n % 2, d] + rb[d, k, j - 1]

                @pl.when(j < 3)
                def _():
                    ring_copy(slot, d, k, j).start()

            for order, at in enumerate(FINALS):
                @pl.when(n == at)
                def _(order=order, at=at):
                    kk = UNITS[at][0]
                    if order >= 2:
                        local, away = out_copies(order % 2, kk)
                        local.wait()
                        away.wait_send()
                    local, away = out_copies(order % 2, kk)
                    for d in (1, 0):
                        ring_copy(0, d, kk, 2).wait_recv()
                        fb[order % 2, d] = (pb[at % 2, d] + db[at % 2, d] + rb[d, kk, 2]).astype(BF16)
                        (local, away)[d].start()

            @pl.when(n < units - 2)
            def _():
                pl.semaphore_signal(credit, inc=1, device_id=dev_p, device_id_type=MESH)

        send([action for action in SEND_MAKE[0] if action[0] != 'lw'])
        load_w(UNITS[0][0])
        first_use(UNITS[0][1])
        for copy in h_loads(0, UNITS[0][1]):
            copy.start()
        seen = [int(at + 1 < units and FIRST_STEP[UNITS[at + 1][1]] <= at) for at in range(units)]

        def operation(at, carry):
            n = look_up([o[1] for o in ORDER], at)

            @pl.when(look_up([o[0] for o in ORDER], at) == 0)
            def _():
                for step, first in FIRST_STEP.items():
                    if first > 0:
                        @pl.when(n == first)
                        def _(step=step, first=first):
                            send(SEND_MAKE[first], load_w)
                            first_use(step)
                            for copy in h_loads(first, step):
                                copy.start()

                make(n)

                @pl.when(look_up(seen, n) == 1)
                def _():
                    for copy in h_loads(n + 1, look_up([u[1] for u in UNITS[1:]], n)):
                        copy.start()

            @pl.when(look_up([o[0] for o in ORDER], at) == 1)
            def _():
                join(n)

            return carry

        lax.fori_loop(0, len(ORDER), operation, 0)
        for d in (0, 1):
            for n in (units - 2, units - 1):
                partner_copy(n, d).wait_send()
            for slot in range(4):
                ring_copy(slot, d, 0, 0).wait_send()
        for slot in (0, 1):
            local, away = out_copies(slot, 0)
            local.wait()
            away.wait_send()
        all_sent()
        for k in range(kc):
            out_copies(0, k)[1].wait_recv()

    lane = min(128, cw)
    send([action for action in SEND_END if action[0] != 'lw'])

    pl.run_scoped(
        phase_two,
        pltpu.VMEM((kc, deep, cw), BF16),
        pltpu.VMEM((2, 4, h_ref.shape[4], 4, per, LANES), BF16),
        pltpu.VMEM((el, 4, per, lane), F32),
        pltpu.VMEM((2, 2, rows, cw), F32),
        pltpu.VMEM((2, 2, rows, cw), F32),
        pltpu.VMEM((4, 2, rows, cw), F32),
        pltpu.VMEM((2, 2, rows, cw), BF16),
        pltpu.SemaphoreType.DMA((kc,)),
        pltpu.SemaphoreType.DMA((2, 4, 4)),
        pltpu.SemaphoreType.DMA((2, 2)),
        pltpu.SemaphoreType.DMA((4, 2)),
        pltpu.SemaphoreType.DMA((2,)),
        pltpu.SemaphoreType.DMA((2,)),
    )


def solution(mesh):
    ny, eps = mesh.shape['tp'], mesh.shape['ep']
    nx = eps // 2
    row_spec = P(('dp', 'ep', 'tp'), None)
    w_in_spec = P('ep', None, 'tp')
    w_out_spec = P('ep', 'tp', None)

    def local_moe(x, ids, gates, w_gate, w_up, w_down):
        rows, width = x.shape
        el, _, ff = w_gate.shape
        experts = el * eps
        per = rows * ids.shape[1] // experts
        pairs = el * per
        cw = width // 2 // CHUNKS
        hbm = pl.BlockSpec(memory_space=pl.ANY)
        vmem = pl.BlockSpec(memory_space=pltpu.VMEM)
        dma = pltpu.SemaphoreType.DMA
        outs = pl.pallas_call(
            functools.partial(moe_kernel, nx, ny),
            name='moe_kernel',
            out_shape=[
                jax.ShapeDtypeStruct((rows, width), BF16),
                jax.ShapeDtypeStruct((nx, ny, 2, rows, width), BF16),
                jax.ShapeDtypeStruct((ny, nx, ny, 2, el * ff // LANES, per, LANES), BF16),
                jax.ShapeDtypeStruct((CHUNKS, ny, el, ff, cw), BF16),
            ],
            in_specs=[hbm, vmem, vmem, hbm, hbm, hbm],
            out_specs=[hbm] * 4,
            scratch_shapes=[
                pltpu.VMEM((ny * eps, 8, pairs), F32),
                pltpu.VMEM((eps, 8, pairs), F32),
                pltpu.VMEM((experts, rows), F32),
                pltpu.VMEM((experts, rows), F32),
                pltpu.VMEM((2, CHUNKS, 3, rows, cw), F32),
                pltpu.VMEM((2, 2, rows, cw), F32),
                dma((ny * eps,)), dma((ny * eps,)),
                dma((4,)), dma((4,)),
                dma((4, 4)), dma((4, 4)),
                dma((width // cw,)), dma((width // cw,)), pltpu.SemaphoreType.REGULAR,
                pltpu.VMEM((12 * pairs, cw), BF16),
                dma((16,)), dma((16,)), dma((16,)), dma((16,)),
            ] + [dma((CHUNKS, PIECES))] * 6 + [
                dma((2, CHUNKS, 3)), dma((2, 2)), dma((CHUNKS,)),
                pltpu.SemaphoreType.REGULAR,
            ],
            compiler_params=pltpu.CompilerParams(collective_id=0, has_side_effects=True, vmem_limit_bytes=67 * 1000 * 1000),
        )(x, ids.T, gates.T, jnp.transpose(w_gate, (0, 2, 1)), jnp.transpose(w_up, (0, 2, 1)), w_down)
        return outs[0]

    return jax.shard_map(
        local_moe, mesh=mesh, in_specs=(row_spec, row_spec, row_spec, w_in_spec, w_in_spec, w_out_spec),
        out_specs=row_spec, check_vma=False)
```

```python
import functools

import jax
import jax.numpy as jnp
from jax import lax
from jax.experimental import pallas as pl
from jax.experimental.pallas import tpu as pltpu
from jax.sharding import PartitionSpec as P

MESH = pl.DeviceIdType.MESH
CHUNKS = 4
LANES = 256
PIECES = 2
BF16 = jnp.bfloat16
F32 = jnp.float32

S, A, B, O = 0, 1, 2, 3

UNITS = ((2, 0), (0, 0), (1, 0), (2, 1), (0, 1), (1, 1), (2, 2), (3, 0), (1, 2), (3, 1), (0, 2), (2, 3), (3, 2), (1, 3), (0, 3), (3, 3), )
ORDER = ((0, 0), (1, 0), (0, 1), (0, 2), (1, 1), (1, 2), (0, 3), (0, 4), (1, 3), (0, 5), (1, 4), (0, 6), (1, 5), (1, 6), (0, 7), (0, 8), (1, 7), (0, 9), (1, 8), (0, 10), (1, 9), (0, 11), (1, 10), (0, 12), (1, 11), (0, 13), (1, 12), (0, 14), (1, 13), (0, 15), (1, 14), (1, 15), )
OPPOSITE_VIA_A = 4
OPPOSITE = (2,)
SEND_START = (('wa', 1, 0), ('wa', 2, 1), ('wb', 1, 1), ('wb', 2, 0), ('wb', 0, 1), )
SEND_BEFORE = (
    (),
    (),
    (('hd', 1), ('wa', 0, 0), ),
    (('wf', 1, 0), ('wb', 2, 1), ('wb', 1, 0), ('wb', 0, 0), ),
    (('wf', 2, 1), ),
    (),
    (('hd', 5), ('wa', 2, 0), ('wa', 0, 1), ('wa', 1, 1), ),
    (),
    (('hd', 7), ),
    (('hd', 8), ('wf', 2, 0), ),
    (),
    (('hf', 8), ('hd', 2), ('wf', 0, 1), ),
    (('wf', 1, 1), ('hd', 11), ('hd', 10), ('wf', 0, 0), ),
    (('hd', 12), ('hf', 7), ('wa', 3, 1), ),
    (),
    (('hf', 11), ('hf', 10), ('hd', 13), ('hd', 14), ),
)
SEND_AFTER = (
    (),
    (),
    (),
    (),
    (),
    (),
    (),
    (),
    (),
    (),
    (),
    (),
    (),
    (),
    (),
    (),
)
SEND_END = (('hd', 15), ('wb', 3, 1), ('wf', 3, 1), ('wb', 3, 0), ('lw', 0), ('lw', 1), ('lw', 2), )
SEND_MAKE = (
    (),
    (('hf', 15), ('wa', 3, 0), ('hd', 4), ('hd', 0), ('hd', 3), ),
    (),
    (),
    (),
    (('wf', 3, 0), ('hd', 6), ('hd', 9), ),
    (),
    (('lw', 3), ),
    (('hf', 6), ),
    (),
    (),
    (),
    (),
    (),
    (),
    (),
)
SEND_JOIN = (
    (('hf', 14), ),
    (),
    (),
    (),
    (),
    (),
    (),
    (),
    (('hf', 9), ),
    (),
    (),
    (),
    (),
    (),
    (),
    (),
)


def order_of(i):
    last, r = i // 12, i % 3
    return (1 - last) * (r + r // 2) + 2 * last, (1 - last) * (i // 3) + last * (i - 12)


BATCH = {order_of(i): i for i in range(16)}
AHEAD = (0, 0, 1, 1, 0, 1, 1, 0, 1, 1, 0, 1, 0, 0, 0, 0)
FIRST_STEP = {}
for place_in_order, (chunk_of, step_of) in enumerate(UNITS):
    FIRST_STEP.setdefault(step_of, place_in_order)
SENDS = [n for n, (_, j) in enumerate(UNITS) if j < 3]
FINALS = [n for n, (_, j) in enumerate(UNITS) if j == 3]


def place(y, q):
    high, low = y // 2, y % 2
    return 2 * ((high + q // 2) % 2) + (low + (q + 1) // 2) % 2


def look_up(table, n):
    value = jnp.int32(table[0])
    for at in range(1, len(table)):
        if table[at] != table[0]:
            value = jnp.where(n == at, table[at], value)
    return value


def routing_tables(ids_ref, gate_ref, meta_ref, slot_ref, weight_ref, per):
    top, rows = ids_ref.shape
    experts = slot_ref.shape[0]
    devices, _, pairs = meta_ref.shape
    group = experts // devices
    expert = lax.broadcasted_iota(jnp.int32, (experts, rows), 0)
    chosen = jnp.zeros((experts, rows), F32)
    weight = jnp.zeros((experts, rows), F32)
    for j in range(top):
        here = expert == ids_ref[j:j + 1, :]
        chosen = jnp.where(here, 1.0, chosen)
        weight = jnp.where(here, gate_ref[j:j + 1, :], weight)
    earlier = lax.broadcasted_iota(jnp.int32, (rows, rows), 0) < lax.broadcasted_iota(jnp.int32, (rows, rows), 1)
    rank = jnp.dot(chosen.astype(BF16), earlier.astype(F32).astype(BF16), preferred_element_type=F32)
    slot_ref[...] = jnp.where(chosen > 0.0, rank, -1.0)
    weight_ref[...] = weight
    lane = lax.broadcasted_iota(jnp.int32, (group, pairs), 1)
    sub = lax.broadcasted_iota(jnp.int32, (group, pairs), 0)
    mine = ((lane >= sub * per) & (lane < (sub + 1) * per)).astype(F32).astype(BF16)
    place_in_expert = lax.broadcasted_iota(jnp.int32, (rows, pairs), 1)
    for m in range(1, group):
        place_in_expert = jnp.where(lax.broadcasted_iota(jnp.int32, (rows, pairs), 1) >= m * per,
                                    lax.broadcasted_iota(jnp.int32, (rows, pairs), 1) - m * per, place_in_expert)
    place_in_expert = place_in_expert.astype(F32)
    row = lax.broadcasted_iota(jnp.int32, (8, rows), 1)
    high = (row // 2).astype(F32).astype(BF16)
    low = (row % 2).astype(F32).astype(BF16)
    top_row = lax.broadcasted_iota(jnp.int32, (8, pairs), 0)

    def spread(part):
        return lax.dot_general(part, mine, (((0,), (0,)), ((), ())), preferred_element_type=F32)

    def table(d, carry):
        at = pl.ds(pl.multiple_of(d * group, group), group)
        hit = (spread(slot_ref[at, :].astype(BF16)) == place_in_expert).astype(F32)
        hot = hit.astype(BF16)
        position = 2.0 * jnp.dot(high, hot, preferred_element_type=F32) + jnp.dot(low, hot, preferred_element_type=F32)
        w = weight_ref[at, :]
        first = w.astype(BF16)
        over = w - first.astype(F32)
        second = over.astype(BF16)
        third = (over - second.astype(F32)).astype(BF16)
        value = jnp.sum((spread(first) + spread(second) + spread(third)) * hit, axis=0, keepdims=True)
        meta_ref[d] = jnp.where(top_row == 0, position, jnp.broadcast_to(value, (8, pairs)))
        return carry

    lax.fori_loop(0, devices, table, 0)


def moe_kernel(nx, ny, x_ref, ids_ref, gate_ref, wg_ref, wu_ref, wd_ref, out_ref, tok_ref, h_ref, w_ref,
               metav, meta_ref, slot_ref, weight_ref, rb, db, ms, mr, ty_s, ty_r, tx_s, tx_r, td_s, td_r, room, o3, hd_s, hd_r, hf_s, hf_r,
               wa_s, wa_r, wb_s, wb_r, wf_s, wf_r, rs_r, db_r, of_r, credit):
    rows, width = x_ref.shape
    half = rows // 2
    el, ff, _ = wg_ref.shape
    per = h_ref.shape[5]
    rest = ff - LANES * (ff // LANES)
    whole = el * (ff // LANES)
    assert ff // LANES == 1 and (el * rest) % LANES == 0 and rest <= 128
    pairs = el * per
    kc, cw = w_ref.shape[0], w_ref.shape[4]
    ep_piece = el // PIECES
    eps = 2 * nx
    y = lax.axis_index('tp')
    ep = lax.axis_index('ep')
    x, c = ep // 2, ep % 2
    ya, yb, yo = place(y, A), place(y, B), place(y, O)
    yq = (y, ya, yb, yo)
    xp, xm = (x + 1) % nx, (x + nx - 1) % nx
    colb = ((y + y // 2) % 2) * (kc * cw)
    cola = ((ya + ya // 2) % 2) * (kc * cw)
    me = y * eps + ep

    dev_a = {'tp': ya, 'ep': ep}
    dev_b = {'tp': yb, 'ep': ep}
    dev_p = {'tp': y, 'ep': 2 * x + 1 - c}
    dev_xp = {'tp': y, 'ep': 2 * xp + c}
    dev_xm = {'tp': y, 'ep': 2 * xm + c}

    def remote(src, dst, send, recv, dev):
        return pltpu.make_async_remote_copy(src_ref=src, dst_ref=dst, send_sem=send, recv_sem=recv, device_id=dev, device_id_type=MESH)

    def lin(xs, ys, cs):
        return ys * eps + 2 * xs + cs

    def either(rel):
        return c if rel == 0 else 1 - c

    barrier = pltpu.get_barrier_semaphore()

    def peer_of(d):
        other = (me + d) % (ny * eps)
        return other // eps, other % eps

    def greet(d, carry):
        py, pe = peer_of(d)
        pl.semaphore_signal(barrier, inc=1, device_id={'tp': py, 'ep': pe}, device_id_type=MESH)
        return carry

    lax.fori_loop(1, ny * eps, greet, 0)
    pl.semaphore_wait(barrier, ny * eps - 1)

    def meta_copy(d):
        py, pe = peer_of(d)
        return remote(meta_ref.at[pe], metav.at[me], ms.at[d], mr.at[me], {'tp': py, 'ep': pe})

    def meta_send(d, carry):
        meta_copy(d).start()
        return carry

    def own(dxm, q):
        return tok_ref.at[(x + dxm) % nx, yq[q], c]

    def rows_of(ref, part, cut=None):
        cut = half if cut is None else cut
        return ref.at[pl.ds(part * cut, (cut, rows - cut)[part])]

    def ty(n):
        if n < 2:
            return remote(x_ref, tok_ref.at[x, y, c], ty_s.at[n], ty_r.at[n], (dev_a, dev_b)[n])
        block = rows_of(own(0, (B, A)[n - 2]), n - 2, rows * OPPOSITE_VIA_A // 4)
        return remote(block, block, ty_s.at[n], ty_r.at[n], (dev_a, dev_b)[n - 2])

    def tx(q, n):
        if n < 2:
            return remote(x_ref if q == S else own(0, q), own(0, q), tx_s.at[q, n], tx_r.at[q, n], (dev_xp, dev_xm)[n])
        block = rows_of(own((3, 1)[n - 2], q), n - 2)
        return remote(block, block, tx_s.at[q, n], tx_r.at[q, n], (dev_xp, dev_xm)[n - 2])


    def wa(k, g):
        src = wd_ref.at[pl.ds(g * ep_piece, ep_piece), :, pl.ds(pl.multiple_of(cola + k * cw, cw), cw)]
        return remote(src, w_ref.at[k, y, pl.ds(g * ep_piece, ep_piece)], wa_s.at[k, g], wa_r.at[k, g], dev_a)

    def wb(k, g):
        src = wd_ref.at[pl.ds(g * ep_piece, ep_piece), :, pl.ds(pl.multiple_of(colb + k * cw, cw), cw)]
        return remote(src, w_ref.at[k, y, pl.ds(g * ep_piece, ep_piece)], wb_s.at[k, g], wb_r.at[k, g], dev_b)

    def wf(k, g):
        block = w_ref.at[k, ya, pl.ds(g * ep_piece, ep_piece)]
        return remote(block, block, wf_s.at[k, g], wf_r.at[k, g], dev_b)

    def hd(i):
        dxm, q = order_of(i)
        block = h_ref.at[y, (x + dxm) % nx, yq[q]]
        return remote(block, block, hd_s.at[i], hd_r.at[i], dev_a if q < 2 else dev_b)

    def hf(i):
        dxm, q = order_of(i)
        block = h_ref.at[yb, (x + dxm) % nx, place(yb, q)]
        return remote(block, block, hf_s.at[i], hf_r.at[i], dev_a)

    def send(actions, load_w=None):
        for action in actions:
            kind, at = action[0], action[1:]
            if kind == 'wf':
                wa(*at).wait_recv()
            if kind == 'hf':
                hd(*at).wait_recv()
            if kind == 'lw':
                load_w(*at)
            else:
                {'wa': wa, 'wb': wb, 'wf': wf, 'hd': hd, 'hf': hf}[kind](*at).start()

    for n in (0, 1):
        ty(n).start()
        tx(S, n).start()
    routing_tables(ids_ref, gate_ref, meta_ref, slot_ref, weight_ref, per)
    lax.fori_loop(1, ny * eps, meta_send, 0)
    metav[me] = meta_ref[ep]
    send(SEND_START)

    def came(q):
        for n in (0, 1):
            tx(q, n).wait_recv()

    def both(q, first):
        tx(q, first).start()
        tx(q, first + 1).start()

    def comm(step):
        if step == 1:
            ty(0).wait_recv()
            ty(1).wait_recv()
            for n in OPPOSITE:
                ty(n).start()
            both(A, 0)
            both(B, 0)
            came(S)
        if step == 4:
            came(A)
            for n in OPPOSITE:
                ty(n).wait_recv()
            both(O, 0)
            both(S, 2)
            both(A, 2)
        if step in (7, 10):
            q = {7: B, 10: O}[step]
            came(q)
            both(q, 2)
        if step >= 12:
            tx(step - 12, 2).wait_recv()
            tx(step - 12, 3).wait_recv()

    row_id = lax.broadcasted_iota(jnp.int32, (rows, pairs), 0)

    def one_hot(src):
        pos = metav[src, 0:1, :].astype(jnp.int32)
        return (row_id == pos).astype(F32).astype(BF16)

    def meta_wait(src):
        remote(meta_ref.at[0], metav.at[src], ms.at[0], mr.at[src], dev_p).wait_recv()

    def phase_one(wg, wu, tb, xg, hb, left, wl, tl, hl):
        load_g = pltpu.make_async_copy(wg_ref, wg, wl.at[0])
        load_u = pltpu.make_async_copy(wu_ref, wu, wl.at[1])
        load_g.start()
        load_u.start()

        def store(i):
            dxm, q = order_of(i)
            return pltpu.make_async_copy(hb, h_ref.at[y, (x + dxm) % nx, place(y, q)], hl.at[0])

        def rows_in(i):
            dxm, q = order_of(i)
            return pltpu.make_async_copy(tok_ref.at[(x + dxm) % nx, place(y, q), c], tb.at[i % 2], tl.at[i % 2])

        def to_partner(i, m):
            return remote(tb.at[i % 2, :, pl.ds(m * cw, cw)], o3.at[pl.ds(m * rows, rows)], td_s.at[i % 2, m], td_r.at[m], dev_p)

        def batch(i, carry):
            @pl.when(i > 0)
            def _():
                store(i - 1).wait()

            for step in range(1, 16):
                if SEND_BEFORE[step] or SEND_AFTER[step] or step in (1, 4, 7, 10) or step >= 12:
                    @pl.when(i == step)
                    def _(step=step):
                        send(SEND_BEFORE[step])
                        comm(step)
                        send(SEND_AFTER[step])

            dxm, q = order_of(i)
            xs, ys = (x + dxm) % nx, place(y, q)
            ahead, next_ahead = look_up(AHEAD, i), look_up(AHEAD[1:] + (0,), i)

            @pl.when(ahead == 0)
            def _():
                @pl.when(i >= 2)
                def _():
                    for m in range(width // cw):
                        to_partner(i - 2, m).wait_send()

                @pl.when(i == 0)
                def _():
                    pltpu.make_async_copy(x_ref, tb.at[0], tl.at[0]).start()

                @pl.when(i > 0)
                def _():
                    rows_in(i).start()

                rows_in(i).wait()

                @pl.when(i > 0)
                def _():
                    pl.semaphore_wait(room, 1)

                for m in range(width // cw):
                    to_partner(i, m).start()

            @pl.when(next_ahead == 1)
            def _():
                for m in range(width // cw):
                    to_partner(i - 1, m).wait_send()
                rows_in(i + 1).start()

            @pl.when(i > 0)
            def _():
                meta_wait(lin(xs, ys, c))

            hot = one_hot(lin(xs, ys, c))
            step = min(512, width)
            for lo in range(0, width, step):
                got = lax.dot_general(hot, tb[i % 2, :, lo:lo + step], (((0,), (0,)), ((), ())), preferred_element_type=F32)
                xg[:, 0, :, lo:lo + step] = got.astype(BF16).reshape(el, per, step)
            meta_wait(lin(xs, ys, 1 - c))
            hot = one_hot(lin(xs, ys, 1 - c))
            for m in range(width // cw):
                to_partner(i, m).wait_recv()
                got = lax.dot_general(hot, o3[m * rows:(m + 1) * rows, :], (((0,), (0,)), ((), ())), preferred_element_type=F32)
                xg[:, 1, :, m * cw:(m + 1) * cw] = got.astype(BF16).reshape(el, per, cw)

            @pl.when(i < 15)
            def _():
                pl.semaphore_signal(room, inc=1, device_id=dev_p, device_id_type=MESH)

            @pl.when(next_ahead == 1)
            def _():
                rows_in(i + 1).wait()
                pl.semaphore_wait(room, 1)
                for m in range(width // cw):
                    to_partner(i + 1, m).start()

            @pl.when(i == 0)
            def _():
                load_g.wait()
                load_u.wait()

            for e in range(el):
                lhs = xg[e].reshape(2 * per, width)
                a = lax.dot_general(lhs, wg[e], (((1,), (1,)), ((), ())), preferred_element_type=F32)
                b = lax.dot_general(lhs, wu[e], (((1,), (1,)), ((), ())), preferred_element_type=F32)
                hid = a * jax.nn.sigmoid(a) * b
                for s in (0, 1):
                    hb[either(s), e] = hid[s * per:(s + 1) * per, :LANES].astype(BF16)
                left[e] = hid[:, LANES:]
            packed = jnp.concatenate([left[e] for e in range(el)], axis=1).astype(BF16)
            for m in range(el * rest // LANES):
                for s in (0, 1):
                    hb[either(s), whole + m] = packed[s * per:(s + 1) * per, m * LANES:(m + 1) * LANES]
            store(i).start()
            return carry

        lax.fori_loop(0, 16, batch, 0)
        for i in (14, 15):
            for m in range(width // cw):
                to_partner(i, m).wait_send()
        store(15).wait()

    pl.run_scoped(
        phase_one,
        pltpu.VMEM((el, ff, width), BF16),
        pltpu.VMEM((el, ff, width), BF16),
        pltpu.VMEM((2, rows, width), BF16),
        pltpu.VMEM((el, 2, per, width), BF16),
        pltpu.VMEM((2,) + h_ref.shape[4:], BF16),
        pltpu.VMEM((el, 2 * per, rest), F32),
        pltpu.SemaphoreType.DMA((2,)),
        pltpu.SemaphoreType.DMA((2,)),
        pltpu.SemaphoreType.DMA((1,)),
    )

    def all_sent():
        def meta_done(d, carry):
            meta_copy(d).wait_send()
            return carry

        lax.fori_loop(1, ny * eps, meta_done, 0)
        for n in (0, 1) + OPPOSITE:
            ty(n).wait_send()
        for q in (S, A, B, O):
            for n in range(4):
                tx(q, n).wait_send()
        for k in range(kc):
            for g in range(PIECES):
                wa(k, g).wait_send()
                wb(k, g).wait_send()
                wf(k, g).wait_send()
        for i in range(16):
            hd(i).wait_send()
            if order_of(i)[1] >= 2:
                hf(i).wait_send()

    def window(e):
        return e * rest // 128 * 128, -(-(e + 1) * rest // 128) * 128

    def offset(e, q):
        before = sum(LANES + window(m)[1] - window(m)[0] for m in range(e))
        return 4 * before + q * (LANES + window(e)[1] - window(e)[0])

    deep = offset(el, S)

    units = len(UNITS)

    def phase_two(wv, hv, gc, pb, pp, sb, fb, wl, hvl, pp_s, rs_s, of_s, ol):
        lane = gc.shape[3]

        def clear(k):
            for e in range(el):
                low, high = window(e)
                for q in (S, A, B, O):
                    at = offset(e, q) + LANES
                    for start, stop in ((0, e * rest - low), ((e + 1) * rest - low, high - low)):
                        if stop > start:
                            wv[k, at + start:at + stop] = jnp.zeros((stop - start, cw), BF16)

        def blocks(j):
            return ((x + 2 * nx - 1 - j) % nx, (x + 1 + j) % nx), (y, ya)

        def w_loads(k):
            copies = []
            for q in (S, A, B, O):
                for e in range(el):
                    if q == S:
                        src = wd_ref.at[e, :, pl.ds(pl.multiple_of(colb + k * cw, cw), cw)]
                    else:
                        src = w_ref.at[k, yq[q], e]
                    low, high = window(e)
                    at = offset(e, q)
                    copies.append(pltpu.make_async_copy(src.at[pl.ds(0, LANES)], wv.at[k, pl.ds(at, LANES)], wl.at[k]))
                    copies.append(pltpu.make_async_copy(
                        src.at[pl.ds(LANES, rest)], wv.at[k, pl.ds(at + LANES + e * rest - low, rest)], wl.at[k]))
            return copies

        def load_w(k):
            for g in range(PIECES):
                wb(k, g).wait_recv()
                wf(k, g).wait_recv()
            for copy in w_loads(k):
                copy.start()
            clear(k)

        def h_loads(n, j):
            xs, ys = blocks(j)
            copies = []
            for d in (0, 1):
                for rel in (0, 1):
                    for q in (S, A, B, O):
                        copies.append(pltpu.make_async_copy(
                            h_ref.at[yq[q], xs[d], ys[d], either(rel)], hv.at[n % 2, q, :, 2 * d + rel], hvl.at[n % 2, q, 2 * d + rel]))
            return copies

        def first_use(j):
            minus, plus = (3 - j) % 4, (1 + j) % 4
            hd(BATCH[(minus, A)]).wait_recv()
            hd(BATCH[(plus, S)]).wait_recv()
            hf(BATCH[(minus, O)]).wait_recv()
            hf(BATCH[(plus, B)]).wait_recv()

        def partner_copy(n, d):
            return remote(pp.at[n % 2, d], db.at[n % 2, d], pp_s.at[n % 2, d], db_r.at[n % 2, d], dev_p)

        def ring_copy(slot, d, k, j):
            return remote(sb.at[slot, d], rb.at[d, k, j], rs_s.at[slot, d], rs_r.at[d, k, j], (dev_xp, dev_xm)[d])

        def out_copies(slot, k):
            cols = out_ref.at[:, pl.ds(pl.multiple_of(colb + k * cw, cw), cw)]
            return (
                pltpu.make_async_copy(fb.at[slot, 0], cols, ol.at[slot]),
                remote(fb.at[slot, 1], cols, of_s.at[slot], of_r.at[k], dev_a),
            )

        def make(n):
            k, j = look_up([u[0] for u in UNITS], n), look_up([u[1] for u in UNITS], n)
            xs, ys = blocks(j)
            for at in range(units):
                new_chunk = UNITS[at][0] not in [u[0] for u in UNITS[:at]]
                first = at in FIRST_STEP.values()
                if (not first and SEND_MAKE[at]) or new_chunk:
                    @pl.when(n == at)
                    def _(at=at, new_chunk=new_chunk, first=first):
                        if not first:
                            send(SEND_MAKE[at], load_w)
                        if new_chunk:
                            pltpu.make_async_copy(w_ref.at[UNITS[at][0]], w_ref.at[UNITS[at][0]], wl.at[UNITS[at][0]]).wait()
            for d in (0, 1):
                for rel in (0, 1):
                    gate = metav[lin(xs[d], ys[d], either(rel)), 1:2, :]
                    gc[:, 2 * d + rel] = jnp.transpose(jnp.broadcast_to(gate, (lane, pairs))).reshape(el, per, lane)
            for copy in h_loads(n, j):
                copy.wait()

            @pl.when(n == 0)
            def _():
                later = [action for action in SEND_END + SEND_MAKE[0] if action[0] == 'lw' and action[1] != UNITS[0][0]]
                send(later, load_w)

            for e in range(el):
                low, high = window(e)
                parts = []
                for q in (S, A, B, O):
                    parts.append(hv[n % 2, q, e].reshape(4 * per, LANES))
                    for at in range(low, high, 128):
                        parts.append(hv[n % 2, q, whole + at // LANES, :, :, at % LANES:at % LANES + 128].reshape(4 * per, 128))
                size = 4 * (LANES + high - low)
                o = jnp.dot(jnp.concatenate(parts, axis=1), wv[k, offset(e, S):offset(e, S) + size], preferred_element_type=F32)
                g = gc[e].reshape(4 * per, lane)
                v = o * jnp.concatenate([g] * (cw // lane), axis=1)
                hi = v.astype(BF16)
                over = v - hi.astype(F32)
                mid = over.astype(BF16)
                low_part = (over - mid.astype(F32)).astype(BF16)
                for m in range(4):
                    for third, value in enumerate((hi, mid, low_part)):
                        at = (3 * m + third) * pairs + e * per
                        o3[at:at + per, :] = value[m * per:(m + 1) * per]

            @pl.when(n >= 2)
            def _():
                for d in (0, 1):
                    partner_copy(n - 2, d).wait_send()
                pl.semaphore_wait(credit, 1)

            for rel in (1, 0):
                for d in (0, 1):
                    hot = one_hot(lin(xs[d], ys[d], either(rel)))
                    at = 3 * (2 * d + rel) * pairs
                    total = jnp.dot(hot, o3[at:at + pairs, :], preferred_element_type=F32)
                    total += jnp.dot(hot, o3[at + pairs:at + 2 * pairs, :], preferred_element_type=F32)
                    total += jnp.dot(hot, o3[at + 2 * pairs:at + 3 * pairs, :], preferred_element_type=F32)
                    if rel == 1:
                        pp[n % 2, d] = total
                        partner_copy(n, d).start()
                    else:
                        pb[n % 2, d] = total

        def join(n):
            k, j = look_up([u[0] for u in UNITS], n), look_up([u[1] for u in UNITS], n)
            count = look_up([sum(1 for m in SENDS if m < at) for at in range(units)], n)
            slot = count % 4
            for at in range(units):
                if SEND_JOIN[at]:
                    @pl.when(n == at)
                    def _(at=at):
                        send(SEND_JOIN[at], load_w)
            for d in (0, 1):
                partner_copy(n, d).wait_recv()

            @pl.when((j < 3) & (count >= 4))
            def _():
                for d in (0, 1):
                    ring_copy(slot, d, k, 0).wait_send()

            for d in (0, 1):
                @pl.when(j == 0)
                def _():
                    sb[slot, d] = pb[n % 2, d] + db[n % 2, d]

                @pl.when((j > 0) & (j < 3))
                def _():
                    ring_copy(slot, d, k, j - 1).wait_recv()
                    sb[slot, d] = pb[n % 2, d] + db[n % 2, d] + rb[d, k, j - 1]

                @pl.when(j < 3)
                def _():
                    ring_copy(slot, d, k, j).start()

            for order, at in enumerate(FINALS):
                @pl.when(n == at)
                def _(order=order, at=at):
                    kk = UNITS[at][0]
                    if order >= 2:
                        local, away = out_copies(order % 2, kk)
                        local.wait()
                        away.wait_send()
                    local, away = out_copies(order % 2, kk)
                    for d in (1, 0):
                        ring_copy(0, d, kk, 2).wait_recv()
                        fb[order % 2, d] = (pb[at % 2, d] + db[at % 2, d] + rb[d, kk, 2]).astype(BF16)
                        (local, away)[d].start()

            @pl.when(n < units - 2)
            def _():
                pl.semaphore_signal(credit, inc=1, device_id=dev_p, device_id_type=MESH)

        send([action for action in SEND_MAKE[0] if action[0] != 'lw'])
        load_w(UNITS[0][0])
        first_use(UNITS[0][1])
        for copy in h_loads(0, UNITS[0][1]):
            copy.start()
        seen = [int(at + 1 < units and FIRST_STEP[UNITS[at + 1][1]] <= at) for at in range(units)]

        def operation(at, carry):
            n = look_up([o[1] for o in ORDER], at)

            @pl.when(look_up([o[0] for o in ORDER], at) == 0)
            def _():
                for step, first in FIRST_STEP.items():
                    if first > 0:
                        @pl.when(n == first)
                        def _(step=step, first=first):
                            send(SEND_MAKE[first], load_w)
                            first_use(step)
                            for copy in h_loads(first, step):
                                copy.start()

                make(n)

                @pl.when(look_up(seen, n) == 1)
                def _():
                    for copy in h_loads(n + 1, look_up([u[1] for u in UNITS[1:]], n)):
                        copy.start()

            @pl.when(look_up([o[0] for o in ORDER], at) == 1)
            def _():
                join(n)

            return carry

        lax.fori_loop(0, len(ORDER), operation, 0)
        for d in (0, 1):
            for n in (units - 2, units - 1):
                partner_copy(n, d).wait_send()
            for slot in range(4):
                ring_copy(slot, d, 0, 0).wait_send()
        for slot in (0, 1):
            local, away = out_copies(slot, 0)
            local.wait()
            away.wait_send()
        all_sent()
        for k in range(kc):
            out_copies(0, k)[1].wait_recv()

    lane = min(128, cw)
    send([action for action in SEND_END if action[0] != 'lw'])

    pl.run_scoped(
        phase_two,
        pltpu.VMEM((kc, deep, cw), BF16),
        pltpu.VMEM((2, 4, h_ref.shape[4], 4, per, LANES), BF16),
        pltpu.VMEM((el, 4, per, lane), F32),
        pltpu.VMEM((2, 2, rows, cw), F32),
        pltpu.VMEM((2, 2, rows, cw), F32),
        pltpu.VMEM((4, 2, rows, cw), F32),
        pltpu.VMEM((2, 2, rows, cw), BF16),
        pltpu.SemaphoreType.DMA((kc,)),
        pltpu.SemaphoreType.DMA((2, 4, 4)),
        pltpu.SemaphoreType.DMA((2, 2)),
        pltpu.SemaphoreType.DMA((4, 2)),
        pltpu.SemaphoreType.DMA((2,)),
        pltpu.SemaphoreType.DMA((2,)),
    )


def solution(mesh):
    ny, eps = mesh.shape['tp'], mesh.shape['ep']
    nx = eps // 2
    row_spec = P(('dp', 'ep', 'tp'), None)
    w_in_spec = P('ep', None, 'tp')
    w_out_spec = P('ep', 'tp', None)

    def local_moe(x, ids, gates, w_gate, w_up, w_down):
        rows, width = x.shape
        el, _, ff = w_gate.shape
        experts = el * eps
        per = rows * ids.shape[1] // experts
        pairs = el * per
        cw = width // 2 // CHUNKS
        hbm = pl.BlockSpec(memory_space=pl.ANY)
        vmem = pl.BlockSpec(memory_space=pltpu.VMEM)
        dma = pltpu.SemaphoreType.DMA
        outs = pl.pallas_call(
            functools.partial(moe_kernel, nx, ny),
            name='moe_kernel',
            out_shape=[
                jax.ShapeDtypeStruct((rows, width), BF16),
                jax.ShapeDtypeStruct((nx, ny, 2, rows, width), BF16),
                jax.ShapeDtypeStruct((ny, nx, ny, 2, el * ff // LANES, per, LANES), BF16),
                jax.ShapeDtypeStruct((CHUNKS, ny, el, ff, cw), BF16),
            ],
            in_specs=[hbm, vmem, vmem, hbm, hbm, hbm],
            out_specs=[hbm] * 4,
            scratch_shapes=[
                pltpu.VMEM((ny * eps, 8, pairs), F32),
                pltpu.VMEM((eps, 8, pairs), F32),
                pltpu.VMEM((experts, rows), F32),
                pltpu.VMEM((experts, rows), F32),
                pltpu.VMEM((2, CHUNKS, 3, rows, cw), F32),
                pltpu.VMEM((2, 2, rows, cw), F32),
                dma((ny * eps,)), dma((ny * eps,)),
                dma((4,)), dma((4,)),
                dma((4, 4)), dma((4, 4)),
                dma((2, width // cw)), dma((width // cw,)), pltpu.SemaphoreType.REGULAR,
                pltpu.VMEM((12 * pairs, cw), BF16),
                dma((16,)), dma((16,)), dma((16,)), dma((16,)),
            ] + [dma((CHUNKS, PIECES))] * 6 + [
                dma((2, CHUNKS, 3)), dma((2, 2)), dma((CHUNKS,)),
                pltpu.SemaphoreType.REGULAR,
            ],
            compiler_params=pltpu.CompilerParams(collective_id=0, has_side_effects=True, vmem_limit_bytes=67 * 1000 * 1000),
        )(x, ids.T, gates.T, jnp.transpose(w_gate, (0, 2, 1)), jnp.transpose(w_up, (0, 2, 1)), w_down)
        return outs[0]

    return jax.shard_map(
        local_moe, mesh=mesh, in_specs=(row_spec, row_spec, row_spec, w_in_spec, w_in_spec, w_out_spec),
        out_specs=row_spec, check_vma=False)
```

```python
import functools

import jax
import jax.numpy as jnp
from jax import lax
from jax.experimental import pallas as pl
from jax.experimental.pallas import tpu as pltpu
from jax.sharding import PartitionSpec as P

MESH = pl.DeviceIdType.MESH
CHUNKS = 4
LANES = 256
PIECES = 2
BF16 = jnp.bfloat16
F32 = jnp.float32

S, A, B, O = 0, 1, 2, 3

UNITS = ((0, 0), (1, 0), (2, 0), (0, 1), (2, 1), (1, 1), (0, 2), (3, 0), (2, 2), (3, 1), (1, 2), (2, 3), (3, 2), (0, 3), (1, 3), (3, 3), )
ORDER = ((0, 0), (0, 1), (1, 0), (0, 2), (1, 1), (1, 2), (0, 3), (0, 4), (1, 3), (0, 5), (1, 4), (0, 6), (1, 5), (0, 7), (1, 6), (0, 8), (1, 7), (1, 8), (0, 9), (0, 10), (1, 9), (0, 11), (1, 10), (0, 12), (1, 11), (0, 13), (1, 12), (0, 14), (1, 13), (0, 15), (1, 14), (1, 15), )
OPPOSITE_VIA_A = 4
OPPOSITE = (2,)
SEND_START = (('wa', 1, 0), ('wb', 0, 0), ('wb', 2, 0), )
SEND_BEFORE = (
    (),
    (),
    (('hd', 1), ('wa', 2, 1), ('wa', 2, 0), ('wa', 0, 1), ('wa', 1, 1), ('wa', 0, 0), ('wf', 1, 0), ('wb', 1, 0), ('wb', 1, 1), ('wb', 0, 1), ('wb', 2, 1), ),
    (),
    (),
    (),
    (),
    (('wf', 2, 1), ),
    (),
    (('hd', 8), ),
    (('wf', 0, 1), ('hd', 7), ),
    (('hd', 10), ),
    (('hd', 11), ('wf', 1, 1), ('wf', 0, 0), ('wf', 2, 0), ),
    (('hf', 7), ('hf', 10), ),
    (('hf', 11), ('hd', 12), ('hd', 13), ),
    (('hd', 14), ),
)
SEND_AFTER = (
    (),
    (),
    (),
    (),
    (),
    (),
    (),
    (),
    (),
    (),
    (('hf', 8), ('wa', 3, 0), ('hd', 5), ('hd', 4), ),
    (),
    (),
    (),
    (),
    (),
)
SEND_END = (('hd', 15), ('wb', 3, 1), ('wb', 3, 0), ('wf', 3, 0), ('lw', 0), ('lw', 1), ('lw', 2), )
SEND_MAKE = (
    (),
    (('hf', 14), ),
    (('hf', 15), ('wa', 3, 1), ('hd', 2), ('hd', 0), ('hd', 3), ),
    (),
    (),
    (),
    (),
    (('lw', 3), ),
    (),
    (),
    (('hf', 9), ),
    (),
    (),
    (),
    (),
    (),
)
SEND_JOIN = (
    (),
    (),
    (),
    (),
    (('wf', 3, 1), ('hd', 6), ('hd', 9), ),
    (),
    (),
    (('hf', 6), ),
    (),
    (),
    (),
    (),
    (),
    (),
    (),
    (),
)


def order_of(i):
    last, r = i // 12, i % 3
    return (1 - last) * (r + r // 2) + 2 * last, (1 - last) * (i // 3) + last * (i - 12)


BATCH = {order_of(i): i for i in range(16)}
AHEAD = (0, 0, 1, 1, 0, 1, 1, 0, 1, 1, 0, 1, 0, 0, 0, 0)
FIRST_STEP = {}
for place_in_order, (chunk_of, step_of) in enumerate(UNITS):
    FIRST_STEP.setdefault(step_of, place_in_order)
SENDS = [n for n, (_, j) in enumerate(UNITS) if j < 3]
FINALS = [n for n, (_, j) in enumerate(UNITS) if j == 3]


def place(y, q):
    high, low = y // 2, y % 2
    return 2 * ((high + q // 2) % 2) + (low + (q + 1) // 2) % 2


def look_up(table, n):
    value = jnp.int32(table[0])
    for at in range(1, len(table)):
        if table[at] != table[0]:
            value = jnp.where(n == at, table[at], value)
    return value


def routing_tables(ids_ref, gate_ref, meta_ref, slot_ref, weight_ref, per):
    top, rows = ids_ref.shape
    experts = slot_ref.shape[0]
    devices, _, pairs = meta_ref.shape
    group = experts // devices
    expert = lax.broadcasted_iota(jnp.int32, (experts, rows), 0)
    chosen = jnp.zeros((experts, rows), F32)
    weight = jnp.zeros((experts, rows), F32)
    for j in range(top):
        here = expert == ids_ref[j:j + 1, :]
        chosen = jnp.where(here, 1.0, chosen)
        weight = jnp.where(here, gate_ref[j:j + 1, :], weight)
    earlier = lax.broadcasted_iota(jnp.int32, (rows, rows), 0) < lax.broadcasted_iota(jnp.int32, (rows, rows), 1)
    rank = jnp.dot(chosen.astype(BF16), earlier.astype(F32).astype(BF16), preferred_element_type=F32)
    slot_ref[...] = jnp.where(chosen > 0.0, rank, -1.0)
    weight_ref[...] = weight
    lane = lax.broadcasted_iota(jnp.int32, (group, pairs), 1)
    sub = lax.broadcasted_iota(jnp.int32, (group, pairs), 0)
    mine = ((lane >= sub * per) & (lane < (sub + 1) * per)).astype(F32).astype(BF16)
    place_in_expert = lax.broadcasted_iota(jnp.int32, (rows, pairs), 1)
    for m in range(1, group):
        place_in_expert = jnp.where(lax.broadcasted_iota(jnp.int32, (rows, pairs), 1) >= m * per,
                                    lax.broadcasted_iota(jnp.int32, (rows, pairs), 1) - m * per, place_in_expert)
    place_in_expert = place_in_expert.astype(F32)
    row = lax.broadcasted_iota(jnp.int32, (8, rows), 1)
    high = (row // 2).astype(F32).astype(BF16)
    low = (row % 2).astype(F32).astype(BF16)
    top_row = lax.broadcasted_iota(jnp.int32, (8, pairs), 0)

    def spread(part):
        return lax.dot_general(part, mine, (((0,), (0,)), ((), ())), preferred_element_type=F32)

    def table(d, carry):
        at = pl.ds(pl.multiple_of(d * group, group), group)
        hit = (spread(slot_ref[at, :].astype(BF16)) == place_in_expert).astype(F32)
        hot = hit.astype(BF16)
        position = 2.0 * jnp.dot(high, hot, preferred_element_type=F32) + jnp.dot(low, hot, preferred_element_type=F32)
        w = weight_ref[at, :]
        first = w.astype(BF16)
        over = w - first.astype(F32)
        second = over.astype(BF16)
        third = (over - second.astype(F32)).astype(BF16)
        value = jnp.sum((spread(first) + spread(second) + spread(third)) * hit, axis=0, keepdims=True)
        meta_ref[d] = jnp.where(top_row == 0, position, jnp.broadcast_to(value, (8, pairs)))
        return carry

    lax.fori_loop(0, devices, table, 0)


def moe_kernel(nx, ny, x_ref, ids_ref, gate_ref, wg_ref, wu_ref, wd_ref, out_ref, tok_ref, h_ref, w_ref,
               metav, meta_ref, slot_ref, weight_ref, rb, db, ms, mr, ty_s, ty_r, tx_s, tx_r, td_s, td_r, room, o3, hd_s, hd_r, hf_s, hf_r,
               wa_s, wa_r, wb_s, wb_r, wf_s, wf_r, rs_r, db_r, of_r, credit):
    rows, width = x_ref.shape
    half = rows // 2
    el, ff, _ = wg_ref.shape
    per = h_ref.shape[5]
    rest = ff - LANES * (ff // LANES)
    whole = el * (ff // LANES)
    assert ff // LANES == 1 and (el * rest) % LANES == 0 and rest <= 128
    pairs = el * per
    kc, cw = w_ref.shape[0], w_ref.shape[4]
    ep_piece = el // PIECES
    eps = 2 * nx
    y = lax.axis_index('tp')
    ep = lax.axis_index('ep')
    x, c = ep // 2, ep % 2
    ya, yb, yo = place(y, A), place(y, B), place(y, O)
    yq = (y, ya, yb, yo)
    xp, xm = (x + 1) % nx, (x + nx - 1) % nx
    colb = ((y + y // 2) % 2) * (kc * cw)
    cola = ((ya + ya // 2) % 2) * (kc * cw)
    me = y * eps + ep

    dev_a = {'tp': ya, 'ep': ep}
    dev_b = {'tp': yb, 'ep': ep}
    dev_p = {'tp': y, 'ep': 2 * x + 1 - c}
    dev_xp = {'tp': y, 'ep': 2 * xp + c}
    dev_xm = {'tp': y, 'ep': 2 * xm + c}

    def remote(src, dst, send, recv, dev):
        return pltpu.make_async_remote_copy(src_ref=src, dst_ref=dst, send_sem=send, recv_sem=recv, device_id=dev, device_id_type=MESH)

    def lin(xs, ys, cs):
        return ys * eps + 2 * xs + cs

    def either(rel):
        return c if rel == 0 else 1 - c

    barrier = pltpu.get_barrier_semaphore()

    def peer_of(d):
        other = (me + d) % (ny * eps)
        return other // eps, other % eps

    def greet(d, carry):
        py, pe = peer_of(d)
        pl.semaphore_signal(barrier, inc=1, device_id={'tp': py, 'ep': pe}, device_id_type=MESH)
        return carry

    lax.fori_loop(1, ny * eps, greet, 0)
    pl.semaphore_wait(barrier, ny * eps - 1)

    def meta_copy(d):
        py, pe = peer_of(d)
        return remote(meta_ref.at[pe], metav.at[me], ms.at[d], mr.at[me], {'tp': py, 'ep': pe})

    def meta_send(d, carry):
        meta_copy(d).start()
        return carry

    def own(dxm, q):
        return tok_ref.at[(x + dxm) % nx, yq[q], c]

    def rows_of(ref, part, cut=None):
        cut = half if cut is None else cut
        return ref.at[pl.ds(part * cut, (cut, rows - cut)[part])]

    def ty(n):
        if n < 2:
            return remote(x_ref, tok_ref.at[x, y, c], ty_s.at[n], ty_r.at[n], (dev_a, dev_b)[n])
        block = rows_of(own(0, (B, A)[n - 2]), n - 2, rows * OPPOSITE_VIA_A // 4)
        return remote(block, block, ty_s.at[n], ty_r.at[n], (dev_a, dev_b)[n - 2])

    def tx(q, n):
        if n < 2:
            return remote(x_ref if q == S else own(0, q), own(0, q), tx_s.at[q, n], tx_r.at[q, n], (dev_xp, dev_xm)[n])
        block = rows_of(own((3, 1)[n - 2], q), n - 2)
        return remote(block, block, tx_s.at[q, n], tx_r.at[q, n], (dev_xp, dev_xm)[n - 2])


    def wa(k, g):
        src = wd_ref.at[pl.ds(g * ep_piece, ep_piece), :, pl.ds(pl.multiple_of(cola + k * cw, cw), cw)]
        return remote(src, w_ref.at[k, y, pl.ds(g * ep_piece, ep_piece)], wa_s.at[k, g], wa_r.at[k, g], dev_a)

    def wb(k, g):
        src = wd_ref.at[pl.ds(g * ep_piece, ep_piece), :, pl.ds(pl.multiple_of(colb + k * cw, cw), cw)]
        return remote(src, w_ref.at[k, y, pl.ds(g * ep_piece, ep_piece)], wb_s.at[k, g], wb_r.at[k, g], dev_b)

    def wf(k, g):
        block = w_ref.at[k, ya, pl.ds(g * ep_piece, ep_piece)]
        return remote(block, block, wf_s.at[k, g], wf_r.at[k, g], dev_b)

    def hd(i):
        dxm, q = order_of(i)
        block = h_ref.at[y, (x + dxm) % nx, yq[q]]
        return remote(block, block, hd_s.at[i], hd_r.at[i], dev_a if q < 2 else dev_b)

    def hf(i):
        dxm, q = order_of(i)
        block = h_ref.at[yb, (x + dxm) % nx, place(yb, q)]
        return remote(block, block, hf_s.at[i], hf_r.at[i], dev_a)

    def send(actions, load_w=None):
        for action in actions:
            kind, at = action[0], action[1:]
            if kind == 'wf':
                wa(*at).wait_recv()
            if kind == 'hf':
                hd(*at).wait_recv()
            if kind == 'lw':
                load_w(*at)
            else:
                {'wa': wa, 'wb': wb, 'wf': wf, 'hd': hd, 'hf': hf}[kind](*at).start()

    for n in (0, 1):
        ty(n).start()
        tx(S, n).start()
    routing_tables(ids_ref, gate_ref, meta_ref, slot_ref, weight_ref, per)
    lax.fori_loop(1, ny * eps, meta_send, 0)
    metav[me] = meta_ref[ep]
    send(SEND_START)

    def came(q):
        for n in (0, 1):
            tx(q, n).wait_recv()

    def both(q, first):
        tx(q, first).start()
        tx(q, first + 1).start()

    def comm(step):
        if step == 1:
            ty(0).wait_recv()
            ty(1).wait_recv()
            for n in OPPOSITE:
                ty(n).start()
            both(A, 0)
            both(B, 0)
            came(S)
        if step == 4:
            came(A)
            for n in OPPOSITE:
                ty(n).wait_recv()
            both(O, 0)
            both(S, 2)
            both(A, 2)
        if step in (7, 10):
            q = {7: B, 10: O}[step]
            came(q)
            both(q, 2)
        if step >= 12:
            tx(step - 12, 2).wait_recv()
            tx(step - 12, 3).wait_recv()

    row_id = lax.broadcasted_iota(jnp.int32, (rows, pairs), 0)

    def one_hot(src):
        pos = metav[src, 0:1, :].astype(jnp.int32)
        return (row_id == pos).astype(F32).astype(BF16)

    def meta_wait(src):
        remote(meta_ref.at[0], metav.at[src], ms.at[0], mr.at[src], dev_p).wait_recv()

    def phase_one(wg, wu, tb, xg, hb, left, wl, tl, hl):
        load_g = pltpu.make_async_copy(wg_ref, wg, wl.at[0])
        load_u = pltpu.make_async_copy(wu_ref, wu, wl.at[1])
        load_g.start()
        load_u.start()

        def store(i):
            dxm, q = order_of(i)
            return pltpu.make_async_copy(hb, h_ref.at[y, (x + dxm) % nx, place(y, q)], hl.at[0])

        def rows_in(i):
            dxm, q = order_of(i)
            return pltpu.make_async_copy(tok_ref.at[(x + dxm) % nx, place(y, q), c], tb.at[i % 2], tl.at[i % 2])

        def to_partner(i, m):
            return remote(tb.at[i % 2, :, pl.ds(m * cw, cw)], o3.at[pl.ds(m * rows, rows)], td_s.at[i % 2, m], td_r.at[m], dev_p)

        def batch(i, carry):
            @pl.when(i > 0)
            def _():
                store(i - 1).wait()

            for step in range(1, 16):
                if SEND_BEFORE[step] or SEND_AFTER[step] or step in (1, 4, 7, 10) or step >= 12:
                    @pl.when(i == step)
                    def _(step=step):
                        send(SEND_BEFORE[step])
                        comm(step)
                        send(SEND_AFTER[step])

            dxm, q = order_of(i)
            xs, ys = (x + dxm) % nx, place(y, q)
            ahead, next_ahead = look_up(AHEAD, i), look_up(AHEAD[1:] + (0,), i)

            @pl.when(ahead == 0)
            def _():
                @pl.when(i >= 2)
                def _():
                    for m in range(width // cw):
                        to_partner(i - 2, m).wait_send()

                @pl.when(i == 0)
                def _():
                    pltpu.make_async_copy(x_ref, tb.at[0], tl.at[0]).start()

                @pl.when(i > 0)
                def _():
                    rows_in(i).start()

                rows_in(i).wait()

                @pl.when(i > 0)
                def _():
                    pl.semaphore_wait(room, 1)

                for m in range(width // cw):
                    to_partner(i, m).start()

            @pl.when(next_ahead == 1)
            def _():
                for m in range(width // cw):
                    to_partner(i - 1, m).wait_send()
                rows_in(i + 1).start()

            @pl.when(i > 0)
            def _():
                meta_wait(lin(xs, ys, c))

            hot = one_hot(lin(xs, ys, c))
            step = min(512, width)
            for lo in range(0, width, step):
                got = lax.dot_general(hot, tb[i % 2, :, lo:lo + step], (((0,), (0,)), ((), ())), preferred_element_type=F32)
                xg[:, 0, :, lo:lo + step] = got.astype(BF16).reshape(el, per, step)
            meta_wait(lin(xs, ys, 1 - c))
            hot = one_hot(lin(xs, ys, 1 - c))
            for m in range(width // cw):
                to_partner(i, m).wait_recv()
                got = lax.dot_general(hot, o3[m * rows:(m + 1) * rows, :], (((0,), (0,)), ((), ())), preferred_element_type=F32)
                xg[:, 1, :, m * cw:(m + 1) * cw] = got.astype(BF16).reshape(el, per, cw)

            @pl.when(i < 15)
            def _():
                pl.semaphore_signal(room, inc=1, device_id=dev_p, device_id_type=MESH)

            @pl.when(next_ahead == 1)
            def _():
                rows_in(i + 1).wait()
                pl.semaphore_wait(room, 1)
                for m in range(width // cw):
                    to_partner(i + 1, m).start()

            @pl.when(i == 0)
            def _():
                load_g.wait()
                load_u.wait()

            for e in range(el):
                lhs = xg[e].reshape(2 * per, width)
                a = lax.dot_general(lhs, wg[e], (((1,), (1,)), ((), ())), preferred_element_type=F32)
                b = lax.dot_general(lhs, wu[e], (((1,), (1,)), ((), ())), preferred_element_type=F32)
                hid = a * jax.nn.sigmoid(a) * b
                for s in (0, 1):
                    hb[either(s), e] = hid[s * per:(s + 1) * per, :LANES].astype(BF16)
                left[e] = hid[:, LANES:]
            packed = jnp.concatenate([left[e] for e in range(el)], axis=1).astype(BF16)
            for m in range(el * rest // LANES):
                for s in (0, 1):
                    hb[either(s), whole + m] = packed[s * per:(s + 1) * per, m * LANES:(m + 1) * LANES]
            store(i).start()
            return carry

        lax.fori_loop(0, 16, batch, 0)
        for i in (14, 15):
            for m in range(width // cw):
                to_partner(i, m).wait_send()
        store(15).wait()

    pl.run_scoped(
        phase_one,
        pltpu.VMEM((el, ff, width), BF16),
        pltpu.VMEM((el, ff, width), BF16),
        pltpu.VMEM((2, rows, width), BF16),
        pltpu.VMEM((el, 2, per, width), BF16),
        pltpu.VMEM((2,) + h_ref.shape[4:], BF16),
        pltpu.VMEM((el, 2 * per, rest), F32),
        pltpu.SemaphoreType.DMA((2,)),
        pltpu.SemaphoreType.DMA((2,)),
        pltpu.SemaphoreType.DMA((1,)),
    )

    def all_sent():
        def meta_done(d, carry):
            meta_copy(d).wait_send()
            return carry

        lax.fori_loop(1, ny * eps, meta_done, 0)
        for n in (0, 1) + OPPOSITE:
            ty(n).wait_send()
        for q in (S, A, B, O):
            for n in range(4):
                tx(q, n).wait_send()
        for k in range(kc):
            for g in range(PIECES):
                wa(k, g).wait_send()
                wb(k, g).wait_send()
                wf(k, g).wait_send()
        for i in range(16):
            hd(i).wait_send()
            if order_of(i)[1] >= 2:
                hf(i).wait_send()

    def window(e):
        return e * rest // 128 * 128, -(-(e + 1) * rest // 128) * 128

    def offset(e, q):
        before = sum(LANES + window(m)[1] - window(m)[0] for m in range(e))
        return 4 * before + q * (LANES + window(e)[1] - window(e)[0])

    deep = offset(el, S)

    units = len(UNITS)

    def phase_two(wv, hv, gc, pb, pp, sb, fb, wl, hvl, pp_s, rs_s, of_s, ol):
        lane = gc.shape[3]

        def clear(k):
            for e in range(el):
                low, high = window(e)
                for q in (S, A, B, O):
                    at = offset(e, q) + LANES
                    for start, stop in ((0, e * rest - low), ((e + 1) * rest - low, high - low)):
                        if stop > start:
                            wv[k, at + start:at + stop] = jnp.zeros((stop - start, cw), BF16)

        def blocks(j):
            return ((x + 2 * nx - 1 - j) % nx, (x + 1 + j) % nx), (y, ya)

        def w_loads(k):
            copies = []
            for q in (S, A, B, O):
                for e in range(el):
                    if q == S:
                        src = wd_ref.at[e, :, pl.ds(pl.multiple_of(colb + k * cw, cw), cw)]
                    else:
                        src = w_ref.at[k, yq[q], e]
                    low, high = window(e)
                    at = offset(e, q)
                    copies.append(pltpu.make_async_copy(src.at[pl.ds(0, LANES)], wv.at[k, pl.ds(at, LANES)], wl.at[k]))
                    copies.append(pltpu.make_async_copy(
                        src.at[pl.ds(LANES, rest)], wv.at[k, pl.ds(at + LANES + e * rest - low, rest)], wl.at[k]))
            return copies

        def load_w(k):
            for g in range(PIECES):
                wb(k, g).wait_recv()
                wf(k, g).wait_recv()
            for copy in w_loads(k):
                copy.start()
            clear(k)

        def h_loads(n, j):
            xs, ys = blocks(j)
            copies = []
            for d in (0, 1):
                for rel in (0, 1):
                    for q in (S, A, B, O):
                        copies.append(pltpu.make_async_copy(
                            h_ref.at[yq[q], xs[d], ys[d], either(rel)], hv.at[n % 2, q, :, 2 * d + rel], hvl.at[n % 2, q, 2 * d + rel]))
            return copies

        def first_use(j):
            minus, plus = (3 - j) % 4, (1 + j) % 4
            hd(BATCH[(minus, A)]).wait_recv()
            hd(BATCH[(plus, S)]).wait_recv()
            hf(BATCH[(minus, O)]).wait_recv()
            hf(BATCH[(plus, B)]).wait_recv()

        def partner_copy(n, d):
            return remote(pp.at[n % 2, d], db.at[n % 2, d], pp_s.at[n % 2, d], db_r.at[n % 2, d], dev_p)

        def ring_copy(slot, d, k, j):
            return remote(sb.at[slot, d], rb.at[d, k, j], rs_s.at[slot, d], rs_r.at[d, k, j], (dev_xp, dev_xm)[d])

        def out_copies(slot, k):
            cols = out_ref.at[:, pl.ds(pl.multiple_of(colb + k * cw, cw), cw)]
            return (
                pltpu.make_async_copy(fb.at[slot, 0], cols, ol.at[slot]),
                remote(fb.at[slot, 1], cols, of_s.at[slot], of_r.at[k], dev_a),
            )

        def make(n):
            k, j = look_up([u[0] for u in UNITS], n), look_up([u[1] for u in UNITS], n)
            xs, ys = blocks(j)
            for at in range(units):
                new_chunk = UNITS[at][0] not in [u[0] for u in UNITS[:at]]
                first = at in FIRST_STEP.values()
                if (not first and SEND_MAKE[at]) or new_chunk:
                    @pl.when(n == at)
                    def _(at=at, new_chunk=new_chunk, first=first):
                        if not first:
                            send(SEND_MAKE[at], load_w)
                        if new_chunk:
                            pltpu.make_async_copy(w_ref.at[UNITS[at][0]], w_ref.at[UNITS[at][0]], wl.at[UNITS[at][0]]).wait()
            for d in (0, 1):
                for rel in (0, 1):
                    gate = metav[lin(xs[d], ys[d], either(rel)), 1:2, :]
                    gc[:, 2 * d + rel] = jnp.transpose(jnp.broadcast_to(gate, (lane, pairs))).reshape(el, per, lane)
            for copy in h_loads(n, j):
                copy.wait()

            @pl.when(n == 0)
            def _():
                later = [action for action in SEND_END + SEND_MAKE[0] if action[0] == 'lw' and action[1] != UNITS[0][0]]
                send(later, load_w)

            for e in range(el):
                low, high = window(e)
                parts = []
                for q in (S, A, B, O):
                    parts.append(hv[n % 2, q, e].reshape(4 * per, LANES))
                    for at in range(low, high, 128):
                        parts.append(hv[n % 2, q, whole + at // LANES, :, :, at % LANES:at % LANES + 128].reshape(4 * per, 128))
                size = 4 * (LANES + high - low)
                o = jnp.dot(jnp.concatenate(parts, axis=1), wv[k, offset(e, S):offset(e, S) + size], preferred_element_type=F32)
                g = gc[e].reshape(4 * per, lane)
                v = o * jnp.concatenate([g] * (cw // lane), axis=1)
                hi = v.astype(BF16)
                over = v - hi.astype(F32)
                mid = over.astype(BF16)
                low_part = (over - mid.astype(F32)).astype(BF16)
                for m in range(4):
                    for third, value in enumerate((hi, mid, low_part)):
                        at = (3 * m + third) * pairs + e * per
                        o3[at:at + per, :] = value[m * per:(m + 1) * per]

            @pl.when(n >= 2)
            def _():
                for d in (0, 1):
                    partner_copy(n - 2, d).wait_send()
                pl.semaphore_wait(credit, 1)

            for rel in (1, 0):
                for d in (0, 1):
                    hot = one_hot(lin(xs[d], ys[d], either(rel)))
                    at = 3 * (2 * d + rel) * pairs
                    total = jnp.dot(hot, o3[at:at + pairs, :], preferred_element_type=F32)
                    total += jnp.dot(hot, o3[at + pairs:at + 2 * pairs, :], preferred_element_type=F32)
                    total += jnp.dot(hot, o3[at + 2 * pairs:at + 3 * pairs, :], preferred_element_type=F32)
                    if rel == 1:
                        pp[n % 2, d] = total
                        partner_copy(n, d).start()
                    else:
                        pb[n % 2, d] = total

        def join(n):
            k, j = look_up([u[0] for u in UNITS], n), look_up([u[1] for u in UNITS], n)
            count = look_up([sum(1 for m in SENDS if m < at) for at in range(units)], n)
            slot = count % 4
            for at in range(units):
                if SEND_JOIN[at]:
                    @pl.when(n == at)
                    def _(at=at):
                        send(SEND_JOIN[at], load_w)
            for d in (0, 1):
                partner_copy(n, d).wait_recv()

            @pl.when((j < 3) & (count >= 4))
            def _():
                for d in (0, 1):
                    ring_copy(slot, d, k, 0).wait_send()

            for d in (0, 1):
                @pl.when(j == 0)
                def _():
                    sb[slot, d] = pb[n % 2, d] + db[n % 2, d]

                @pl.when((j > 0) & (j < 3))
                def _():
                    ring_copy(slot, d, k, j - 1).wait_recv()
                    sb[slot, d] = pb[n % 2, d] + db[n % 2, d] + rb[d, k, j - 1]

                @pl.when(j < 3)
                def _():
                    ring_copy(slot, d, k, j).start()

            for order, at in enumerate(FINALS):
                @pl.when(n == at)
                def _(order=order, at=at):
                    kk = UNITS[at][0]
                    if order >= 2:
                        local, away = out_copies(order % 2, kk)
                        local.wait()
                        away.wait_send()
                    local, away = out_copies(order % 2, kk)
                    for d in (1, 0):
                        ring_copy(0, d, kk, 2).wait_recv()
                        fb[order % 2, d] = (pb[at % 2, d] + db[at % 2, d] + rb[d, kk, 2]).astype(BF16)
                        (local, away)[d].start()

            @pl.when(n < units - 2)
            def _():
                pl.semaphore_signal(credit, inc=1, device_id=dev_p, device_id_type=MESH)

        send([action for action in SEND_MAKE[0] if action[0] != 'lw'])
        load_w(UNITS[0][0])
        first_use(UNITS[0][1])
        for copy in h_loads(0, UNITS[0][1]):
            copy.start()
        seen = [int(at + 1 < units and FIRST_STEP[UNITS[at + 1][1]] <= at) for at in range(units)]

        def operation(at, carry):
            n = look_up([o[1] for o in ORDER], at)

            @pl.when(look_up([o[0] for o in ORDER], at) == 0)
            def _():
                for step, first in FIRST_STEP.items():
                    if first > 0:
                        @pl.when(n == first)
                        def _(step=step, first=first):
                            send(SEND_MAKE[first], load_w)
                            first_use(step)
                            for copy in h_loads(first, step):
                                copy.start()

                make(n)

                @pl.when(look_up(seen, n) == 1)
                def _():
                    for copy in h_loads(n + 1, look_up([u[1] for u in UNITS[1:]], n)):
                        copy.start()

            @pl.when(look_up([o[0] for o in ORDER], at) == 1)
            def _():
                join(n)

            return carry

        lax.fori_loop(0, len(ORDER), operation, 0)
        for d in (0, 1):
            for n in (units - 2, units - 1):
                partner_copy(n, d).wait_send()
            for slot in range(4):
                ring_copy(slot, d, 0, 0).wait_send()
        for slot in (0, 1):
            local, away = out_copies(slot, 0)
            local.wait()
            away.wait_send()
        all_sent()
        for k in range(kc):
            out_copies(0, k)[1].wait_recv()

    lane = min(128, cw)
    send([action for action in SEND_END if action[0] != 'lw'])

    pl.run_scoped(
        phase_two,
        pltpu.VMEM((kc, deep, cw), BF16),
        pltpu.VMEM((2, 4, h_ref.shape[4], 4, per, LANES), BF16),
        pltpu.VMEM((el, 4, per, lane), F32),
        pltpu.VMEM((2, 2, rows, cw), F32),
        pltpu.VMEM((2, 2, rows, cw), F32),
        pltpu.VMEM((4, 2, rows, cw), F32),
        pltpu.VMEM((2, 2, rows, cw), BF16),
        pltpu.SemaphoreType.DMA((kc,)),
        pltpu.SemaphoreType.DMA((2, 4, 4)),
        pltpu.SemaphoreType.DMA((2, 2)),
        pltpu.SemaphoreType.DMA((4, 2)),
        pltpu.SemaphoreType.DMA((2,)),
        pltpu.SemaphoreType.DMA((2,)),
    )


def solution(mesh):
    ny, eps = mesh.shape['tp'], mesh.shape['ep']
    nx = eps // 2
    row_spec = P(('dp', 'ep', 'tp'), None)
    w_in_spec = P('ep', None, 'tp')
    w_out_spec = P('ep', 'tp', None)

    def local_moe(x, ids, gates, w_gate, w_up, w_down):
        rows, width = x.shape
        el, _, ff = w_gate.shape
        experts = el * eps
        per = rows * ids.shape[1] // experts
        pairs = el * per
        cw = width // 2 // CHUNKS
        hbm = pl.BlockSpec(memory_space=pl.ANY)
        vmem = pl.BlockSpec(memory_space=pltpu.VMEM)
        dma = pltpu.SemaphoreType.DMA
        outs = pl.pallas_call(
            functools.partial(moe_kernel, nx, ny),
            name='moe_kernel',
            out_shape=[
                jax.ShapeDtypeStruct((rows, width), BF16),
                jax.ShapeDtypeStruct((nx, ny, 2, rows, width), BF16),
                jax.ShapeDtypeStruct((ny, nx, ny, 2, el * ff // LANES, per, LANES), BF16),
                jax.ShapeDtypeStruct((CHUNKS, ny, el, ff, cw), BF16),
            ],
            in_specs=[hbm, vmem, vmem, hbm, hbm, hbm],
            out_specs=[hbm] * 4,
            scratch_shapes=[
                pltpu.VMEM((ny * eps, 8, pairs), F32),
                pltpu.VMEM((eps, 8, pairs), F32),
                pltpu.VMEM((experts, rows), F32),
                pltpu.VMEM((experts, rows), F32),
                pltpu.VMEM((2, CHUNKS, 3, rows, cw), F32),
                pltpu.VMEM((2, 2, rows, cw), F32),
                dma((ny * eps,)), dma((ny * eps,)),
                dma((4,)), dma((4,)),
                dma((4, 4)), dma((4, 4)),
                dma((2, width // cw)), dma((width // cw,)), pltpu.SemaphoreType.REGULAR,
                pltpu.VMEM((12 * pairs, cw), BF16),
                dma((16,)), dma((16,)), dma((16,)), dma((16,)),
            ] + [dma((CHUNKS, PIECES))] * 6 + [
                dma((2, CHUNKS, 3)), dma((2, 2)), dma((CHUNKS,)),
                pltpu.SemaphoreType.REGULAR,
            ],
            compiler_params=pltpu.CompilerParams(collective_id=0, has_side_effects=True, vmem_limit_bytes=67 * 1000 * 1000),
        )(x, ids.T, gates.T, jnp.transpose(w_gate, (0, 2, 1)), jnp.transpose(w_up, (0, 2, 1)), w_down)
        return outs[0]

    return jax.shard_map(
        local_moe, mesh=mesh, in_specs=(row_spec, row_spec, row_spec, w_in_spec, w_in_spec, w_out_spec),
        out_specs=row_spec, check_vma=False)
```

```python
import functools

import jax
import jax.numpy as jnp
from jax import lax
from jax.experimental import pallas as pl
from jax.experimental.pallas import tpu as pltpu
from jax.sharding import PartitionSpec as P

MESH = pl.DeviceIdType.MESH
CHUNKS = 4
LANES = 256
PIECES = 2
BF16 = jnp.bfloat16
F32 = jnp.float32

S, A, B, O = 0, 1, 2, 3

SPLIT = (14, 15)
UNITS = ((1, 0), (0, 0), (2, 0), (0, 1), (1, 1), (2, 1), (1, 2), (3, 0), (2, 2), (3, 1), (0, 2), (2, 3), (3, 2), (1, 3), (0, 3), (3, 3), )
ORDER = ((0, 0), (1, 0), (0, 1), (0, 2), (1, 1), (1, 2), (0, 3), (0, 4), (1, 3), (0, 5), (1, 4), (0, 6), (1, 5), (0, 7), (1, 6), (0, 8), (1, 7), (1, 8), (0, 9), (0, 10), (1, 9), (0, 11), (1, 10), (0, 12), (1, 11), (0, 13), (1, 12), (0, 14), (1, 13), (0, 15), (1, 14), (1, 15), )
OPPOSITE_VIA_A = 4
OPPOSITE = (2,)
SEND_START = (('wa', 1, 1), ('wb', 0, 0), ('wb', 2, 0), ('wb', 1, 1), ('wb', 3, 1), )
SEND_BEFORE = (
    (),
    (),
    (('hd', 1), ('wa', 1, 0), ('wa', 0, 1), ('wa', 2, 0), ('wa', 3, 0), ('wf', 1, 1), ('wb', 1, 0), ('wb', 2, 1), ),
    (),
    (),
    (),
    (('hd', 5), ('wa', 0, 0), ('hd', 2), ),
    (('wf', 1, 0), ),
    (('wf', 0, 1), ),
    (('hd', 8), ('wb', 0, 1), ),
    (),
    (('hf', 8), ('wa', 2, 1), ('hd', 10), ),
    (('hd', 11), ('hd', 7), ('wf', 2, 0), ('wf', 0, 0), ),
    (('hd', 12), ),
    (('hf', 11), ),
    (('hd', 14, 1), ('hd', 14, 0), ('wf', 2, 1), ),
)
SEND_AFTER = (
    (),
    (),
    (),
    (),
    (),
    (),
    (),
    (),
    (),
    (),
    (),
    (),
    (),
    (('hf', 10), ),
    (('hf', 7), ('hd', 13), ),
    (),
)
SEND_END = (('hf', 14, 1), ('hd', 15, 1), ('hd', 15, 0), ('wb', 3, 0), ('wf', 3, 0), ('lw', 0), ('lw', 1), )
SEND_MAKE = (
    (),
    (('lw', 2), ),
    (('hf', 15, 1), ),
    (),
    (),
    (),
    (),
    (('lw', 3), ),
    (),
    (),
    (('hf', 9), ),
    (),
    (),
    (),
    (),
    (),
)
SEND_JOIN = (
    (('hf', 14, 0), ),
    (('hf', 15, 0), ('wa', 3, 1), ('hd', 4), ('hd', 0), ('hd', 3), ),
    (),
    (),
    (('wf', 3, 1), ('hd', 6), ('hd', 9), ),
    (),
    (),
    (('hf', 6), ),
    (),
    (),
    (),
    (),
    (),
    (),
    (),
    (),
)


def order_of(i):
    last, r = i // 12, i % 3
    return (1 - last) * (r + r // 2) + 2 * last, (1 - last) * (i // 3) + last * (i - 12)


BATCH = {order_of(i): i for i in range(16)}
AHEAD = (0, 0, 1, 1, 0, 1, 1, 0, 1, 1, 0, 1, 0, 0, 0, 0)
FIRST_STEP = {}
for place_in_order, (chunk_of, step_of) in enumerate(UNITS):
    FIRST_STEP.setdefault(step_of, place_in_order)
SENDS = [n for n, (_, j) in enumerate(UNITS) if j < 3]
FINALS = [n for n, (_, j) in enumerate(UNITS) if j == 3]


def place(y, q):
    high, low = y // 2, y % 2
    return 2 * ((high + q // 2) % 2) + (low + (q + 1) // 2) % 2


def look_up(table, n):
    value = jnp.int32(table[0])
    for at in range(1, len(table)):
        if table[at] != table[0]:
            value = jnp.where(n == at, table[at], value)
    return value


def routing_tables(ids_ref, gate_ref, meta_ref, slot_ref, weight_ref, per):
    top, rows = ids_ref.shape
    experts = slot_ref.shape[0]
    devices, _, pairs = meta_ref.shape
    group = experts // devices
    expert = lax.broadcasted_iota(jnp.int32, (experts, rows), 0)
    chosen = jnp.zeros((experts, rows), F32)
    weight = jnp.zeros((experts, rows), F32)
    for j in range(top):
        here = expert == ids_ref[j:j + 1, :]
        chosen = jnp.where(here, 1.0, chosen)
        weight = jnp.where(here, gate_ref[j:j + 1, :], weight)
    earlier = lax.broadcasted_iota(jnp.int32, (rows, rows), 0) < lax.broadcasted_iota(jnp.int32, (rows, rows), 1)
    rank = jnp.dot(chosen.astype(BF16), earlier.astype(F32).astype(BF16), preferred_element_type=F32)
    slot_ref[...] = jnp.where(chosen > 0.0, rank, -1.0)
    weight_ref[...] = weight
    lane = lax.broadcasted_iota(jnp.int32, (group, pairs), 1)
    sub = lax.broadcasted_iota(jnp.int32, (group, pairs), 0)
    mine = ((lane >= sub * per) & (lane < (sub + 1) * per)).astype(F32).astype(BF16)
    place_in_expert = lax.broadcasted_iota(jnp.int32, (rows, pairs), 1)
    for m in range(1, group):
        place_in_expert = jnp.where(lax.broadcasted_iota(jnp.int32, (rows, pairs), 1) >= m * per,
                                    lax.broadcasted_iota(jnp.int32, (rows, pairs), 1) - m * per, place_in_expert)
    place_in_expert = place_in_expert.astype(F32)
    row = lax.broadcasted_iota(jnp.int32, (8, rows), 1)
    high = (row // 2).astype(F32).astype(BF16)
    low = (row % 2).astype(F32).astype(BF16)
    top_row = lax.broadcasted_iota(jnp.int32, (8, pairs), 0)

    def spread(part):
        return lax.dot_general(part, mine, (((0,), (0,)), ((), ())), preferred_element_type=F32)

    def table(d, carry):
        at = pl.ds(pl.multiple_of(d * group, group), group)
        hit = (spread(slot_ref[at, :].astype(BF16)) == place_in_expert).astype(F32)
        hot = hit.astype(BF16)
        position = 2.0 * jnp.dot(high, hot, preferred_element_type=F32) + jnp.dot(low, hot, preferred_element_type=F32)
        w = weight_ref[at, :]
        first = w.astype(BF16)
        over = w - first.astype(F32)
        second = over.astype(BF16)
        third = (over - second.astype(F32)).astype(BF16)
        value = jnp.sum((spread(first) + spread(second) + spread(third)) * hit, axis=0, keepdims=True)
        meta_ref[d] = jnp.where(top_row == 0, position, jnp.broadcast_to(value, (8, pairs)))
        return carry

    lax.fori_loop(0, devices, table, 0)


def moe_kernel(nx, ny, x_ref, ids_ref, gate_ref, wg_ref, wu_ref, wd_ref, out_ref, tok_ref, h_ref, w_ref,
               metav, meta_ref, slot_ref, weight_ref, rb, db, ms, mr, ty_s, ty_r, tx_s, tx_r, td_s, td_r, room, o3, hd_s, hd_r, hf_s, hf_r,
               wa_s, wa_r, wb_s, wb_r, wf_s, wf_r, rs_r, db_r, of_r, credit):
    rows, width = x_ref.shape
    half = rows // 2
    el, ff, _ = wg_ref.shape
    per = h_ref.shape[5]
    rest = ff - LANES * (ff // LANES)
    whole = el * (ff // LANES)
    assert ff // LANES == 1 and (el * rest) % LANES == 0 and rest <= 128
    pairs = el * per
    kc, cw = w_ref.shape[0], w_ref.shape[4]
    ep_piece = el // PIECES
    eps = 2 * nx
    y = lax.axis_index('tp')
    ep = lax.axis_index('ep')
    x, c = ep // 2, ep % 2
    ya, yb, yo = place(y, A), place(y, B), place(y, O)
    yq = (y, ya, yb, yo)
    xp, xm = (x + 1) % nx, (x + nx - 1) % nx
    colb = ((y + y // 2) % 2) * (kc * cw)
    cola = ((ya + ya // 2) % 2) * (kc * cw)
    me = y * eps + ep

    dev_a = {'tp': ya, 'ep': ep}
    dev_b = {'tp': yb, 'ep': ep}
    dev_p = {'tp': y, 'ep': 2 * x + 1 - c}
    dev_xp = {'tp': y, 'ep': 2 * xp + c}
    dev_xm = {'tp': y, 'ep': 2 * xm + c}

    def remote(src, dst, send, recv, dev):
        return pltpu.make_async_remote_copy(src_ref=src, dst_ref=dst, send_sem=send, recv_sem=recv, device_id=dev, device_id_type=MESH)

    def lin(xs, ys, cs):
        return ys * eps + 2 * xs + cs

    def either(rel):
        return c if rel == 0 else 1 - c

    barrier = pltpu.get_barrier_semaphore()

    def peer_of(d):
        other = (me + d) % (ny * eps)
        return other // eps, other % eps

    def greet(d, carry):
        py, pe = peer_of(d)
        pl.semaphore_signal(barrier, inc=1, device_id={'tp': py, 'ep': pe}, device_id_type=MESH)
        return carry

    lax.fori_loop(1, ny * eps, greet, 0)
    pl.semaphore_wait(barrier, ny * eps - 1)

    def meta_copy(d):
        py, pe = peer_of(d)
        return remote(meta_ref.at[pe], metav.at[me], ms.at[d], mr.at[me], {'tp': py, 'ep': pe})

    def meta_send(d, carry):
        meta_copy(d).start()
        return carry

    def own(dxm, q):
        return tok_ref.at[(x + dxm) % nx, yq[q], c]

    def rows_of(ref, part, cut=None):
        cut = half if cut is None else cut
        return ref.at[pl.ds(part * cut, (cut, rows - cut)[part])]

    def ty(n):
        if n < 2:
            return remote(x_ref, tok_ref.at[x, y, c], ty_s.at[n], ty_r.at[n], (dev_a, dev_b)[n])
        block = rows_of(own(0, (B, A)[n - 2]), n - 2, rows * OPPOSITE_VIA_A // 4)
        return remote(block, block, ty_s.at[n], ty_r.at[n], (dev_a, dev_b)[n - 2])

    def tx(q, n):
        if n < 2:
            return remote(x_ref if q == S else own(0, q), own(0, q), tx_s.at[q, n], tx_r.at[q, n], (dev_xp, dev_xm)[n])
        block = rows_of(own((3, 1)[n - 2], q), n - 2)
        return remote(block, block, tx_s.at[q, n], tx_r.at[q, n], (dev_xp, dev_xm)[n - 2])


    def wa(k, g):
        src = wd_ref.at[pl.ds(g * ep_piece, ep_piece), :, pl.ds(pl.multiple_of(cola + k * cw, cw), cw)]
        return remote(src, w_ref.at[k, y, pl.ds(g * ep_piece, ep_piece)], wa_s.at[k, g], wa_r.at[k, g], dev_a)

    def wb(k, g):
        src = wd_ref.at[pl.ds(g * ep_piece, ep_piece), :, pl.ds(pl.multiple_of(colb + k * cw, cw), cw)]
        return remote(src, w_ref.at[k, y, pl.ds(g * ep_piece, ep_piece)], wb_s.at[k, g], wb_r.at[k, g], dev_b)

    def wf(k, g):
        block = w_ref.at[k, ya, pl.ds(g * ep_piece, ep_piece)]
        return remote(block, block, wf_s.at[k, g], wf_r.at[k, g], dev_b)

    def hd(i, s=None):
        dxm, q = order_of(i)
        block = h_ref.at[y, (x + dxm) % nx, yq[q]]
        at = i
        if s is not None:
            block, at = block.at[either(s)], 16 * s + i
        return remote(block, block, hd_s.at[at], hd_r.at[at], dev_a if q < 2 else dev_b)

    def hf(i, s=None):
        dxm, q = order_of(i)
        block = h_ref.at[yb, (x + dxm) % nx, place(yb, q)]
        at = i
        if s is not None:
            block, at = block.at[either(s)], 16 * s + i
        return remote(block, block, hf_s.at[at], hf_r.at[at], dev_a)

    def messages(i):
        return ((i, 0), (i, 1)) if i in SPLIT else ((i,),)

    def send(actions, load_w=None):
        for action in actions:
            kind, at = action[0], action[1:]
            if kind == 'wf':
                wa(*at).wait_recv()
            if kind == 'hf':
                hd(*at).wait_recv()
            if kind == 'lw':
                load_w(*at)
            else:
                {'wa': wa, 'wb': wb, 'wf': wf, 'hd': hd, 'hf': hf}[kind](*at).start()

    for n in (0, 1):
        ty(n).start()
        tx(S, n).start()
    routing_tables(ids_ref, gate_ref, meta_ref, slot_ref, weight_ref, per)
    lax.fori_loop(1, ny * eps, meta_send, 0)
    metav[me] = meta_ref[ep]
    send(SEND_START)

    def came(q):
        for n in (0, 1):
            tx(q, n).wait_recv()

    def both(q, first):
        tx(q, first).start()
        tx(q, first + 1).start()

    def comm(step):
        if step == 1:
            ty(0).wait_recv()
            ty(1).wait_recv()
            for n in OPPOSITE:
                ty(n).start()
            both(A, 0)
            both(B, 0)
            came(S)
        if step == 4:
            came(A)
            for n in OPPOSITE:
                ty(n).wait_recv()
            both(O, 0)
            both(S, 2)
            both(A, 2)
        if step in (7, 10):
            q = {7: B, 10: O}[step]
            came(q)
            both(q, 2)
        if step >= 12:
            tx(step - 12, 2).wait_recv()
            tx(step - 12, 3).wait_recv()

    row_id = lax.broadcasted_iota(jnp.int32, (rows, pairs), 0)

    def one_hot(src):
        pos = metav[src, 0:1, :].astype(jnp.int32)
        return (row_id == pos).astype(F32).astype(BF16)

    def meta_wait(src):
        remote(meta_ref.at[0], metav.at[src], ms.at[0], mr.at[src], dev_p).wait_recv()

    def phase_one(wg, wu, tb, xg, hb, left, wl, tl, hl):
        load_g = pltpu.make_async_copy(wg_ref, wg, wl.at[0])
        load_u = pltpu.make_async_copy(wu_ref, wu, wl.at[1])
        load_g.start()
        load_u.start()

        def store(i):
            dxm, q = order_of(i)
            return pltpu.make_async_copy(hb, h_ref.at[y, (x + dxm) % nx, place(y, q)], hl.at[0])

        def rows_in(i):
            dxm, q = order_of(i)
            return pltpu.make_async_copy(tok_ref.at[(x + dxm) % nx, place(y, q), c], tb.at[i % 2], tl.at[i % 2])

        def to_partner(i, m):
            return remote(tb.at[i % 2, :, pl.ds(m * cw, cw)], o3.at[pl.ds(m * rows, rows)], td_s.at[i % 2, m], td_r.at[m], dev_p)

        def batch(i, carry):
            @pl.when(i > 0)
            def _():
                store(i - 1).wait()

            for step in range(1, 16):
                if SEND_BEFORE[step] or SEND_AFTER[step] or step in (1, 4, 7, 10) or step >= 12:
                    @pl.when(i == step)
                    def _(step=step):
                        send(SEND_BEFORE[step])
                        comm(step)
                        send(SEND_AFTER[step])

            dxm, q = order_of(i)
            xs, ys = (x + dxm) % nx, place(y, q)
            ahead, next_ahead = look_up(AHEAD, i), look_up(AHEAD[1:] + (0,), i)

            @pl.when(ahead == 0)
            def _():
                @pl.when(i >= 2)
                def _():
                    for m in range(width // cw):
                        to_partner(i - 2, m).wait_send()

                @pl.when(i == 0)
                def _():
                    pltpu.make_async_copy(x_ref, tb.at[0], tl.at[0]).start()

                @pl.when(i > 0)
                def _():
                    rows_in(i).start()

                rows_in(i).wait()

                @pl.when(i > 0)
                def _():
                    pl.semaphore_wait(room, 1)

                for m in range(width // cw):
                    to_partner(i, m).start()

            @pl.when(next_ahead == 1)
            def _():
                for m in range(width // cw):
                    to_partner(i - 1, m).wait_send()
                rows_in(i + 1).start()

            @pl.when(i > 0)
            def _():
                meta_wait(lin(xs, ys, c))

            hot = one_hot(lin(xs, ys, c))
            step = min(512, width)
            for lo in range(0, width, step):
                got = lax.dot_general(hot, tb[i % 2, :, lo:lo + step], (((0,), (0,)), ((), ())), preferred_element_type=F32)
                xg[:, 0, :, lo:lo + step] = got.astype(BF16).reshape(el, per, step)
            meta_wait(lin(xs, ys, 1 - c))
            hot = one_hot(lin(xs, ys, 1 - c))
            for m in range(width // cw):
                to_partner(i, m).wait_recv()
                got = lax.dot_general(hot, o3[m * rows:(m + 1) * rows, :], (((0,), (0,)), ((), ())), preferred_element_type=F32)
                xg[:, 1, :, m * cw:(m + 1) * cw] = got.astype(BF16).reshape(el, per, cw)

            @pl.when(i < 15)
            def _():
                pl.semaphore_signal(room, inc=1, device_id=dev_p, device_id_type=MESH)

            @pl.when(next_ahead == 1)
            def _():
                rows_in(i + 1).wait()
                pl.semaphore_wait(room, 1)
                for m in range(width // cw):
                    to_partner(i + 1, m).start()

            @pl.when(i == 0)
            def _():
                load_g.wait()
                load_u.wait()

            for e in range(el):
                lhs = xg[e].reshape(2 * per, width)
                a = lax.dot_general(lhs, wg[e], (((1,), (1,)), ((), ())), preferred_element_type=F32)
                b = lax.dot_general(lhs, wu[e], (((1,), (1,)), ((), ())), preferred_element_type=F32)
                hid = a * jax.nn.sigmoid(a) * b
                for s in (0, 1):
                    hb[either(s), e] = hid[s * per:(s + 1) * per, :LANES].astype(BF16)
                left[e] = hid[:, LANES:]
            packed = jnp.concatenate([left[e] for e in range(el)], axis=1).astype(BF16)
            for m in range(el * rest // LANES):
                for s in (0, 1):
                    hb[either(s), whole + m] = packed[s * per:(s + 1) * per, m * LANES:(m + 1) * LANES]
            store(i).start()
            return carry

        lax.fori_loop(0, 16, batch, 0)
        for i in (14, 15):
            for m in range(width // cw):
                to_partner(i, m).wait_send()
        store(15).wait()

    pl.run_scoped(
        phase_one,
        pltpu.VMEM((el, ff, width), BF16),
        pltpu.VMEM((el, ff, width), BF16),
        pltpu.VMEM((2, rows, width), BF16),
        pltpu.VMEM((el, 2, per, width), BF16),
        pltpu.VMEM((2,) + h_ref.shape[4:], BF16),
        pltpu.VMEM((el, 2 * per, rest), F32),
        pltpu.SemaphoreType.DMA((2,)),
        pltpu.SemaphoreType.DMA((2,)),
        pltpu.SemaphoreType.DMA((1,)),
    )

    def all_sent():
        def meta_done(d, carry):
            meta_copy(d).wait_send()
            return carry

        lax.fori_loop(1, ny * eps, meta_done, 0)
        for n in (0, 1) + OPPOSITE:
            ty(n).wait_send()
        for q in (S, A, B, O):
            for n in range(4):
                tx(q, n).wait_send()
        for k in range(kc):
            for g in range(PIECES):
                wa(k, g).wait_send()
                wb(k, g).wait_send()
                wf(k, g).wait_send()
        for i in range(16):
            for message in messages(i):
                hd(*message).wait_send()
                if order_of(i)[1] >= 2:
                    hf(*message).wait_send()

    def window(e):
        return e * rest // 128 * 128, -(-(e + 1) * rest // 128) * 128

    def offset(e, q):
        before = sum(LANES + window(m)[1] - window(m)[0] for m in range(e))
        return 4 * before + q * (LANES + window(e)[1] - window(e)[0])

    deep = offset(el, S)

    units = len(UNITS)

    def phase_two(wv, hv, gc, pb, pp, sb, fb, wl, hvl, pp_s, rs_s, of_s, ol):
        lane = gc.shape[3]

        def clear(k):
            for e in range(el):
                low, high = window(e)
                for q in (S, A, B, O):
                    at = offset(e, q) + LANES
                    for start, stop in ((0, e * rest - low), ((e + 1) * rest - low, high - low)):
                        if stop > start:
                            wv[k, at + start:at + stop] = jnp.zeros((stop - start, cw), BF16)

        def blocks(j):
            return ((x + 2 * nx - 1 - j) % nx, (x + 1 + j) % nx), (y, ya)

        def w_loads(k):
            copies = []
            for q in (S, A, B, O):
                for e in range(el):
                    if q == S:
                        src = wd_ref.at[e, :, pl.ds(pl.multiple_of(colb + k * cw, cw), cw)]
                    else:
                        src = w_ref.at[k, yq[q], e]
                    low, high = window(e)
                    at = offset(e, q)
                    copies.append(pltpu.make_async_copy(src.at[pl.ds(0, LANES)], wv.at[k, pl.ds(at, LANES)], wl.at[k]))
                    copies.append(pltpu.make_async_copy(
                        src.at[pl.ds(LANES, rest)], wv.at[k, pl.ds(at + LANES + e * rest - low, rest)], wl.at[k]))
            return copies

        def load_w(k):
            for g in range(PIECES):
                wb(k, g).wait_recv()
                wf(k, g).wait_recv()
            for copy in w_loads(k):
                copy.start()
            clear(k)

        def h_loads(n, j):
            xs, ys = blocks(j)
            copies = []
            for d in (0, 1):
                for rel in (0, 1):
                    for q in (S, A, B, O):
                        copies.append(pltpu.make_async_copy(
                            h_ref.at[yq[q], xs[d], ys[d], either(rel)], hv.at[n % 2, q, :, 2 * d + rel], hvl.at[n % 2, q, 2 * d + rel]))
            return copies

        def first_use(j):
            minus, plus = (3 - j) % 4, (1 + j) % 4
            for copy, block in ((hd, (minus, A)), (hd, (plus, S)), (hf, (minus, O)), (hf, (plus, B))):
                for message in messages(BATCH[block]):
                    copy(*message).wait_recv()

        def partner_copy(n, d):
            return remote(pp.at[n % 2, d], db.at[n % 2, d], pp_s.at[n % 2, d], db_r.at[n % 2, d], dev_p)

        def ring_copy(slot, d, k, j):
            return remote(sb.at[slot, d], rb.at[d, k, j], rs_s.at[slot, d], rs_r.at[d, k, j], (dev_xp, dev_xm)[d])

        def out_copies(slot, k):
            cols = out_ref.at[:, pl.ds(pl.multiple_of(colb + k * cw, cw), cw)]
            return (
                pltpu.make_async_copy(fb.at[slot, 0], cols, ol.at[slot]),
                remote(fb.at[slot, 1], cols, of_s.at[slot], of_r.at[k], dev_a),
            )

        def make(n):
            k, j = look_up([u[0] for u in UNITS], n), look_up([u[1] for u in UNITS], n)
            xs, ys = blocks(j)
            for at in range(units):
                new_chunk = UNITS[at][0] not in [u[0] for u in UNITS[:at]]
                first = at in FIRST_STEP.values()
                if (not first and SEND_MAKE[at]) or new_chunk:
                    @pl.when(n == at)
                    def _(at=at, new_chunk=new_chunk, first=first):
                        if not first:
                            send(SEND_MAKE[at], load_w)
                        if new_chunk:
                            pltpu.make_async_copy(w_ref.at[UNITS[at][0]], w_ref.at[UNITS[at][0]], wl.at[UNITS[at][0]]).wait()
            for d in (0, 1):
                for rel in (0, 1):
                    gate = metav[lin(xs[d], ys[d], either(rel)), 1:2, :]
                    gc[:, 2 * d + rel] = jnp.transpose(jnp.broadcast_to(gate, (lane, pairs))).reshape(el, per, lane)
            for copy in h_loads(n, j):
                copy.wait()

            @pl.when(n == 0)
            def _():
                later = [action for action in SEND_END + SEND_MAKE[0] if action[0] == 'lw' and action[1] != UNITS[0][0]]
                send(later, load_w)

            for e in range(el):
                low, high = window(e)
                parts = []
                for q in (S, A, B, O):
                    parts.append(hv[n % 2, q, e].reshape(4 * per, LANES))
                    for at in range(low, high, 128):
                        parts.append(hv[n % 2, q, whole + at // LANES, :, :, at % LANES:at % LANES + 128].reshape(4 * per, 128))
                size = 4 * (LANES + high - low)
                o = jnp.dot(jnp.concatenate(parts, axis=1), wv[k, offset(e, S):offset(e, S) + size], preferred_element_type=F32)
                g = gc[e].reshape(4 * per, lane)
                v = o * jnp.concatenate([g] * (cw // lane), axis=1)
                hi = v.astype(BF16)
                over = v - hi.astype(F32)
                mid = over.astype(BF16)
                low_part = (over - mid.astype(F32)).astype(BF16)
                for m in range(4):
                    for third, value in enumerate((hi, mid, low_part)):
                        at = (3 * m + third) * pairs + e * per
                        o3[at:at + per, :] = value[m * per:(m + 1) * per]

            @pl.when(n >= 2)
            def _():
                for d in (0, 1):
                    partner_copy(n - 2, d).wait_send()
                pl.semaphore_wait(credit, 1)

            for rel in (1, 0):
                for d in (0, 1):
                    hot = one_hot(lin(xs[d], ys[d], either(rel)))
                    at = 3 * (2 * d + rel) * pairs
                    total = jnp.dot(hot, o3[at:at + pairs, :], preferred_element_type=F32)
                    total += jnp.dot(hot, o3[at + pairs:at + 2 * pairs, :], preferred_element_type=F32)
                    total += jnp.dot(hot, o3[at + 2 * pairs:at + 3 * pairs, :], preferred_element_type=F32)
                    if rel == 1:
                        pp[n % 2, d] = total
                        partner_copy(n, d).start()
                    else:
                        pb[n % 2, d] = total

        def join(n):
            k, j = look_up([u[0] for u in UNITS], n), look_up([u[1] for u in UNITS], n)
            count = look_up([sum(1 for m in SENDS if m < at) for at in range(units)], n)
            slot = count % 4
            for at in range(units):
                if SEND_JOIN[at]:
                    @pl.when(n == at)
                    def _(at=at):
                        send(SEND_JOIN[at], load_w)
            for d in (0, 1):
                partner_copy(n, d).wait_recv()

            @pl.when((j < 3) & (count >= 4))
            def _():
                for d in (0, 1):
                    ring_copy(slot, d, k, 0).wait_send()

            for d in (0, 1):
                @pl.when(j == 0)
                def _():
                    sb[slot, d] = pb[n % 2, d] + db[n % 2, d]

                @pl.when((j > 0) & (j < 3))
                def _():
                    ring_copy(slot, d, k, j - 1).wait_recv()
                    sb[slot, d] = pb[n % 2, d] + db[n % 2, d] + rb[d, k, j - 1]

                @pl.when(j < 3)
                def _():
                    ring_copy(slot, d, k, j).start()

            for order, at in enumerate(FINALS):
                @pl.when(n == at)
                def _(order=order, at=at):
                    kk = UNITS[at][0]
                    if order >= 2:
                        local, away = out_copies(order % 2, kk)
                        local.wait()
                        away.wait_send()
                    local, away = out_copies(order % 2, kk)
                    for d in (1, 0):
                        ring_copy(0, d, kk, 2).wait_recv()
                        fb[order % 2, d] = (pb[at % 2, d] + db[at % 2, d] + rb[d, kk, 2]).astype(BF16)
                        (local, away)[d].start()

            @pl.when(n < units - 2)
            def _():
                pl.semaphore_signal(credit, inc=1, device_id=dev_p, device_id_type=MESH)

        send([action for action in SEND_MAKE[0] if action[0] != 'lw'])
        load_w(UNITS[0][0])
        first_use(UNITS[0][1])
        for copy in h_loads(0, UNITS[0][1]):
            copy.start()
        seen = [int(at + 1 < units and FIRST_STEP[UNITS[at + 1][1]] <= at) for at in range(units)]

        def operation(at, carry):
            n = look_up([o[1] for o in ORDER], at)

            @pl.when(look_up([o[0] for o in ORDER], at) == 0)
            def _():
                for step, first in FIRST_STEP.items():
                    if first > 0:
                        @pl.when(n == first)
                        def _(step=step, first=first):
                            send(SEND_MAKE[first], load_w)
                            first_use(step)
                            for copy in h_loads(first, step):
                                copy.start()

                make(n)

                @pl.when(look_up(seen, n) == 1)
                def _():
                    for copy in h_loads(n + 1, look_up([u[1] for u in UNITS[1:]], n)):
                        copy.start()

            @pl.when(look_up([o[0] for o in ORDER], at) == 1)
            def _():
                join(n)

            return carry

        lax.fori_loop(0, len(ORDER), operation, 0)
        for d in (0, 1):
            for n in (units - 2, units - 1):
                partner_copy(n, d).wait_send()
            for slot in range(4):
                ring_copy(slot, d, 0, 0).wait_send()
        for slot in (0, 1):
            local, away = out_copies(slot, 0)
            local.wait()
            away.wait_send()
        all_sent()
        for k in range(kc):
            out_copies(0, k)[1].wait_recv()

    lane = min(128, cw)
    send([action for action in SEND_END if action[0] != 'lw'])

    pl.run_scoped(
        phase_two,
        pltpu.VMEM((kc, deep, cw), BF16),
        pltpu.VMEM((2, 4, h_ref.shape[4], 4, per, LANES), BF16),
        pltpu.VMEM((el, 4, per, lane), F32),
        pltpu.VMEM((2, 2, rows, cw), F32),
        pltpu.VMEM((2, 2, rows, cw), F32),
        pltpu.VMEM((4, 2, rows, cw), F32),
        pltpu.VMEM((2, 2, rows, cw), BF16),
        pltpu.SemaphoreType.DMA((kc,)),
        pltpu.SemaphoreType.DMA((2, 4, 4)),
        pltpu.SemaphoreType.DMA((2, 2)),
        pltpu.SemaphoreType.DMA((4, 2)),
        pltpu.SemaphoreType.DMA((2,)),
        pltpu.SemaphoreType.DMA((2,)),
    )


def solution(mesh):
    ny, eps = mesh.shape['tp'], mesh.shape['ep']
    nx = eps // 2
    row_spec = P(('dp', 'ep', 'tp'), None)
    w_in_spec = P('ep', None, 'tp')
    w_out_spec = P('ep', 'tp', None)

    def local_moe(x, ids, gates, w_gate, w_up, w_down):
        rows, width = x.shape
        el, _, ff = w_gate.shape
        experts = el * eps
        per = rows * ids.shape[1] // experts
        pairs = el * per
        cw = width // 2 // CHUNKS
        hbm = pl.BlockSpec(memory_space=pl.ANY)
        vmem = pl.BlockSpec(memory_space=pltpu.VMEM)
        dma = pltpu.SemaphoreType.DMA
        outs = pl.pallas_call(
            functools.partial(moe_kernel, nx, ny),
            name='moe_kernel',
            out_shape=[
                jax.ShapeDtypeStruct((rows, width), BF16),
                jax.ShapeDtypeStruct((nx, ny, 2, rows, width), BF16),
                jax.ShapeDtypeStruct((ny, nx, ny, 2, el * ff // LANES, per, LANES), BF16),
                jax.ShapeDtypeStruct((CHUNKS, ny, el, ff, cw), BF16),
            ],
            in_specs=[hbm, vmem, vmem, hbm, hbm, hbm],
            out_specs=[hbm] * 4,
            scratch_shapes=[
                pltpu.VMEM((ny * eps, 8, pairs), F32),
                pltpu.VMEM((eps, 8, pairs), F32),
                pltpu.VMEM((experts, rows), F32),
                pltpu.VMEM((experts, rows), F32),
                pltpu.VMEM((2, CHUNKS, 3, rows, cw), F32),
                pltpu.VMEM((2, 2, rows, cw), F32),
                dma((ny * eps,)), dma((ny * eps,)),
                dma((4,)), dma((4,)),
                dma((4, 4)), dma((4, 4)),
                dma((2, width // cw)), dma((width // cw,)), pltpu.SemaphoreType.REGULAR,
                pltpu.VMEM((12 * pairs, cw), BF16),
                dma((32,)), dma((32,)), dma((32,)), dma((32,)),
            ] + [dma((CHUNKS, PIECES))] * 6 + [
                dma((2, CHUNKS, 3)), dma((2, 2)), dma((CHUNKS,)),
                pltpu.SemaphoreType.REGULAR,
            ],
            compiler_params=pltpu.CompilerParams(collective_id=0, has_side_effects=True, vmem_limit_bytes=67 * 1000 * 1000),
        )(x, ids.T, gates.T, jnp.transpose(w_gate, (0, 2, 1)), jnp.transpose(w_up, (0, 2, 1)), w_down)
        return outs[0]

    return jax.shard_map(
        local_moe, mesh=mesh, in_specs=(row_spec, row_spec, row_spec, w_in_spec, w_in_spec, w_out_spec),
        out_specs=row_spec, check_vma=False)
```
